32 devices in a mesh: section: 4 (over y, x), tok: 8 (over z, core).
Axes of the slice: x: 2, y: 2, z: 4, core: 2. Of those that a mesh axis runs over, the one named last changes fastest.
Arguments:
- activations: bfloat16 [8, 2048, 8192], P('section', 'tok'), may hold values from -12 to 12
- projection: bfloat16 [8192, 512], P('tok'), may hold values from -0.0625 to 0.0625
Outputs:
- sketch: float32 [8, 512, 512], P('section', None, 'tok')
- similarity: float32 [8, 2], P('section')
The draws below stay inside these ranges and needn't reach their ends.
All inputs are finite; a program needn't handle non-finite values.
Results may differ from the reference program's by a relative error of at most 0.0003.
Values may be sent and summed in bfloat16 or wider, within the bound.
A program may use at most 64 MiB of HBM per device.

```python
import jax
import jax.numpy as jnp
from jax import lax

D = 8192
RANK = 512
LAYERS = 8
TOKENS = 2048


def draw_activations(key, part):
    keyed = jax.random.fold_in(key, 11)
    key_base, key_weight, key_rows, key_mean, key_noise = jax.random.split(keyed, 5)
    shared = jax.random.normal(key_base, (TOKENS, D), jnp.float32)
    offset = jnp.zeros((D,), jnp.float32)
    mixing = jax.random.uniform(key_weight, (LAYERS,), jnp.float32, 0.2, 1.5)
    row_scale = jnp.exp(jax.random.uniform(key_rows, (LAYERS, TOKENS, 1), jnp.float32, jnp.log(0.3), jnp.log(3.0)))

    def one_layer(layer):
        noise = jax.random.normal(jax.random.fold_in(key_noise, layer), (TOKENS, D), jnp.float32)
        values = row_scale[layer] * (mixing[layer] * shared + noise) + offset
        return jnp.clip(values, -12.0, 12.0).astype(jnp.bfloat16)
    return lax.map(one_layer, jnp.arange(LAYERS, dtype=jnp.int32))


def block_levels(rng, shape, pieces, least, top_value):
    loudness, own = 1.0, jax.random.fold_in(rng, 6)
    for position, blocks in pieces:
        draws = jnp.exp(jax.random.uniform(jax.random.fold_in(own, position), (blocks,), jnp.float32, least / len(pieces), top_value / len(pieces)))
        loudness = loudness * jnp.repeat(draws, shape[position] // blocks).reshape([-1 if axis == position else 1 for axis in range(len(shape))])
    return loudness


def bell_draw(rng, shape, spread, most, cuts=(), held_as=jnp.bfloat16):
    level = block_levels(rng, shape, cuts, -0.22, 0.18) if cuts else 1.0
    drawn = jax.random.normal(rng, shape, jnp.float32) * spread * level
    return jnp.minimum(jnp.maximum(drawn, -most), most).astype(held_as)


def setup_inputs(seed: int = 0) -> dict:
    key_list = jax.random.split(jax.random.key(seed), 3)
    activations = draw_activations(jax.random.fold_in(key_list[2], 71), 0)
    projection = bell_draw(key_list[1], (D, RANK), D ** -0.5, 0.0625, ((0, 8),))
    return {"activations": activations, "projection": projection}


def reference(activations, projection):

    def layer_sketch(layer_acts):
        projected = jnp.dot(layer_acts, projection, preferred_element_type=jnp.float32)
        centred = projected - lax.optimization_barrier(jnp.sum(projected, axis=0)) / TOKENS
        return jnp.dot(centred.T, centred, precision=lax.Precision.HIGHEST)
    sketch = lax.map(layer_sketch, activations)
    flattened = sketch.reshape(sketch.shape[0], -1)
    squares = lax.optimization_barrier(jnp.sum(flattened * flattened, axis=1))
    before = jnp.concatenate([flattened[:1], flattened[:-1]], axis=0)
    beyond = jnp.concatenate([flattened[1:], flattened[-1:]], axis=0)
    square_before = jnp.concatenate([squares[:1], squares[:-1]])
    square_beyond = jnp.concatenate([squares[1:], squares[-1:]])
    earlier = lax.optimization_barrier(jnp.sum(flattened * before, axis=1)) / jnp.sqrt(squares * square_before)
    later = lax.optimization_barrier(jnp.sum(flattened * beyond, axis=1)) / jnp.sqrt(squares * square_beyond)
    return (sketch, jnp.stack([earlier, later], axis=1))
```

```python
import functools
import math

import jax
import jax.numpy as jnp
from jax import lax
from jax.experimental import pallas as pl
from jax.experimental.pallas import tpu as pltpu
from jax.sharding import PartitionSpec as P

F32, BF16 = jnp.float32, jnp.bfloat16
SHARE = 80


def flip(index, mask, size):
    result, bit = 0, 1
    while bit < size:
        digit = (index // bit) % 2
        result = result + bit * ((1 - digit) if mask & bit else digit)
        bit *= 2
    return result


def nearest(chip, n, chips):
    short = jnp.minimum(chip, chips - 1 - chip)
    low_side = chip < chips // 2
    paired = n <= 2 * short
    distance = jnp.where(paired, (n + 1) // 2, n - short)
    lower = jnp.where(paired, jnp.logical_xor(low_side, n % 2 == 0), jnp.logical_not(low_side))
    return jnp.where(lower, chip - distance, chip + distance)


def snake(place, sections):
    half = sections // 2
    return jnp.where(place < half, place, 3 * half - 1 - place)


def gather_plan(half_ring, others, chunks):
    def ring(k, j, c):
        return [("ring", k, j, way, c) for way in ((0, 1) if j < half_ring else (c,))]

    def near(k):
        return [event for c in chunks for j in range(1, half_ring) for event in ring(k, j, c)]

    def relay(k):
        return [("relay", k, way) for way in range(2)] if half_ring > 1 else []

    def far(k):
        return ring(k, half_ring, 0) + ring(k, half_ring, 1)

    before = range(1, others)
    order = [event for k in before for event in near(k)]
    order += [event for k in before for event in relay(k)]
    order += [("own", k) for k in before]
    for k in before:
        order += [("partner", k)] + ([("inner_extra", 2)] if k == 1 else [])
    order += [("inner_extra", k) for k in range(3, others + 1)]
    order += near(others) + relay(others)
    order += [("outer_extra", k) for k in (1, 2)]
    order += [("own", others), ("partner", others)]
    for k in before:
        order += far(k)
    order += [("own_far", k) for k in before] + [("partner_far", k) for k in before]
    order += [("outer_extra", k) for k in range(3, others + 1)]
    return order + far(others) + [("own_far", others), ("partner_far", others)]


def kernel(
    sections, groups, layers, share_rows, acts_hbm, proj_hbm, sketch_ref, sim_ref,
    acts, proj, total, left_op, right_op, gram, pair_in, line_in, mean_out, means, corr,
    edge_out, edge_in, prod_out, prods, prev_prods,
    acts_sem, own_sem, d2d_own, line_s, line_r, ring_s, ring_r, d2d_s, d2d_r,
    mean_s, mean_r, pair_s, pair_r, gl_s, gl_r, edge_s, edge_r, prod_s, prod_r, prev_s, prev_r,
):
    section = lax.axis_index("section")
    tok = lax.axis_index("tok")
    chips = groups // 2
    chip, core = tok // 2, tok % 2
    partner = chip * 2 + 1 - core
    rows = acts.shape[1]
    tok_rows = rows // layers
    depth = proj.shape[1]
    width = proj.shape[2]
    slab = width // groups
    half_ring = sections // 2
    piece = depth // sections
    sizes = (share_rows, share_rows, piece - 2 * share_rows)
    chunks = [c for c in range(3) if sizes[c]]
    align = math.gcd(piece, share_rows)
    place = snake(section, sections)
    to_right = snake((place + 1) % sections, sections)
    to_left = snake((place + sections - 1) % sections, sections)

    def rows_of(at, c):
        start = at % sections * piece + sum(sizes[:c])
        return pl.ds(pl.multiple_of(start, align), sizes[c])

    own_copies = []
    for n in range(sections):
        part = pl.ds(pl.multiple_of((place + n) % sections * piece, piece), piece)
        own_copies.append(
            pltpu.make_async_copy(proj_hbm.at[part], proj.at[tok, part], own_sem.at[n])
        )
        own_copies[-1].start()

    with jax.named_scope("barrier"):
        barrier = pltpu.get_barrier_semaphore()
        beside = [{"tok": partner}, {"section": to_right}]
        if sections > 2:
            beside.append({"section": to_left})
        for where in beside:
            pl.semaphore_signal(
                barrier, inc=1, device_id=where, device_id_type=pl.DeviceIdType.MESH
            )
        inner_chip = jnp.logical_and(chip > 0, chip < chips - 1)
        for step in (-1, 1):
            @pl.when(jnp.logical_and(chip + step >= 0, chip + step <= chips - 1))
            def _():
                pl.semaphore_signal(
                    barrier, inc=1, device_id={"tok": tok + 2 * step},
                    device_id_type=pl.DeviceIdType.MESH,
                )
        pl.semaphore_wait(barrier, len(beside) + 1 + inner_chip.astype(jnp.int32))

    pending = []

    def remote(src, dst, send_sem, recv_sem, **where):
        pending.append(
            pltpu.make_async_remote_copy(
                src_ref=src, dst_ref=dst, send_sem=send_sem, recv_sem=recv_sem,
                device_id=where, device_id_type=pl.DeviceIdType.MESH,
            )
        )
        return pending[-1]

    def send(*args, **where):
        copy = remote(*args, **where)
        copy.start()
        return copy

    def line_ref(t, c):
        return proj.at[t, rows_of(place, c) if c < 3 else rows_of(place + half_ring, 2)]

    def line_copy(source, c, step):
        ref = line_ref(source * 2 + core, c)
        return pltpu.make_async_remote_copy(
            src_ref=ref, dst_ref=ref,
            send_sem=line_s.at[source, c, (step + 1) // 2], recv_sem=line_r.at[source, c],
            device_id={"tok": (chip + step + chips) % chips * 2 + core},
            device_id_type=pl.DeviceIdType.MESH,
        )

    def along(source, c, action):
        for step in (-1, 1):
            inside = chip + step <= chips - 1 if step == 1 else chip + step >= 0
            away = source <= chip if step == 1 else source >= chip

            @pl.when(jnp.logical_and(inside, away))
            def _():
                action(line_copy(source, c, step))

    with jax.named_scope("own_wait"):
        own_copies[0].wait()
    for c in chunks:
        along(chip, c, lambda copy: copy.start())
    for copy in own_copies[1:]:
        copy.wait()
    partner_slab = send(proj.at[tok], proj.at[tok], d2d_own.at[0], d2d_own.at[1], tok=partner)
    outer_chip = jnp.minimum(chip, chips - 1 - chip) == 0
    if sizes[2]:
        @pl.when(outer_chip)
        def _():
            along(chip, 3, lambda copy: copy.start())

    order = [tok, partner]
    for k in range(1, chips):
        other = nearest(chip, k, chips)
        order += [other * 2 + core, other * 2 + 1 - core]
    loads = []
    for n, t in enumerate(order):
        start = pl.multiple_of(t * depth, depth)
        loads.append(
            pltpu.make_async_copy(acts_hbm.at[:, pl.ds(start, depth)], acts.at[n], acts_sem.at[n])
        )
        loads[-1].start()

    def multiply(n, first=False):
        product = jnp.dot(acts[n], proj[order[n]], preferred_element_type=F32)
        if first:
            total[...] = product
        else:
            total[...] += product

    def multiply_piece(n, at):
        part = pl.ds(pl.multiple_of(at % sections * piece, piece), piece)
        total[...] += jnp.dot(acts[n, :, part], proj[order[n], part], preferred_element_type=F32)

    with jax.named_scope("mul0"):
        loads[0].wait()
        multiply(0, True)
    with jax.named_scope("mul1"):
        partner_slab.wait_recv()
        loads[1].wait()
        multiply(1)

    split = piece % 128 == 0
    shared = {k: [] for k in range(1, chips)}
    late = {k: [] for k in range(1, chips)}
    ring = {}

    def share(k, ref, opposite=False):
        n = len(shared[k]) + len(late[k])
        copy = remote(ref, ref, d2d_s.at[k - 1, n], d2d_r.at[k - 1, n], tok=partner)
        (late if opposite else shared)[k].append(copy)
        return copy

    def pass_on(k, j, way, c, ref):
        ring[k, j, way, c] = remote(
            ref, ref, ring_s.at[k - 1, j - 1, way, c], ring_r.at[k - 1, j - 1, way, c],
            section=(to_right if way == 0 else to_left),
        )
        return ring[k, j, way, c]

    near = [place]
    for step in range(1, half_ring):
        near += [place + step, place + sections - step]

    first = {}
    for k in range(1, chips):
        for c in chunks:
            ref = line_ref(order[2 * k], c)
            onward = [pass_on(k, 1, way, c, ref) for way in range(2) if half_ring > 1 or way == c]
            first[k, c] = onward + [share(k, ref)]

    def line_event(k, c):
        with jax.named_scope("ev_line_%d_%d" % (k, c)):
            source = order[2 * k] // 2
            line_copy(source, c, 1).wait_recv()
            along(source, c, lambda copy: copy.start())
            for copy in first[k, c]:
                copy.start()

    extras = {}
    if sizes[2]:
        for k in range(1, chips):
            extras[k] = share(k, line_ref(order[2 * k], 3), True)

    def extra_event(k):
        if k in extras:
            with jax.named_scope("ev_extra_%d" % k):
                source = order[2 * k] // 2
                line_copy(source, 3, 1).wait_recv()
                along(source, 3, lambda copy: copy.start())
                extras[k].start()

    early = min(3, chips)

    @pl.when(outer_chip)
    def _():
        for k in range(1, early):
            for c in chunks:
                line_event(k, c)

    @pl.when(jnp.logical_not(outer_chip))
    def _():
        for c in chunks:
            for k in reversed(range(1, early)):
                line_event(k, c)

    for k in range(early, chips):
        for c in chunks:
            line_event(k, c)
    if sizes[2]:
        @pl.when(jnp.logical_not(outer_chip))
        def _():
            along(chip, 3, lambda copy: copy.start())
            extra_event(1)

    for event in gather_plan(half_ring, chips - 1, chunks):
        kind, k = event[:2]
        t = order[2 * k] if k < chips else None
        with jax.named_scope("ev_" + "_".join(str(part) for part in event)):
            if kind == "outer_extra":
                pl.when(outer_chip)(functools.partial(extra_event, k))
            elif kind == "inner_extra":
                pl.when(jnp.logical_not(outer_chip))(functools.partial(extra_event, k))
            elif kind == "ring":
                _, _, j, way, c = event
                ring[k, j, way, c].wait_recv()
                at = place + sections - j if way == 0 else place + j
                ref = proj.at[t, rows_of(at, c)]
                if j + 1 < half_ring:
                    pass_on(k, j + 1, way, c, ref).start()
                share(k, ref, j == half_ring).start()
            elif kind == "relay":
                way = event[2]
                at = place + sections - half_ring + 1 if way == 0 else place + half_ring - 1
                pass_on(k, half_ring, way, way, proj.at[t, rows_of(at, way)]).start()
            elif kind in ("own", "partner"):
                if split:
                    n = 2 * k + (kind == "partner")
                    loads[n].wait()
                    if kind == "partner":
                        for copy in shared[k]:
                            copy.wait_recv()
                    for at in near:
                        multiply_piece(n, at)
            else:
                n = 2 * k + (kind == "partner_far")
                if kind == "partner_far":
                    for copy in late[k] if split else shared[k] + late[k]:
                        copy.wait_recv()
                if split:
                    multiply_piece(n, place + half_ring)
                else:
                    loads[n].wait()
                    multiply(n)

    mean_out[...] = jnp.zeros_like(mean_out)
    for l in range(layers):
        block = total[l * tok_rows : (l + 1) * tok_rows]
        mean = jnp.sum(block, axis=0, keepdims=True) / tok_rows
        mean_out[l : l + 1] = mean
        block = block - mean
        high = block.astype(BF16)
        low = (block - high.astype(F32)).astype(BF16)
        left_op[l, :tok_rows] = high
        left_op[l, tok_rows : 2 * tok_rows] = high
        left_op[l, 2 * tok_rows :] = low
        right_op[l, :tok_rows] = high
        right_op[l, tok_rows : 2 * tok_rows] = low
        right_op[l, 2 * tok_rows :] = high
    mean_copies = []
    for k in range(1, groups):
        mean_copies.append(
            send(mean_out, means.at[k - 1], mean_s.at[k - 1], mean_r.at[k - 1], tok=flip(tok, k, groups))
        )

    low_side = chip < chips // 2
    rank = jnp.where(low_side, chip, chips - 1 - chip)

    def mirror(d):
        return jnp.where(low_side, d, chips - 1 - d)

    pair = {}
    outward = [chips - 1 - d for d in range(chips)]
    for l in range(layers):
        product = lax.dot_general(
            left_op[l], right_op[l], (((0,), (0,)), ((), ())), preferred_element_type=F32
        )
        for t in range(groups):
            gram[t, l] = product[t * slab : (t + 1) * slab]
        for d in outward:
            pair[d, l] = send(
                gram.at[mirror(d) * 2 + 1 - core, l], pair_in.at[d, l], pair_s.at[d, l], pair_r.at[d, l],
                tok=partner,
            )

    def line_sum(d, l, primary):
        upward = low_side if primary else jnp.logical_not(low_side)
        way = jnp.where(upward, 0, 1)
        target = mirror(d)
        return pltpu.make_async_remote_copy(
            src_ref=gram.at[target * 2 + core, l], dst_ref=line_in.at[way, target, l],
            send_sem=gl_s.at[way, target, l], recv_sem=gl_r.at[way, target, l],
            device_id={"tok": jnp.clip(jnp.where(upward, chip + 1, chip - 1), 0, chips - 1) * 2 + core},
            device_id_type=pl.DeviceIdType.MESH,
        )

    def add_pair(d, l):
        pair[d, l].wait_recv()
        mine = mirror(d) * 2 + core
        gram[mine, l] = gram[mine, l] + pair_in[d, l]

    def arrive(d, l, primary):
        upward = low_side if primary else jnp.logical_not(low_side)
        way = jnp.where(upward, 0, 1)
        target = mirror(d)
        line_sum(d, l, primary).wait_recv()
        mine = target * 2 + core
        gram[mine, l] = gram[mine, l] + line_in[way, target, l]

    def arrive_own(l, primary):
        upward = low_side if primary else jnp.logical_not(low_side)
        way = jnp.where(upward, 0, 1)
        pltpu.make_async_remote_copy(
            src_ref=gram.at[tok, l], dst_ref=line_in.at[way, chip, l],
            send_sem=gl_s.at[way, chip, l], recv_sem=gl_r.at[way, chip, l],
            device_id={"tok": partner}, device_id_type=pl.DeviceIdType.MESH,
        ).wait_recv()
        gram[tok, l] = gram[tok, l] + line_in[way, chip, l]

    def forward(d, l, primary):
        @pl.when(d > rank if primary else d < rank)
        def _():
            if primary:
                @pl.when(rank > 0)
                def _():
                    arrive(d, l, primary)
            else:
                arrive(d, l, primary)
            line_sum(d, l, primary).start()

    def correct():
        for copy in mean_copies:
            copy.wait_recv()
        overall = mean_out[...]
        for k in range(1, groups):
            overall = overall + means[k - 1]
        overall = overall / groups
        for l in range(layers):
            shifts = [mean_out[l : l + 1] - overall[l : l + 1]]
            for k in range(1, groups):
                shifts.append(means[k - 1, l : l + 1] - overall[l : l + 1])
            shifts = jnp.concatenate(shifts, axis=0)
            outer = lax.dot_general(
                shifts, shifts * tok_rows, (((0,), (0,)), ((), ())),
                precision=lax.Precision.HIGHEST, preferred_element_type=F32,
            )
            for t in range(groups):
                corr[t, l] = outer[t * slab : (t + 1) * slab]

    steps = []
    for d in range(chips):
        for l in range(layers):
            turn = (chips - 1 - d) * layers + l
            steps.append((turn, 1, d, l))
            if d < chips - 1:
                steps.append((d * layers + l + layers - 0.5, 0, d, l))
    early = True
    for turn, primary, d, l in sorted(steps):
        if turn > layers - 1 and early:
            early = False
            for other in outward[1:]:
                for m in range(layers):
                    add_pair(other, m)
            correct()
        if early:
            add_pair(d, l)
        if d > 0 or not primary:
            forward(d, l, bool(primary))

    edge = None
    for l in range(layers):
        @pl.when(rank > 0)
        def _():
            arrive_own(l, True)

        arrive_own(l, False)
        result = gram[tok, l] + corr[tok, l]
        sketch_ref[l] = result
        if l == 0:
            edge_out[...] = result.astype(BF16)
            edge = send(
                edge_out, edge_in, edge_s, edge_r, section=(section + sections - 1) % sections
            )

    def inner(first, second):
        columns = jnp.sum(first * second, axis=0, keepdims=True)
        lanes = columns[:, :128]
        for start in range(128, width, 128):
            lanes = lanes + columns[:, start : start + 128]
        return lanes

    prod_out[...] = jnp.zeros_like(prod_out)
    own = [sketch_ref[l] for l in range(layers)]
    for l in range(layers):
        prod_out[l : l + 1] = inner(own[l], own[l])
        if l:
            prod_out[layers + l - 1 : layers + l] = inner(own[l - 1], own[l])
    base = 2 * layers - 1
    edge.wait_recv()
    beyond = edge_in[...].astype(F32)
    prod_out[base : base + 1] = inner(own[-1], beyond)
    prod_out[base + 1 : base + 2] = inner(beyond, beyond)
    prod_copies, prev_copies = [], []
    for k in range(groups):
        other = flip(tok, k, groups)
        prev_copies.append(
            send(prod_out, prev_prods.at[k], prev_s.at[k], prev_r.at[k],
                 section=(section + 1) % sections, tok=other)
        )
        if k:
            prod_copies.append(
                send(prod_out, prods.at[k - 1], prod_s.at[k - 1], prod_r.at[k - 1], tok=other)
            )
    products = prod_out[...]
    for k in range(1, groups):
        prod_copies[k - 1].wait_recv()
        products = products + prods[k - 1]
    prev_copies[0].wait_recv()
    earlier = prev_prods[0]
    for k in range(1, groups):
        prev_copies[k].wait_recv()
        earlier = earlier + prev_prods[k]
    products = jnp.broadcast_to(jnp.sum(products, axis=1, keepdims=True), products.shape)
    earlier = jnp.broadcast_to(jnp.sum(earlier, axis=1, keepdims=True), earlier.shape)

    def item(i):
        return products[i : i + 1]

    first, last = section == 0, section == sections - 1
    before = jnp.where(first, item(0), earlier[layers - 1 : layers])
    before_cross = jnp.where(first, item(0), earlier[base : base + 1])
    beyond_square = jnp.where(last, item(layers - 1), item(base + 1))
    beyond_cross = jnp.where(last, item(layers - 1), item(base))
    squares = [before] + [item(l) for l in range(layers)] + [beyond_square]
    chained = [before_cross] + [item(layers + l) for l in range(layers - 1)] + [beyond_cross]
    ratios = [chained[i] / jnp.sqrt(squares[i] * squares[i + 1]) for i in range(layers + 1)]
    sim_ref[...] = jnp.zeros_like(sim_ref)
    lane = lax.broadcasted_iota(jnp.int32, (1, 128), 1)
    for l in range(layers):
        sim_ref[l : l + 1] = jnp.where(lane == 0, ratios[l], ratios[l + 1])

    for copy in pending:
        copy.wait_send()
    for d in range(chips):
        for l in range(layers):
            for primary in (True, False):
                @pl.when(d > rank if primary else d < rank)
                def _():
                    line_sum(d, l, primary).wait_send()
    for source in [chip] + [t // 2 for t in order[2::2]]:
        for c in chunks + ([3] if sizes[2] else []):
            along(source, c, lambda copy: copy.wait_send())


def finish(sketch_in, sim_in, sketch_out, sim_out, sem):
    copy = pltpu.make_async_copy(sketch_in, sketch_out, sem)
    copy.start()
    sim_out[...] = sim_in[: sim_out.shape[0], : sim_out.shape[1]]
    copy.wait()


def local(sections, groups, activations, projection):
    layers, tok_rows, model_width = activations.shape
    depth, width = projection.shape
    rows = layers * tok_rows
    chips, slab = groups // 2, width // groups
    tall = -(-(2 * layers + 3) // 8) * 8
    piece = depth // sections
    share_rows = piece * SHARE // 256 // 16 * 16 if piece % 64 == 0 else piece // 2
    dma = pltpu.SemaphoreType.DMA
    sketch, sim = pl.pallas_call(
        functools.partial(kernel, sections, groups, layers, share_rows),
        out_shape=(pltpu.VMEM((layers, slab, width), F32), pltpu.VMEM((tall, 128), F32)),
        in_specs=[pl.BlockSpec(memory_space=pl.ANY)] * 2,
        out_specs=(pl.BlockSpec(memory_space=pltpu.VMEM),) * 2,
        scratch_shapes=[
            pltpu.VMEM((groups, rows, depth), BF16),
            pltpu.VMEM((groups, depth, width), BF16),
            pltpu.VMEM((rows, width), F32),
            pltpu.VMEM((layers, 3 * tok_rows, width), BF16),
            pltpu.VMEM((layers, 3 * tok_rows, width), BF16),
            pltpu.VMEM((groups, layers, slab, width), F32),
            pltpu.VMEM((chips, layers, slab, width), F32),
            pltpu.VMEM((2, chips, layers, slab, width), F32),
            pltpu.VMEM((tall, width), F32),
            pltpu.VMEM((groups - 1, tall, width), F32),
            pltpu.VMEM((groups, layers, slab, width), F32),
            pltpu.VMEM((slab, width), BF16),
            pltpu.VMEM((slab, width), BF16),
            pltpu.VMEM((tall, 128), F32),
            pltpu.VMEM((groups - 1, tall, 128), F32),
            pltpu.VMEM((groups, tall, 128), F32),
            dma((groups,)), dma((sections,)), dma((2,)),
            dma((chips, 4, 2)), dma((chips, 4)),
            dma((chips - 1, sections // 2, 2, 3)), dma((chips - 1, sections // 2, 2, 3)),
            dma((chips - 1, 3 * sections)), dma((chips - 1, 3 * sections)),
            dma((groups - 1,)), dma((groups - 1,)),
            dma((chips, layers)), dma((chips, layers)),
            dma((2, chips, layers)), dma((2, chips, layers)),
            dma(()), dma(()),
            dma((groups - 1,)), dma((groups - 1,)),
            dma((groups,)), dma((groups,)),
        ],
        compiler_params=pltpu.CompilerParams(
            collective_id=0, has_side_effects=True, vmem_limit_bytes=60 * 1024 * 1024
        ),
    )(activations.reshape(rows, model_width), projection)
    sketch, similarity = pl.pallas_call(
        finish,
        out_shape=(
            jax.ShapeDtypeStruct((layers, slab, width), F32),
            jax.ShapeDtypeStruct((layers, 2), F32),
        ),
        in_specs=[pl.BlockSpec(memory_space=pltpu.VMEM)] * 2,
        out_specs=(pl.BlockSpec(memory_space=pl.ANY), pl.BlockSpec(memory_space=pltpu.VMEM)),
        scratch_shapes=[pltpu.SemaphoreType.DMA(())],
    )(*(pltpu.with_memory_space_constraint(part, pltpu.VMEM) for part in (sketch, sim)))
    return jnp.swapaxes(sketch, 1, 2), similarity


def solution(mesh):
    return jax.shard_map(
        functools.partial(local, mesh.shape["section"], mesh.shape["tok"]),
        mesh=mesh,
        in_specs=(P("section", "tok", None), P("tok", None)),
        out_specs=(P("section", None, "tok"), P("section", None)),
        check_vma=False,
    )
```

```python
import functools
import math

import jax
import jax.numpy as jnp
from jax import lax
from jax.experimental import pallas as pl
from jax.experimental.pallas import tpu as pltpu
from jax.sharding import PartitionSpec as P

F32, BF16 = jnp.float32, jnp.bfloat16
SHARE = 80
TOP = 1400.0


def flip(index, mask, size):
    result, bit = 0, 1
    while bit < size:
        digit = (index // bit) % 2
        result = result + bit * ((1 - digit) if mask & bit else digit)
        bit *= 2
    return result


def nearest(chip, n, chips):
    short = jnp.minimum(chip, chips - 1 - chip)
    low_side = chip < chips // 2
    paired = n <= 2 * short
    distance = jnp.where(paired, (n + 1) // 2, n - short)
    lower = jnp.where(paired, jnp.logical_xor(low_side, n % 2 == 0), jnp.logical_not(low_side))
    return jnp.where(lower, chip - distance, chip + distance)


def snake(place, sections):
    half = sections // 2
    return jnp.where(place < half, place, 3 * half - 1 - place)


def encode(value, bound):
    scaled = value * (TOP / bound)
    square = scaled * scaled
    fourth = square * square
    power = fourth * fourth * fourth
    return jnp.where(scaled < 0, -power, power).astype(BF16)


def decode(code, bound):
    power = code.astype(F32)
    size = jnp.abs(power)
    root = jnp.exp(jnp.log(size) * (1 / 12)) * (bound / TOP)
    root = jnp.where(size > 0, root, 0.0)
    return jnp.where(power < 0, -root, root)


def gather_plan(half_ring, others, chunks):
    def ring(k, j, c):
        return [("ring", k, j, way, c) for way in ((0, 1) if j < half_ring else (c,))]

    def near(k):
        return [event for c in chunks for j in range(1, half_ring) for event in ring(k, j, c)]

    def relay(k):
        return [("relay", k, way) for way in range(2)] if half_ring > 1 else []

    def far(k):
        return ring(k, half_ring, 0) + ring(k, half_ring, 1)

    before = range(1, others)
    order = [event for k in before for event in near(k)]
    order += [event for k in before for event in relay(k)]
    order += [("own", k) for k in before]
    for k in before:
        order += [("partner", k)] + ([("inner_extra", 2)] if k == 1 else [])
    order += [("inner_extra", k) for k in range(3, others + 1)]
    order += near(others) + relay(others)
    order += [("outer_extra", k) for k in (1, 2)]
    order += [("own", others), ("partner", others)]
    for k in before:
        order += far(k)
    order += [("own_far", k) for k in before] + [("partner_far", k) for k in before]
    order += [("outer_extra", k) for k in range(3, others + 1)]
    return order + far(others) + [("own_far", others), ("partner_far", others)]


def kernel(
    sections, groups, layers, share_rows, coded, acts_hbm, proj_hbm, sketch_ref, sim_ref,
    acts, proj, total, left_op, right_op, gram, pair_in, line_in, code_out, mean_out, means, corr,
    shifts_t, bound_out, bound_in, sum_out, sum_in, edge_out, edge_in, prod_out, prods, prev_prods,
    acts_sem, own_sem, d2d_own, line_s, line_r, ring_s, ring_r, d2d_s, d2d_r,
    mean_s, mean_r, bound_sem, sum_s, sum_r, pair_s, pair_r, gl_s, gl_r, edge_s, edge_r, prod_s, prod_r, prev_s, prev_r,
):
    section = lax.axis_index("section")
    tok = lax.axis_index("tok")
    chips = groups // 2
    chip, core = tok // 2, tok % 2
    partner = chip * 2 + 1 - core
    rows = acts.shape[1]
    tok_rows = rows // layers
    depth = proj.shape[1]
    width = proj.shape[2]
    slab = width // groups
    half_ring = sections // 2
    piece = depth // sections
    sizes = (share_rows, share_rows, piece - 2 * share_rows)
    chunks = [c for c in range(3) if sizes[c]]
    align = math.gcd(piece, share_rows)
    place = snake(section, sections)
    to_right = snake((place + 1) % sections, sections)
    to_left = snake((place + sections - 1) % sections, sections)

    def rows_of(at, c):
        start = at % sections * piece + sum(sizes[:c])
        return pl.ds(pl.multiple_of(start, align), sizes[c])

    own_copies = []
    for n in range(sections):
        part = pl.ds(pl.multiple_of((place + n) % sections * piece, piece), piece)
        own_copies.append(
            pltpu.make_async_copy(proj_hbm.at[part], proj.at[tok, part], own_sem.at[n])
        )
        own_copies[-1].start()

    with jax.named_scope("barrier"):
        barrier = pltpu.get_barrier_semaphore()
        beside = [{"tok": partner}, {"section": to_right}]
        if sections > 2:
            beside.append({"section": to_left})
        for where in beside:
            pl.semaphore_signal(
                barrier, inc=1, device_id=where, device_id_type=pl.DeviceIdType.MESH
            )
        inner_chip = jnp.logical_and(chip > 0, chip < chips - 1)
        for step in (-1, 1):
            @pl.when(jnp.logical_and(chip + step >= 0, chip + step <= chips - 1))
            def _():
                pl.semaphore_signal(
                    barrier, inc=1, device_id={"tok": tok + 2 * step},
                    device_id_type=pl.DeviceIdType.MESH,
                )
        pl.semaphore_wait(barrier, len(beside) + 1 + inner_chip.astype(jnp.int32))

    pending = []

    def remote(src, dst, send_sem, recv_sem, **where):
        pending.append(
            pltpu.make_async_remote_copy(
                src_ref=src, dst_ref=dst, send_sem=send_sem, recv_sem=recv_sem,
                device_id=where, device_id_type=pl.DeviceIdType.MESH,
            )
        )
        return pending[-1]

    def send(*args, **where):
        copy = remote(*args, **where)
        copy.start()
        return copy

    def line_ref(t, c):
        return proj.at[t, rows_of(place, c) if c < 3 else rows_of(place + half_ring, 2)]

    def line_copy(source, c, step):
        ref = line_ref(source * 2 + core, c)
        return pltpu.make_async_remote_copy(
            src_ref=ref, dst_ref=ref,
            send_sem=line_s.at[source, c, (step + 1) // 2], recv_sem=line_r.at[source, c],
            device_id={"tok": (chip + step + chips) % chips * 2 + core},
            device_id_type=pl.DeviceIdType.MESH,
        )

    def along(source, c, action):
        for step in (-1, 1):
            inside = chip + step <= chips - 1 if step == 1 else chip + step >= 0
            away = source <= chip if step == 1 else source >= chip

            @pl.when(jnp.logical_and(inside, away))
            def _():
                action(line_copy(source, c, step))

    with jax.named_scope("own_wait"):
        own_copies[0].wait()
    for c in chunks:
        along(chip, c, lambda copy: copy.start())
    for copy in own_copies[1:]:
        copy.wait()
    partner_slab = send(proj.at[tok], proj.at[tok], d2d_own.at[0], d2d_own.at[1], tok=partner)
    outer_chip = jnp.minimum(chip, chips - 1 - chip) == 0
    if sizes[2]:
        @pl.when(outer_chip)
        def _():
            along(chip, 3, lambda copy: copy.start())

    order = [tok, partner]
    for k in range(1, chips):
        other = nearest(chip, k, chips)
        order += [other * 2 + core, other * 2 + 1 - core]
    loads = []
    for n, t in enumerate(order):
        start = pl.multiple_of(t * depth, depth)
        loads.append(
            pltpu.make_async_copy(acts_hbm.at[:, pl.ds(start, depth)], acts.at[n], acts_sem.at[n])
        )
        loads[-1].start()

    def multiply(n, first=False):
        product = jnp.dot(acts[n], proj[order[n]], preferred_element_type=F32)
        if first:
            total[...] = product
        else:
            total[...] += product

    def multiply_piece(n, at):
        part = pl.ds(pl.multiple_of(at % sections * piece, piece), piece)
        total[...] += jnp.dot(acts[n, :, part], proj[order[n], part], preferred_element_type=F32)

    with jax.named_scope("mul0"):
        loads[0].wait()
        multiply(0, True)
    with jax.named_scope("mul1"):
        partner_slab.wait_recv()
        loads[1].wait()
        multiply(1)

    split = piece % 128 == 0
    shared = {k: [] for k in range(1, chips)}
    late = {k: [] for k in range(1, chips)}
    ring = {}

    def share(k, ref, opposite=False):
        n = len(shared[k]) + len(late[k])
        copy = remote(ref, ref, d2d_s.at[k - 1, n], d2d_r.at[k - 1, n], tok=partner)
        (late if opposite else shared)[k].append(copy)
        return copy

    def pass_on(k, j, way, c, ref):
        ring[k, j, way, c] = remote(
            ref, ref, ring_s.at[k - 1, j - 1, way, c], ring_r.at[k - 1, j - 1, way, c],
            section=(to_right if way == 0 else to_left),
        )
        return ring[k, j, way, c]

    near = [place]
    for step in range(1, half_ring):
        near += [place + step, place + sections - step]

    first = {}
    for k in range(1, chips):
        for c in chunks:
            ref = line_ref(order[2 * k], c)
            onward = [pass_on(k, 1, way, c, ref) for way in range(2) if half_ring > 1 or way == c]
            first[k, c] = onward + [share(k, ref)]

    def line_event(k, c):
        with jax.named_scope("ev_line_%d_%d" % (k, c)):
            source = order[2 * k] // 2
            line_copy(source, c, 1).wait_recv()
            along(source, c, lambda copy: copy.start())
            for copy in first[k, c]:
                copy.start()

    extras = {}
    if sizes[2]:
        for k in range(1, chips):
            extras[k] = share(k, line_ref(order[2 * k], 3), True)

    def extra_event(k):
        if k in extras:
            with jax.named_scope("ev_extra_%d" % k):
                source = order[2 * k] // 2
                line_copy(source, 3, 1).wait_recv()
                along(source, 3, lambda copy: copy.start())
                extras[k].start()

    early = min(3, chips)

    @pl.when(outer_chip)
    def _():
        for k in range(1, early):
            for c in chunks:
                line_event(k, c)

    @pl.when(jnp.logical_not(outer_chip))
    def _():
        for c in chunks:
            for k in reversed(range(1, early)):
                line_event(k, c)

    for k in range(early, chips):
        for c in chunks:
            line_event(k, c)
    if sizes[2]:
        @pl.when(jnp.logical_not(outer_chip))
        def _():
            along(chip, 3, lambda copy: copy.start())
            extra_event(1)

    for event in gather_plan(half_ring, chips - 1, chunks):
        kind, k = event[:2]
        t = order[2 * k] if k < chips else None
        with jax.named_scope("ev_" + "_".join(str(part) for part in event)):
            if kind == "outer_extra":
                pl.when(outer_chip)(functools.partial(extra_event, k))
            elif kind == "inner_extra":
                pl.when(jnp.logical_not(outer_chip))(functools.partial(extra_event, k))
            elif kind == "ring":
                _, _, j, way, c = event
                ring[k, j, way, c].wait_recv()
                at = place + sections - j if way == 0 else place + j
                ref = proj.at[t, rows_of(at, c)]
                if j + 1 < half_ring:
                    pass_on(k, j + 1, way, c, ref).start()
                share(k, ref, j == half_ring).start()
            elif kind == "relay":
                way = event[2]
                at = place + sections - half_ring + 1 if way == 0 else place + half_ring - 1
                pass_on(k, half_ring, way, way, proj.at[t, rows_of(at, way)]).start()
            elif kind in ("own", "partner"):
                if split:
                    n = 2 * k + (kind == "partner")
                    loads[n].wait()
                    if kind == "partner":
                        for copy in shared[k]:
                            copy.wait_recv()
                    for at in near:
                        multiply_piece(n, at)
            else:
                n = 2 * k + (kind == "partner_far")
                if kind == "partner_far":
                    for copy in late[k] if split else shared[k] + late[k]:
                        copy.wait_recv()
                if split:
                    multiply_piece(n, place + half_ring)
                else:
                    loads[n].wait()
                    multiply(n)

    with jax.named_scope("center"):
        for l in range(layers):
            block = total[l * tok_rows : (l + 1) * tok_rows]
            mean = jnp.sum(block, axis=0, keepdims=True) / tok_rows
            mean_out[l : l + 1] = mean
            block = block - mean
            high = block.astype(BF16)
            low = (block - high.astype(F32)).astype(BF16)
            left_op[l, :tok_rows] = high
            left_op[l, tok_rows : 2 * tok_rows] = high
            left_op[l, 2 * tok_rows :] = low
            right_op[l, :tok_rows] = high
            right_op[l, tok_rows : 2 * tok_rows] = low
            right_op[l, 2 * tok_rows :] = high
            if coded:
                most = jnp.sum(block * block, axis=0, keepdims=True)
                most = jnp.max(most, axis=1, keepdims=True)
                bound_out[l : l + 1] = jnp.broadcast_to(most, (1, 128))
    if coded:
        bound_pair = send(bound_out, bound_in, bound_sem.at[0], bound_sem.at[1], tok=partner)
    mean_copies = []
    for k in range(1, groups):
        mean_copies.append(
            send(mean_out, means.at[k - 1], mean_s.at[k - 1], mean_r.at[k - 1], tok=flip(tok, k, groups))
        )

    low_side = chip < chips // 2
    rank = jnp.where(low_side, chip, chips - 1 - chip)

    def mirror(d):
        return jnp.where(low_side, d, chips - 1 - d)

    pair = {}
    outward = [chips - 1 - d for d in range(chips)]
    for l in range(layers):
        with jax.named_scope("gram_%d" % l):
            product = lax.dot_general(
                left_op[l], right_op[l], (((0,), (0,)), ((), ())), preferred_element_type=F32
            )
            for t in range(groups):
                gram[t, l] = product[t * slab : (t + 1) * slab]
            for d in outward:
                pair[d, l] = send(
                    gram.at[mirror(d) * 2 + 1 - core, l], pair_in.at[d, l], pair_s.at[d, l],
                    pair_r.at[d, l], tok=partner,
                )

    def heading(primary):
        upward = low_side if primary else jnp.logical_not(low_side)
        way = jnp.where(upward, 0, 1)
        beyond = jnp.clip(jnp.where(upward, chip + 1, chip - 1), 0, chips - 1)
        return way, beyond * 2 + core

    def line_sum(d, l, primary):
        way, beyond = heading(primary)
        target = mirror(d)
        source = code_out.at[target, l] if coded else gram.at[target * 2 + core, l]
        return pltpu.make_async_remote_copy(
            src_ref=source, dst_ref=line_in.at[way, target, l],
            send_sem=gl_s.at[way, target, l], recv_sem=gl_r.at[way, target, l],
            device_id={"tok": beyond}, device_id_type=pl.DeviceIdType.MESH,
        )

    def line_bound(primary):
        way, beyond = heading(primary)
        return pltpu.make_async_remote_copy(
            src_ref=sum_out.at[way], dst_ref=sum_in.at[way],
            send_sem=sum_s.at[way], recv_sem=sum_r.at[way],
            device_id={"tok": beyond}, device_id_type=pl.DeviceIdType.MESH,
        )

    def arrived(d, l, primary):
        way, _ = heading(primary)
        line_sum(d, l, primary).wait_recv()
        value = line_in[way, mirror(d), l]
        return decode(value, sum_in[way, l : l + 1, :1]) if coded else value

    def add_pair(d, l):
        pair[d, l].wait_recv()
        mine = mirror(d) * 2 + core
        gram[mine, l] = gram[mine, l] + pair_in[d, l]

    def forward(d, l, primary):
        @pl.when(d > rank if primary else d < rank)
        def _():
            mine = mirror(d) * 2 + core

            def add_arrived():
                gram[mine, l] = gram[mine, l] + arrived(d, l, primary)

            if primary:
                pl.when(rank > 0)(add_arrived)
            else:
                add_arrived()
            if coded:
                way, _ = heading(primary)
                code_out[mirror(d), l] = encode(gram[mine, l], sum_out[way, l : l + 1, :1])
            line_sum(d, l, primary).start()

    def pass_bound(primary):
        way, _ = heading(primary)
        own_bound = jnp.maximum(bound_out[...] + bound_in[...], 1e-30)

        @pl.when(rank > 0)
        def _():
            line_bound(primary).wait_recv()
            sum_out[way] = sum_in[way] + own_bound
            line_bound(primary).start()

        if primary:
            @pl.when(rank == 0)
            def _():
                sum_out[way] = own_bound
                line_bound(primary).start()

    def correct():
        for copy in mean_copies:
            copy.wait_recv()
        overall = mean_out[...]
        for k in range(1, groups):
            overall = overall + means[k - 1]
        overall = overall / groups
        own_columns = pl.ds(pl.multiple_of(tok * slab, slab), slab)
        for l in range(layers):
            shifts = [mean_out[l : l + 1] - overall[l : l + 1]]
            for k in range(1, groups):
                shifts.append(means[k - 1, l : l + 1] - overall[l : l + 1])
            shifts = jnp.concatenate(shifts, axis=0)
            shifts_t[...] = shifts.T
            corr[l] = jnp.dot(
                shifts_t[own_columns] * tok_rows, shifts,
                precision=lax.Precision.HIGHEST, preferred_element_type=F32,
            )

    steps = []
    for d in range(chips):
        for l in range(layers):
            turn = (chips - 1 - d) * layers + l
            steps.append((turn, 1, d, l))
            if d < chips - 1:
                steps.append((d * layers + l + layers - 0.5, 0, d, l))
    if coded:
        with jax.named_scope("bound1"):
            bound_pair.wait_recv()
            pass_bound(True)
    paired, seen = set(), False
    for _, primary, d, l in sorted(steps):
        with jax.named_scope("st_d%d_l%d_p%d" % (d, l, primary)):
            if coded and not primary and not seen:
                seen = True
                pass_bound(False)
            if (d, l) not in paired:
                paired.add((d, l))
                add_pair(d, l)
            if d > 0 or not primary:
                forward(d, l, bool(primary))
    with jax.named_scope("correct"):
        correct()
    if coded:
        @pl.when(rank == 0)
        def _():
            line_bound(False).wait_recv()

    def arrive_own(l, primary):
        way, _ = heading(primary)
        pltpu.make_async_remote_copy(
            src_ref=code_out.at[chip, l] if coded else gram.at[tok, l], dst_ref=line_in.at[way, chip, l],
            send_sem=gl_s.at[way, chip, l], recv_sem=gl_r.at[way, chip, l],
            device_id={"tok": partner}, device_id_type=pl.DeviceIdType.MESH,
        ).wait_recv()
        value = line_in[way, chip, l]
        if coded:
            value = decode(value, sum_in[way, l : l + 1, :1])
        gram[tok, l] = gram[tok, l] + value

    edge = None
    for l in range(layers):
        with jax.named_scope("own_%d" % l):
            @pl.when(rank > 0)
            def _():
                arrive_own(l, True)

            arrive_own(l, False)
        result = gram[tok, l] + corr[l]
        sketch_ref[l] = result
        if l == 0:
            edge_out[...] = result.astype(BF16)
            edge = send(
                edge_out, edge_in, edge_s, edge_r, section=(section + sections - 1) % sections
            )

    def inner(first, second):
        columns = jnp.sum(first * second, axis=0, keepdims=True)
        lanes = columns[:, :128]
        for start in range(128, width, 128):
            lanes = lanes + columns[:, start : start + 128]
        return lanes

    with jax.named_scope("prods"):
        prod_out[...] = jnp.zeros_like(prod_out)
        own = [sketch_ref[l] for l in range(layers)]
        for l in range(layers):
            prod_out[l : l + 1] = inner(own[l], own[l])
            if l:
                prod_out[layers + l - 1 : layers + l] = inner(own[l - 1], own[l])
    base = 2 * layers - 1
    with jax.named_scope("edge_wait"):
        edge.wait_recv()
    beyond = edge_in[...].astype(F32)
    prod_out[base : base + 1] = inner(own[-1], beyond)
    prod_out[base + 1 : base + 2] = inner(beyond, beyond)
    prod_copies, prev_copies = [], []
    for k in range(groups):
        other = flip(tok, k, groups)
        prev_copies.append(
            send(prod_out, prev_prods.at[k], prev_s.at[k], prev_r.at[k],
                 section=(section + 1) % sections, tok=other)
        )
        if k:
            prod_copies.append(
                send(prod_out, prods.at[k - 1], prod_s.at[k - 1], prod_r.at[k - 1], tok=other)
            )
    with jax.named_scope("prodwait"):
        products = prod_out[...]
        for k in range(1, groups):
            prod_copies[k - 1].wait_recv()
            products = products + prods[k - 1]
        prev_copies[0].wait_recv()
        earlier = prev_prods[0]
        for k in range(1, groups):
            prev_copies[k].wait_recv()
            earlier = earlier + prev_prods[k]
    with jax.named_scope("final"):
        products = jnp.broadcast_to(jnp.sum(products, axis=1, keepdims=True), products.shape)
        earlier = jnp.broadcast_to(jnp.sum(earlier, axis=1, keepdims=True), earlier.shape)

        def item(i):
            return products[i : i + 1]

        first, last = section == 0, section == sections - 1
        before = jnp.where(first, item(0), earlier[layers - 1 : layers])
        before_cross = jnp.where(first, item(0), earlier[base : base + 1])
        beyond_square = jnp.where(last, item(layers - 1), item(base + 1))
        beyond_cross = jnp.where(last, item(layers - 1), item(base))
        squares = [before] + [item(l) for l in range(layers)] + [beyond_square]
        chained = [before_cross] + [item(layers + l) for l in range(layers - 1)] + [beyond_cross]
        ratios = [chained[i] / jnp.sqrt(squares[i] * squares[i + 1]) for i in range(layers + 1)]
        sim_ref[...] = jnp.zeros_like(sim_ref)
        lane = lax.broadcasted_iota(jnp.int32, (1, 128), 1)
        for l in range(layers):
            sim_ref[l : l + 1] = jnp.where(lane == 0, ratios[l], ratios[l + 1])

    with jax.named_scope("sends"):
        for copy in pending:
            copy.wait_send()
        for d in range(chips):
            for l in range(layers):
                for primary in (True, False):
                    @pl.when(d > rank if primary else d < rank)
                    def _():
                        line_sum(d, l, primary).wait_send()
        if coded:
            line_bound(True).wait_send()

            @pl.when(rank > 0)
            def _():
                line_bound(False).wait_send()
        for source in [chip] + [t // 2 for t in order[2::2]]:
            for c in chunks + ([3] if sizes[2] else []):
                along(source, c, lambda copy: copy.wait_send())


def finish(sketch_in, sim_in, sketch_out, sim_out, sem):
    copy = pltpu.make_async_copy(sketch_in, sketch_out, sem)
    copy.start()
    sim_out[...] = sim_in[: sim_out.shape[0], : sim_out.shape[1]]
    copy.wait()


def local(sections, groups, activations, projection):
    layers, tok_rows, model_width = activations.shape
    depth, width = projection.shape
    rows = layers * tok_rows
    chips, slab = groups // 2, width // groups
    tall = -(-(2 * layers + 3) // 8) * 8
    piece = depth // sections
    share_rows = piece * SHARE // 256 // 16 * 16 if piece % 64 == 0 else piece // 2
    coded = chips <= 4
    dma = pltpu.SemaphoreType.DMA
    sketch, sim = pl.pallas_call(
        functools.partial(kernel, sections, groups, layers, share_rows, coded),
        out_shape=(pltpu.VMEM((layers, slab, width), F32), pltpu.VMEM((tall, 128), F32)),
        in_specs=[pl.BlockSpec(memory_space=pl.ANY)] * 2,
        out_specs=(pl.BlockSpec(memory_space=pltpu.VMEM),) * 2,
        scratch_shapes=[
            pltpu.VMEM((groups, rows, depth), BF16),
            pltpu.VMEM((groups, depth, width), BF16),
            pltpu.VMEM((rows, width), F32),
            pltpu.VMEM((layers, 3 * tok_rows, width), BF16),
            pltpu.VMEM((layers, 3 * tok_rows, width), BF16),
            pltpu.VMEM((groups, layers, slab, width), F32),
            pltpu.VMEM((chips, layers, slab, width), F32),
            pltpu.VMEM((2, chips, layers, slab, width), BF16 if coded else F32),
            pltpu.VMEM((chips, layers, slab, width), BF16),
            pltpu.VMEM((layers, width), F32),
            pltpu.VMEM((groups - 1, layers, width), F32),
            pltpu.VMEM((layers, slab, width), F32),
            pltpu.VMEM((width, groups), F32),
            pltpu.VMEM((layers, 128), F32),
            pltpu.VMEM((layers, 128), F32),
            pltpu.VMEM((2, layers, 128), F32),
            pltpu.VMEM((2, layers, 128), F32),
            pltpu.VMEM((slab, width), BF16),
            pltpu.VMEM((slab, width), BF16),
            pltpu.VMEM((tall, 128), F32),
            pltpu.VMEM((groups - 1, tall, 128), F32),
            pltpu.VMEM((groups, tall, 128), F32),
            dma((groups,)), dma((sections,)), dma((2,)),
            dma((chips, 4, 2)), dma((chips, 4)),
            dma((chips - 1, sections // 2, 2, 3)), dma((chips - 1, sections // 2, 2, 3)),
            dma((chips - 1, 3 * sections)), dma((chips - 1, 3 * sections)),
            dma((groups - 1,)), dma((groups - 1,)), dma((2,)), dma((2,)), dma((2,)),
            dma((chips, layers)), dma((chips, layers)),
            dma((2, chips, layers)), dma((2, chips, layers)),
            dma(()), dma(()),
            dma((groups - 1,)), dma((groups - 1,)),
            dma((groups,)), dma((groups,)),
        ],
        compiler_params=pltpu.CompilerParams(
            collective_id=0, has_side_effects=True, vmem_limit_bytes=60 * 1024 * 1024
        ),
    )(activations.reshape(rows, model_width), projection)
    sketch, similarity = pl.pallas_call(
        finish,
        out_shape=(
            jax.ShapeDtypeStruct((layers, slab, width), F32),
            jax.ShapeDtypeStruct((layers, 2), F32),
        ),
        in_specs=[pl.BlockSpec(memory_space=pltpu.VMEM)] * 2,
        out_specs=(pl.BlockSpec(memory_space=pl.ANY), pl.BlockSpec(memory_space=pltpu.VMEM)),
        scratch_shapes=[pltpu.SemaphoreType.DMA(())],
    )(*(pltpu.with_memory_space_constraint(part, pltpu.VMEM) for part in (sketch, sim)))
    return jnp.swapaxes(sketch, 1, 2), similarity


def solution(mesh):
    return jax.shard_map(
        functools.partial(local, mesh.shape["section"], mesh.shape["tok"]),
        mesh=mesh,
        in_specs=(P("section", "tok", None), P("tok", None)),
        out_specs=(P("section", None, "tok"), P("section", None)),
        check_vma=False,
    )
```

```python
import functools
import math

import jax
import jax.numpy as jnp
from jax import lax
from jax.experimental import pallas as pl
from jax.experimental.pallas import tpu as pltpu
from jax.sharding import PartitionSpec as P

F32, BF16 = jnp.float32, jnp.bfloat16
SHARE = 80
TOP = 1400.0


def flip(index, mask, size):
    result, bit = 0, 1
    while bit < size:
        digit = (index // bit) % 2
        result = result + bit * ((1 - digit) if mask & bit else digit)
        bit *= 2
    return result


def nearest(chip, n, chips):
    short = jnp.minimum(chip, chips - 1 - chip)
    low_side = chip < chips // 2
    paired = n <= 2 * short
    distance = jnp.where(paired, (n + 1) // 2, n - short)
    lower = jnp.where(paired, jnp.logical_xor(low_side, n % 2 == 0), jnp.logical_not(low_side))
    return jnp.where(lower, chip - distance, chip + distance)


def snake(place, sections):
    half = sections // 2
    return jnp.where(place < half, place, 3 * half - 1 - place)


def encode(value, bound):
    scaled = value * (TOP / bound)
    square = scaled * scaled
    fourth = square * square
    power = fourth * fourth * fourth
    return jnp.where(scaled < 0, -power, power).astype(BF16)


def decode(code, bound):
    power = code.astype(F32)
    size = jnp.abs(power)
    root = jnp.exp(jnp.log(size) * (1 / 12)) * (bound / TOP)
    root = jnp.where(size > 0, root, 0.0)
    return jnp.where(power < 0, -root, root)


def gather_plan(half_ring, others, chunks):
    def ring(k, j, c):
        return [("ring", k, j, way, c) for way in ((0, 1) if j < half_ring else (c,))]

    def near(k):
        return [event for c in chunks for j in range(1, half_ring) for event in ring(k, j, c)]

    def relay(k):
        return [("relay", k, way) for way in range(2)] if half_ring > 1 else []

    def far(k):
        return ring(k, half_ring, 0) + ring(k, half_ring, 1)

    before = range(1, others)
    order = [event for k in before for event in near(k)]
    order += [event for k in before for event in relay(k)]
    order += [("own", k) for k in before]
    for k in before:
        order += [("partner", k)] + ([("inner_extra", 2)] if k == 1 else [])
    order += [("inner_extra", k) for k in range(3, others + 1)]
    order += near(others) + relay(others)
    order += [("outer_extra", k) for k in (1, 2)]
    order += [("own", others), ("partner", others)]
    for k in before:
        order += far(k)
    order += [("own_far", k) for k in before] + [("partner_far", k) for k in before]
    order += [("outer_extra", k) for k in range(3, others + 1)]
    return order + far(others) + [("own_far", others), ("partner_far", others)]


def kernel(
    sections, groups, layers, share_rows, coded, acts_hbm, proj_hbm, sketch_ref, sim_ref,
    acts, proj, total, left_op, right_op, gram, pair_in, line_in, code_out, mean_out, means, corr,
    shifts_t, edge_out, edge_in, prod_out, prods,
    out_sem, acts_sem, own_sem, slab_r, line_r, ring_r, far_r, d2d_r, mean_r, pair_r, gl_r, edge_r, prod_r,
):
    section = lax.axis_index("section")
    tok = lax.axis_index("tok")
    chips = groups // 2
    chip, core = tok // 2, tok % 2
    partner = chip * 2 + 1 - core
    rows = acts.shape[1]
    tok_rows = rows // layers
    depth = proj.shape[1]
    width = proj.shape[2]
    slab = width // groups
    half_ring = sections // 2
    piece = depth // sections
    sizes = (share_rows, share_rows, piece - 2 * share_rows)
    chunks = [c for c in range(3) if sizes[c]]
    align = math.gcd(piece, share_rows)
    place = snake(section, sections)
    to_right = snake((place + 1) % sections, sections)
    to_left = snake((place + sections - 1) % sections, sections)

    def rows_of(at, c):
        start = at % sections * piece + sum(sizes[:c])
        return pl.ds(pl.multiple_of(start, align), sizes[c])

    for n in range(sections):
        part = pl.ds(pl.multiple_of((place + n) % sections * piece, piece), piece)
        pltpu.make_async_copy(proj_hbm.at[part], proj.at[tok, part], own_sem.at[min(n, 1)]).start()

    def wait_bytes(ref, sem):
        pltpu.make_async_copy(ref, ref, sem).wait()

    with jax.named_scope("barrier"):
        barrier = pltpu.get_barrier_semaphore()
        beside = [{"tok": partner}, {"section": to_right}]
        if sections > 2:
            beside.append({"section": to_left})
        for where in beside:
            pl.semaphore_signal(
                barrier, inc=1, device_id=where, device_id_type=pl.DeviceIdType.MESH
            )
        inner_chip = jnp.logical_and(chip > 0, chip < chips - 1)
        for step in (-1, 1):
            @pl.when(jnp.logical_and(chip + step >= 0, chip + step <= chips - 1))
            def _():
                pl.semaphore_signal(
                    barrier, inc=1, device_id={"tok": tok + 2 * step},
                    device_id_type=pl.DeviceIdType.MESH,
                )
        pl.semaphore_wait(barrier, len(beside) + 1 + inner_chip.astype(jnp.int32))

    pending = []

    def remote(src, dst, recv_sem, **where):
        pending.append(
            pltpu.make_async_remote_copy(
                src_ref=src, dst_ref=dst, send_sem=out_sem, recv_sem=recv_sem,
                device_id=where, device_id_type=pl.DeviceIdType.MESH,
            )
        )
        return pending[-1]

    def send(*args, **where):
        copy = remote(*args, **where)
        copy.start()
        return copy

    def line_ref(t, c):
        return proj.at[t, rows_of(place, c) if c < 3 else rows_of(place + half_ring, 2)]

    def line_copy(source, c, step):
        ref = line_ref(source * 2 + core, c)
        return pltpu.make_async_remote_copy(
            src_ref=ref, dst_ref=ref,
            send_sem=out_sem, recv_sem=line_r.at[source, c],
            device_id={"tok": (chip + step + chips) % chips * 2 + core},
            device_id_type=pl.DeviceIdType.MESH,
        )

    def along(source, c, action):
        for step in (-1, 1):
            inside = chip + step <= chips - 1 if step == 1 else chip + step >= 0
            away = source <= chip if step == 1 else source >= chip

            @pl.when(jnp.logical_and(inside, away))
            def _():
                action(line_copy(source, c, step))

    with jax.named_scope("own_wait"):
        wait_bytes(proj.at[tok, pl.ds(0, piece)], own_sem.at[0])
    for c in chunks:
        along(chip, c, lambda copy: copy.start())
    wait_bytes(proj.at[tok, pl.ds(0, depth - piece)], own_sem.at[1])
    partner_slab = send(proj.at[tok], proj.at[tok], slab_r, tok=partner)
    outer_chip = jnp.minimum(chip, chips - 1 - chip) == 0
    if sizes[2]:
        @pl.when(outer_chip)
        def _():
            along(chip, 3, lambda copy: copy.start())

    order = [tok, partner]
    for k in range(1, chips):
        other = nearest(chip, k, chips)
        order += [other * 2 + core, other * 2 + 1 - core]
    for n, t in enumerate(order):
        start = pl.multiple_of(t * depth, depth)
        pltpu.make_async_copy(
            acts_hbm.at[:, pl.ds(start, depth)], acts.at[n], acts_sem.at[min(n, 2)]
        ).start()
    loaded = []

    def await_acts(n):
        if min(n, 2) not in loaded:
            loaded.append(min(n, 2))
            wait_bytes(acts.at[n] if n < 2 else acts.at[2:], acts_sem.at[min(n, 2)])

    def multiply(n, first=False):
        product = jnp.dot(acts[n], proj[order[n]], preferred_element_type=F32)
        if first:
            total[...] = product
        else:
            total[...] += product

    def multiply_piece(n, at):
        part = pl.ds(pl.multiple_of(at % sections * piece, piece), piece)
        total[...] += jnp.dot(acts[n, :, part], proj[order[n], part], preferred_element_type=F32)

    with jax.named_scope("mul0"):
        await_acts(0)
        multiply(0, True)
    with jax.named_scope("mul1"):
        partner_slab.wait_recv()
        await_acts(1)
        multiply(1)

    split = piece % 128 == 0
    ring = {}

    def share(k, ref, opposite=False):
        return remote(ref, ref, d2d_r.at[k - 1, int(opposite)], tok=partner)

    def await_shares(k, opposite):
        n = piece if opposite else depth - piece
        wait_bytes(proj.at[order[2 * k + 1], pl.ds(0, n)], d2d_r.at[k - 1, int(opposite)])

    def pass_on(k, j, way, c, ref):
        ring[k, j, way, c] = remote(
            ref, ref, ring_r.at[k - 1, j - 1, way, c] if j < half_ring else far_r.at[k - 1, way],
            section=(to_right if way == 0 else to_left),
        )
        return ring[k, j, way, c]

    near = [place]
    for step in range(1, half_ring):
        near += [place + step, place + sections - step]

    first = {}
    for k in range(1, chips):
        for c in chunks:
            ref = line_ref(order[2 * k], c)
            onward = [pass_on(k, 1, way, c, ref) for way in range(2) if half_ring > 1 or way == c]
            first[k, c] = onward + [share(k, ref)]

    def line_event(k, c):
        with jax.named_scope("ev_line_%d_%d" % (k, c)):
            source = order[2 * k] // 2
            line_copy(source, c, 1).wait_recv()
            along(source, c, lambda copy: copy.start())
            for copy in first[k, c]:
                copy.start()

    extras = {}
    if sizes[2]:
        for k in range(1, chips):
            extras[k] = share(k, line_ref(order[2 * k], 3), True)

    def extra_event(k):
        if k in extras:
            with jax.named_scope("ev_extra_%d" % k):
                source = order[2 * k] // 2
                line_copy(source, 3, 1).wait_recv()
                along(source, 3, lambda copy: copy.start())
                extras[k].start()

    early = min(3, chips)

    @pl.when(outer_chip)
    def _():
        for k in range(1, early):
            for c in chunks:
                line_event(k, c)

    @pl.when(jnp.logical_not(outer_chip))
    def _():
        for c in chunks:
            for k in reversed(range(1, early)):
                line_event(k, c)

    for k in range(early, chips):
        for c in chunks:
            line_event(k, c)
    if sizes[2]:
        @pl.when(jnp.logical_not(outer_chip))
        def _():
            along(chip, 3, lambda copy: copy.start())
            extra_event(1)

    for event in gather_plan(half_ring, chips - 1, chunks):
        kind, k = event[:2]
        t = order[2 * k] if k < chips else None
        with jax.named_scope("ev_" + "_".join(str(part) for part in event)):
            if kind == "outer_extra":
                pl.when(outer_chip)(functools.partial(extra_event, k))
            elif kind == "inner_extra":
                pl.when(jnp.logical_not(outer_chip))(functools.partial(extra_event, k))
            elif kind == "ring":
                _, _, j, way, c = event
                ring[k, j, way, c].wait_recv()
                at = place + sections - j if way == 0 else place + j
                ref = proj.at[t, rows_of(at, c)]
                if j + 1 < half_ring:
                    pass_on(k, j + 1, way, c, ref).start()
                share(k, ref, j == half_ring).start()
            elif kind == "relay":
                way = event[2]
                at = place + sections - half_ring + 1 if way == 0 else place + half_ring - 1
                pass_on(k, half_ring, way, way, proj.at[t, rows_of(at, way)]).start()
            elif kind in ("own", "partner"):
                if split:
                    n = 2 * k + (kind == "partner")
                    await_acts(n)
                    if kind == "partner":
                        await_shares(k, False)
                    for at in near:
                        multiply_piece(n, at)
            else:
                n = 2 * k + (kind == "partner_far")
                if kind == "partner_far":
                    if not split:
                        await_shares(k, False)
                    await_shares(k, True)
                if split:
                    multiply_piece(n, place + half_ring)
                else:
                    await_acts(n)
                    multiply(n)

    with jax.named_scope("center"):
        for l in range(layers):
            block = total[l * tok_rows : (l + 1) * tok_rows]
            mean = jnp.sum(block, axis=0, keepdims=True) / tok_rows
            mean_out[l : l + 1, :width] = mean
            block = block - mean
            high = block.astype(BF16)
            low = (block - high.astype(F32)).astype(BF16)
            left_op[l, :tok_rows] = high
            left_op[l, tok_rows : 2 * tok_rows] = high
            left_op[l, 2 * tok_rows :] = low
            right_op[l, :tok_rows] = high
            right_op[l, tok_rows : 2 * tok_rows] = low
            right_op[l, 2 * tok_rows :] = high
            most = jnp.sum(block * block, axis=0, keepdims=True)
            most = jnp.max(most, axis=1, keepdims=True)
            mean_out[l : l + 1, width:] = jnp.broadcast_to(most, (1, 128))
    for k in range(1, groups):
        send(mean_out, means.at[k - 1], mean_r.at[k.bit_length() - 1], tok=flip(tok, k, groups))

    low_side = chip < chips // 2
    rank = jnp.where(low_side, chip, chips - 1 - chip)

    def mirror(d):
        return jnp.where(low_side, d, chips - 1 - d)

    pair = {}
    outward = [chips - 1 - d for d in range(chips)]
    for l in range(layers):
        with jax.named_scope("gram_%d" % l):
            product = lax.dot_general(
                left_op[l], right_op[l], (((0,), (0,)), ((), ())), preferred_element_type=F32
            )
            for t in range(groups):
                gram[t, l] = product[t * slab : (t + 1) * slab]
            for d in outward:
                pair[d, l] = send(
                    gram.at[mirror(d) * 2 + 1 - core, l], pair_in.at[d, l], pair_r.at[d, l], tok=partner
                )

    def add_pair(d, l):
        pair[d, l].wait_recv()
        mine = mirror(d) * 2 + core
        gram[mine, l] = gram[mine, l] + pair_in[d, l]

    def correct():
        overall = mean_out[:, :width]
        for k in range(1, groups):
            overall = overall + means[k - 1, :, :width]
        overall = overall / groups
        own_columns = pl.ds(pl.multiple_of(tok * slab, slab), slab)
        for l in range(layers):
            shifts = [mean_out[l : l + 1, :width] - overall[l : l + 1]]
            for k in range(1, groups):
                shifts.append(means[k - 1, l : l + 1, :width] - overall[l : l + 1])
            shifts = jnp.concatenate(shifts, axis=0)
            shifts_t[...] = shifts.T
            corr[l] = jnp.dot(
                shifts_t[own_columns] * tok_rows, shifts,
                precision=lax.Precision.HIGHEST, preferred_element_type=F32,
            )

    def await_means(bit):
        wait_bytes(means.at[2**bit - 1 : 2 ** (bit + 1) - 1], mean_r.at[bit])

    bits = range(1, groups.bit_length() - 1)
    if coded:
        def bound(l, *masks):
            total_bound = None
            for mask in masks:
                same = means[2 * mask - 1] if mask else mean_out
                both = same[l : l + 1, width:] + means[2 * mask, l : l + 1, width:]
                total_bound = both if total_bound is None else total_bound + both
            return jnp.maximum(total_bound[:, :1], 1e-30)

        def paired(d, l):
            pair[d, l].wait_recv()
            return gram[mirror(d) * 2 + core, l] + pair_in[d, l]

        def box(d, l, beyond, slot):
            return pltpu.make_async_remote_copy(
                src_ref=code_out.at[d, l], dst_ref=line_in.at[slot, l], send_sem=out_sem,
                recv_sem=gl_r.at[slot, l], device_id={"tok": mirror(beyond) * 2 + core},
                device_id_type=pl.DeviceIdType.MESH,
            )

        def post(d, l, beyond, slot, *masks, value=None):
            code_out[d, l] = encode(paired(d, l) if value is None else value, bound(l, *masks))
            box(d, l, beyond, slot).start()

        def unbox(l, slot, *masks):
            wait_bytes(line_in.at[slot, l], gl_r.at[slot, l])
            return decode(line_in[slot, l], bound(l, *masks))

        far_end = chips - 1
        with jax.named_scope("bound"):
            await_means(0)

        @pl.when(rank == 0)
        def _():
            with jax.named_scope("post"):
                for l in range(layers):
                    post(far_end, l, 1, 0, 0)
                post(2, 0, 2, 3, 0)
                for l in range(layers):
                    if l:
                        post(2, l, 2, 3, 0)
                    post(1, l, 1, 1, 0)
            await_means(1)

        @pl.when(rank == 1)
        def _():
            with jax.named_scope("post"):
                for l in range(layers):
                    post(2, l, 2, 2, 0)
                    post(0, l, 0, 1, 0)
            await_means(1)
            with jax.named_scope("relay"):
                for l in range(layers):
                    value = paired(far_end, l)
                    post(far_end, l, far_end, 2, 0, 1, value=value + unbox(l, 0, 1))

        for bit in bits[1:]:
            await_means(bit)
        with jax.named_scope("correct"):
            correct()

        def finish_sum(l):
            if l is None:
                for _ in range(3 * layers):
                    wait_bytes(code_out.at[0, 0], out_sem)
                return

            @pl.when(rank == 0)
            def _():
                value = paired(0, l) + unbox(l, 1, 1)
                gram[tok, l] = value + unbox(l, 2, 2, 3)

            @pl.when(rank == 1)
            def _():
                value = paired(1, l) + unbox(l, 3, 2)
                value = value + unbox(l, 2, 3)
                gram[tok, l] = value + unbox(l, 1, 1)

    else:
        def line_sum(d, l, primary):
            upward = low_side if primary else jnp.logical_not(low_side)
            way = jnp.where(upward, 0, 1)
            target = mirror(d)
            beyond = jnp.clip(jnp.where(upward, chip + 1, chip - 1), 0, chips - 1)
            return way, pltpu.make_async_remote_copy(
                src_ref=gram.at[target * 2 + core, l], dst_ref=line_in.at[way, target, l],
                send_sem=out_sem, recv_sem=gl_r.at[way, target, l],
                device_id={"tok": beyond * 2 + core}, device_id_type=pl.DeviceIdType.MESH,
            )

        def arrive(d, l, primary):
            way, copy = line_sum(d, l, primary)
            copy.wait_recv()
            mine = mirror(d) * 2 + core
            gram[mine, l] = gram[mine, l] + line_in[way, mirror(d), l]

        def forward(d, l, primary):
            @pl.when(d > rank if primary else d < rank)
            def _():
                if primary:
                    pl.when(rank > 0)(functools.partial(arrive, d, l, True))
                else:
                    arrive(d, l, False)
                line_sum(d, l, primary)[1].start()

        steps = []
        for d in range(chips):
            for l in range(layers):
                steps.append(((chips - 1 - d) * layers + l, True, d, l))
                if d < chips - 1:
                    steps.append((d * layers + l + layers - 0.5, False, d, l))
        seen = set()
        for _, primary, d, l in sorted(steps):
            if (d, l) not in seen:
                seen.add((d, l))
                add_pair(d, l)
            if d > 0 or not primary:
                forward(d, l, primary)
        for bit in range(groups.bit_length() - 1):
            await_means(bit)
        correct()

        def finish_sum(l):
            if l is None:
                for d in range(chips):
                    for m in range(layers):
                        for primary in (True, False):
                            @pl.when(d > rank if primary else d < rank)
                            def _():
                                line_sum(d, m, primary)[1].wait_send()
                return

            for primary in (True, False):
                @pl.when(jnp.logical_or(rank > 0, not primary))
                def _():
                    upward = low_side if primary else jnp.logical_not(low_side)
                    way = jnp.where(upward, 0, 1)
                    wait_bytes(line_in.at[way, chip, l], gl_r.at[way, chip, l])
                    gram[tok, l] = gram[tok, l] + line_in[way, chip, l]

    edge = None
    for l in range(layers):
        with jax.named_scope("own_%d" % l):
            finish_sum(l)
        result = gram[tok, l] + corr[l]
        sketch_ref[l] = result
        if l == 0:
            edge_out[...] = result.astype(BF16)
            edge = send(
                edge_out, edge_in, edge_r, section=(section + sections - 1) % sections
            )

    lane = lax.broadcasted_iota(jnp.int32, (1, 128), 1)

    def inner(first, second):
        columns = jnp.sum(first * second, axis=0, keepdims=True)
        return jnp.sum(columns, axis=1, keepdims=True)

    with jax.named_scope("prods"):
        own = [sketch_ref[l] for l in range(layers)]
        terms = [inner(own[l], own[l]) for l in range(layers)]
        terms += [inner(own[l - 1], own[l]) for l in range(1, layers)]
        row = jnp.zeros((1, 128), F32)
        for i, term in enumerate(terms):
            row = jnp.where(lane == i, term, row)
    base = 2 * layers - 1
    with jax.named_scope("edge_wait"):
        edge.wait_recv()
    beyond = edge_in[...].astype(F32)
    row = jnp.where(lane == base, inner(own[-1], beyond), row)
    prod_out[...] = jnp.where(lane == base + 1, inner(beyond, beyond), row)
    for k in range(groups):
        other = flip(tok, k, groups)
        send(prod_out, prods.at[1, k], prod_r.at[1], section=(section + 1) % sections, tok=other)
        if k:
            send(prod_out, prods.at[0, k], prod_r.at[0], tok=other)
    with jax.named_scope("prodwait"):
        wait_bytes(prods.at[0, 1:], prod_r.at[0])
        products = prod_out[...]
        for k in range(1, groups):
            products = products + prods[0, k]
        wait_bytes(prods.at[1], prod_r.at[1])
        earlier = prods[1, 0]
        for k in range(1, groups):
            earlier = earlier + prods[1, k]
    with jax.named_scope("final"):
        def item(i, values=products):
            return jnp.sum(jnp.where(lane == i, values, 0.0), axis=1, keepdims=True)

        first, last = section == 0, section == sections - 1
        before = jnp.where(first, item(0), item(layers - 1, earlier))
        before_cross = jnp.where(first, item(0), item(base, earlier))
        beyond_square = jnp.where(last, item(layers - 1), item(base + 1))
        beyond_cross = jnp.where(last, item(layers - 1), item(base))
        squares = [before] + [item(l) for l in range(layers)] + [beyond_square]
        chained = [before_cross] + [item(layers + l) for l in range(layers - 1)] + [beyond_cross]
        ratios = [chained[i] / jnp.sqrt(squares[i] * squares[i + 1]) for i in range(layers + 1)]
        sim_ref[...] = jnp.zeros_like(sim_ref)
        for l in range(layers):
            sim_ref[l : l + 1] = jnp.where(lane == 0, ratios[l], ratios[l + 1])

    with jax.named_scope("sends"):
        for copy in pending:
            copy.wait_send()
        finish_sum(None)
        for source in [chip] + [t // 2 for t in order[2::2]]:
            for c in chunks + ([3] if sizes[2] else []):
                along(source, c, lambda copy: copy.wait_send())


def finish(sketch_in, sim_in, sketch_out, sim_out, sem):
    copy = pltpu.make_async_copy(sketch_in, sketch_out, sem)
    copy.start()
    sim_out[...] = sim_in[: sim_out.shape[0], : sim_out.shape[1]]
    copy.wait()


def local(sections, groups, activations, projection):
    layers, tok_rows, model_width = activations.shape
    depth, width = projection.shape
    rows = layers * tok_rows
    chips, slab = groups // 2, width // groups
    tall = -(-(2 * layers + 3) // 8) * 8
    piece = depth // sections
    share_rows = piece * SHARE // 256 // 16 * 16 if piece % 64 == 0 else piece // 2
    coded = chips == 4
    dma = pltpu.SemaphoreType.DMA
    sketch, sim = pl.pallas_call(
        functools.partial(kernel, sections, groups, layers, share_rows, coded),
        out_shape=(pltpu.VMEM((layers, slab, width), F32), pltpu.VMEM((tall, 128), F32)),
        in_specs=[pl.BlockSpec(memory_space=pl.ANY)] * 2,
        out_specs=(pl.BlockSpec(memory_space=pltpu.VMEM),) * 2,
        scratch_shapes=[
            pltpu.VMEM((groups, rows, depth), BF16),
            pltpu.VMEM((groups, depth, width), BF16),
            pltpu.VMEM((rows, width), F32),
            pltpu.VMEM((layers, 3 * tok_rows, width), BF16),
            pltpu.VMEM((layers, 3 * tok_rows, width), BF16),
            pltpu.VMEM((groups, layers, slab, width), F32),
            pltpu.VMEM((chips, layers, slab, width), F32),
            pltpu.VMEM((4, layers, slab, width), BF16) if coded
            else pltpu.VMEM((2, chips, layers, slab, width), F32),
            pltpu.VMEM((chips, layers, slab, width), BF16),
            pltpu.VMEM((layers, width + 128), F32),
            pltpu.VMEM((groups - 1, layers, width + 128), F32),
            pltpu.VMEM((layers, slab, width), F32),
            pltpu.VMEM((width, groups), F32),
            pltpu.VMEM((slab, width), BF16),
            pltpu.VMEM((slab, width), BF16),
            pltpu.VMEM((1, 128), F32),
            pltpu.VMEM((2, groups, 1, 128), F32),
            dma(()), dma((3,)), dma((2,)), dma(()),
            dma((chips, 4)), dma((chips - 1, max(sections // 2 - 1, 1), 2, 3)), dma((chips - 1, 2)),
            dma((chips - 1, 2)), dma((groups.bit_length() - 1,)), dma((chips, layers)),
            dma((4, layers)) if coded else dma((2, chips, layers)), dma(()), dma((2,)),
        ],
        compiler_params=pltpu.CompilerParams(
            collective_id=0, has_side_effects=True, vmem_limit_bytes=60 * 1024 * 1024
        ),
    )(activations.reshape(rows, model_width), projection)
    sketch, similarity = pl.pallas_call(
        finish,
        out_shape=(
            jax.ShapeDtypeStruct((layers, slab, width), F32),
            jax.ShapeDtypeStruct((layers, 2), F32),
        ),
        in_specs=[pl.BlockSpec(memory_space=pltpu.VMEM)] * 2,
        out_specs=(pl.BlockSpec(memory_space=pl.ANY), pl.BlockSpec(memory_space=pltpu.VMEM)),
        scratch_shapes=[pltpu.SemaphoreType.DMA(())],
    )(*(pltpu.with_memory_space_constraint(part, pltpu.VMEM) for part in (sketch, sim)))
    return jnp.swapaxes(sketch, 1, 2), similarity


def solution(mesh):
    return jax.shard_map(
        functools.partial(local, mesh.shape["section"], mesh.shape["tok"]),
        mesh=mesh,
        in_specs=(P("section", "tok", None), P("tok", None)),
        out_specs=(P("section", None, "tok"), P("section", None)),
        check_vma=False,
    )
```

```python
import functools
import math

import jax
import jax.numpy as jnp
from jax import lax
from jax.experimental import pallas as pl
from jax.experimental.pallas import tpu as pltpu
from jax.sharding import PartitionSpec as P

F32, BF16 = jnp.float32, jnp.bfloat16
SHARE = 64
FIRST = 32
TOP = 1400.0


def flip(index, mask, size):
    result, bit = 0, 1
    while bit < size:
        digit = (index // bit) % 2
        result = result + bit * ((1 - digit) if mask & bit else digit)
        bit *= 2
    return result


def nearest(chip, n, chips):
    short = jnp.minimum(chip, chips - 1 - chip)
    low_side = chip < chips // 2
    paired = n <= 2 * short
    distance = jnp.where(paired, (n + 1) // 2, n - short)
    lower = jnp.where(paired, jnp.logical_xor(low_side, n % 2 == 0), jnp.logical_not(low_side))
    return jnp.where(lower, chip - distance, chip + distance)


def snake(place, sections):
    half = sections // 2
    return jnp.where(place < half, place, 3 * half - 1 - place)


def encode(value, bound):
    scaled = value * (TOP / bound)
    square = scaled * scaled
    fourth = square * square
    power = fourth * fourth * fourth
    return jnp.where(scaled < 0, -power, power).astype(BF16)


def decode(code, bound):
    power = code.astype(F32)
    size = jnp.abs(power)
    root = jnp.exp(jnp.log(size) * (1 / 12)) * (bound / TOP)
    root = jnp.where(size > 0, root, 0.0)
    return jnp.where(power < 0, -root, root)


def gather_plan(half_ring, others, relayed, extra):
    def near(k):
        return [("near", k, j, g) for g in range(2 if extra else 1) for j in range(1, half_ring)]

    def relay(k):
        return [("relay", k)] if half_ring > 1 else []

    before = range(1, others)
    order = [("inner_first",)] if others > 1 else []
    order += [event for k in before if k > 1 for event in near(k)]
    order += [event for k in before if k > 1 for event in relay(k)]
    order += [("own", k) for k in before]
    for k in before:
        order += [("partner", k)] + ([("inner_extra", 2)] if k == 1 else [])
    order += [("inner_extra", k) for k in range(3, others + 1)]
    last_near = near(others)
    order += last_near[: half_ring - 1] + relay(others)
    order += [("outer_extra", 1)] + last_near[half_ring - 1 :]
    order += [("far", k) for k in before] + [("outer_extra", 2), ("own", others)]
    order += [("own_far", k) for k in before] + [("partner", others), ("far", others)]
    order += [("outer_extra", k) for k in range(3, others + 1)]
    order += [("partner_far", k) for k in before]
    return [event for event in order if extra or "extra" not in event[0]]


def kernel(
    sections, groups, layers, parts, coded, acts_hbm, proj_hbm, sketch_ref, sim_ref,
    acts, proj, total, left_op, right_op, gram, pair_in, line_in, code_out, mean_out, means, corr,
    shifts_t, edge_out, edge_in, prod_out, prods,
    out_sem, acts_sem, own_sem, slab_r, line_r, ring_r, d2d_r, mean_r, pair_r, gl_r, edge_r, prod_r,
):
    section = lax.axis_index("section")
    tok = lax.axis_index("tok")
    chips = groups // 2
    chip, core = tok // 2, tok % 2
    partner = chip * 2 + 1 - core
    rows = acts.shape[1]
    tok_rows = rows // layers
    depth = proj.shape[1]
    width = proj.shape[2]
    slab = width // groups
    half_ring = sections // 2
    piece = depth // sections
    sizes = [size for size, _ in parts]
    chunks = range(len(parts))
    relayed = [c for c in chunks if parts[c][1] is not None]
    extra = len(parts) if len(relayed) < len(parts) else None
    align = math.gcd(piece, *sizes)
    place = snake(section, sections)
    to_right = snake((place + 1) % sections, sections)
    to_left = snake((place + sections - 1) % sections, sections)

    def rows_of(at, c):
        start = at % sections * piece + sum(sizes[:c])
        return pl.ds(pl.multiple_of(start, align), sizes[c])

    for n in range(sections):
        part = pl.ds(pl.multiple_of((place + n) % sections * piece, piece), piece)
        pltpu.make_async_copy(proj_hbm.at[part], proj.at[tok, part], own_sem.at[min(n, 1)]).start()

    def wait_bytes(ref, sem):
        pltpu.make_async_copy(ref, ref, sem).wait()

    with jax.named_scope("barrier"):
        barrier = pltpu.get_barrier_semaphore()
        beside = [{"tok": partner}, {"section": to_right}]
        if sections > 2:
            beside.append({"section": to_left})
        for where in beside:
            pl.semaphore_signal(
                barrier, inc=1, device_id=where, device_id_type=pl.DeviceIdType.MESH
            )
        inner_chip = jnp.logical_and(chip > 0, chip < chips - 1)
        for step in (-1, 1):
            @pl.when(jnp.logical_and(chip + step >= 0, chip + step <= chips - 1))
            def _():
                pl.semaphore_signal(
                    barrier, inc=1, device_id={"tok": tok + 2 * step},
                    device_id_type=pl.DeviceIdType.MESH,
                )
        pl.semaphore_wait(barrier, len(beside) + 1 + inner_chip.astype(jnp.int32))

    pending = []

    def remote(src, dst, recv_sem, **where):
        pending.append(
            pltpu.make_async_remote_copy(
                src_ref=src, dst_ref=dst, send_sem=out_sem, recv_sem=recv_sem,
                device_id=where, device_id_type=pl.DeviceIdType.MESH,
            )
        )
        return pending[-1]

    def send(*args, **where):
        copy = remote(*args, **where)
        copy.start()
        return copy

    def line_ref(t, c):
        return proj.at[t, rows_of(place + half_ring, c - 1) if c == extra else rows_of(place, c)]

    def line_copy(source, c, step):
        ref = line_ref(source * 2 + core, c)
        return pltpu.make_async_remote_copy(
            src_ref=ref, dst_ref=ref,
            send_sem=out_sem, recv_sem=line_r.at[source, c],
            device_id={"tok": (chip + step + chips) % chips * 2 + core},
            device_id_type=pl.DeviceIdType.MESH,
        )

    def along(source, c, action):
        for step in (-1, 1):
            inside = chip + step <= chips - 1 if step == 1 else chip + step >= 0
            away = source <= chip if step == 1 else source >= chip

            @pl.when(jnp.logical_and(inside, away))
            def _():
                action(line_copy(source, c, step))

    with jax.named_scope("own_wait"):
        wait_bytes(proj.at[tok, pl.ds(0, piece)], own_sem.at[0])
    for c in chunks:
        along(chip, c, lambda copy: copy.start())
    wait_bytes(proj.at[tok, pl.ds(0, depth - piece)], own_sem.at[1])
    partner_slab = send(proj.at[tok], proj.at[tok], slab_r, tok=partner)
    outer_chip = jnp.minimum(chip, chips - 1 - chip) == 0
    if extra:
        @pl.when(outer_chip)
        def _():
            along(chip, extra, lambda copy: copy.start())

    order = [tok, partner]
    for k in range(1, chips):
        other = nearest(chip, k, chips)
        order += [other * 2 + core, other * 2 + 1 - core]
    for n, t in enumerate(order):
        start = pl.multiple_of(t * depth, depth)
        pltpu.make_async_copy(
            acts_hbm.at[:, pl.ds(start, depth)], acts.at[n], acts_sem.at[min(n, 2)]
        ).start()
    loaded = []

    def await_acts(n):
        if min(n, 2) not in loaded:
            loaded.append(min(n, 2))
            wait_bytes(acts.at[n] if n < 2 else acts.at[2:], acts_sem.at[min(n, 2)])

    def multiply(n, first=False):
        product = jnp.dot(acts[n], proj[order[n]], preferred_element_type=F32)
        if first:
            total[...] = product
        else:
            total[...] += product

    def multiply_piece(n, at):
        part = pl.ds(pl.multiple_of(at % sections * piece, piece), piece)
        total[...] += jnp.dot(acts[n, :, part], proj[order[n], part], preferred_element_type=F32)

    with jax.named_scope("mul0"):
        await_acts(0)
        multiply(0, True)
    with jax.named_scope("mul1"):
        partner_slab.wait_recv()
        await_acts(1)
        multiply(1)

    split = piece % 128 == 0

    def share(k, ref, opposite=False):
        return remote(ref, ref, d2d_r.at[k - 1, int(opposite)], tok=partner)

    def await_shares(k, opposite):
        n = piece if opposite else depth - piece
        wait_bytes(proj.at[order[2 * k + 1], pl.ds(0, n)], d2d_r.at[k - 1, int(opposite)])

    def pass_on(k, j, way, g, ref):
        return remote(
            ref, ref, ring_r.at[k - 1, j - 1, g], section=(to_right if way == 0 else to_left)
        )

    relayed_rows = sum(sizes[c] for c in relayed)
    spans = [(0, relayed_rows)] + ([(relayed_rows, piece - relayed_rows)] if extra else [])

    near = [place]
    for step in range(1, half_ring):
        near += [place + step, place + sections - step]

    first = {}
    for k in range(1, chips):
        for c in chunks:
            ref = line_ref(order[2 * k], c)
            ways = [way for way in range(2) if half_ring > 1 or way == parts[c][1]]
            first[k, c] = [pass_on(k, 1, way, int(c not in relayed), ref) for way in ways] + [share(k, ref)]

    def line_event(k, c):
        with jax.named_scope("ev_line_%d_%d" % (k, c)):
            source = order[2 * k] // 2
            line_copy(source, c, 1).wait_recv()
            along(source, c, lambda copy: copy.start())
            for copy in first[k, c]:
                copy.start()

    nears, relays = {}, {}
    for k in range(1, chips):
        t = order[2 * k]
        for j in range(1, half_ring):
            for g, (start, n) in enumerate(spans):
                nears[k, j, g] = []
                for way in range(2):
                    at = (place + sections - j if way == 0 else place + j) % sections * piece
                    ref = proj.at[t, pl.ds(pl.multiple_of(at + start, align), n)]
                    if j + 1 < half_ring:
                        nears[k, j, g].append(pass_on(k, j + 1, way, g, ref))
                    nears[k, j, g].append(share(k, ref))
        relays[k] = []
        for c in relayed if half_ring > 1 else []:
            way = parts[c][1]
            at = place + sections - half_ring + 1 if way == 0 else place + half_ring - 1
            relays[k].append(pass_on(k, half_ring, way, 0, proj.at[t, rows_of(at, c)]))

    def near_event(k, j, g):
        with jax.named_scope("ev_near_%d_%d_%d" % (k, j, g)):
            wait_bytes(proj.at[order[2 * k], pl.ds(0, 2 * spans[g][1])], ring_r.at[k - 1, j - 1, g])
            for copy in nears[k, j, g]:
                copy.start()

    def relay_event(k):
        for copy in relays[k]:
            copy.start()

    def first_near():
        for j in range(1, half_ring):
            for g in range(len(spans)):
                near_event(1, j, g)
        relay_event(1)

    extras = {}
    if extra:
        for k in range(1, chips):
            extras[k] = share(k, line_ref(order[2 * k], extra), True)

    def extra_event(k):
        if k in extras:
            with jax.named_scope("ev_extra_%d" % k):
                source = order[2 * k] // 2
                line_copy(source, extra, 1).wait_recv()
                along(source, extra, lambda copy: copy.start())
                extras[k].start()

    early = min(3, chips)

    @pl.when(outer_chip)
    def _():
        for k in range(1, early):
            for c in chunks:
                line_event(k, c)
        if chips > 2:
            first_near()

    @pl.when(jnp.logical_not(outer_chip))
    def _():
        for c in chunks:
            for k in reversed(range(1, early)):
                line_event(k, c)

    for k in range(early, chips):
        for c in chunks:
            line_event(k, c)
    if extra:
        @pl.when(jnp.logical_not(outer_chip))
        def _():
            along(chip, extra, lambda copy: copy.start())
            extra_event(1)

    def finish_block(k, from_partner):
        n = 2 * k + from_partner
        if from_partner:
            if not split:
                await_shares(k, False)
            await_shares(k, True)
        if split:
            multiply_piece(n, place + half_ring)
        else:
            await_acts(n)
            multiply(n)

    for event in gather_plan(half_ring, chips - 1, relayed, extra):
        kind = event[0]
        if kind == "inner_first":
            pl.when(jnp.logical_not(outer_chip))(first_near)
            continue
        k = event[1]
        t = order[2 * k] if k < chips else None
        with jax.named_scope("ev_" + "_".join(str(part) for part in event)):
            if kind == "outer_extra":
                pl.when(outer_chip)(functools.partial(extra_event, k))
            elif kind == "inner_extra":
                pl.when(jnp.logical_not(outer_chip))(functools.partial(extra_event, k))
            elif kind == "near":
                near_event(*event[1:])
            elif kind == "relay":
                relay_event(k)
            elif kind == "far":
                wait_bytes(proj.at[t, pl.ds(0, relayed_rows)], ring_r.at[k - 1, half_ring - 1, 0])
                start = (place + half_ring) % sections * piece
                share(k, proj.at[t, pl.ds(pl.multiple_of(start, piece), relayed_rows)], True).start()
            elif kind in ("own", "partner"):
                if split:
                    n = 2 * k + (kind == "partner")
                    await_acts(n)
                    if kind == "partner":
                        await_shares(k, False)
                    for at in near:
                        multiply_piece(n, at)
            else:
                finish_block(k, kind == "partner_far")

    low_side = chip < chips // 2
    rank = jnp.where(low_side, chip, chips - 1 - chip)

    def mirror(d):
        return jnp.where(low_side, d, chips - 1 - d)

    pair = {}
    outward = [chips - 1 - d for d in range(chips)]
    with jax.named_scope("own_end"):
        finish_block(chips - 1, 0)
        finish_block(chips - 1, 1)
    with jax.named_scope("center"):
        for l in range(layers):
            block = total[l * tok_rows : (l + 1) * tok_rows]
            mean = jnp.sum(block, axis=0, keepdims=True) / tok_rows
            mean_out[l : l + 1, :width] = mean
            block = block - mean
            high = block.astype(BF16)
            low = (block - high.astype(F32)).astype(BF16)
            left_op[l, :tok_rows] = high
            left_op[l, tok_rows : 2 * tok_rows] = high
            left_op[l, 2 * tok_rows :] = low
            right_op[l, :tok_rows] = high
            right_op[l, tok_rows : 2 * tok_rows] = low
            right_op[l, 2 * tok_rows :] = high
            most = jnp.sum(block * block, axis=0, keepdims=True)
            most = jnp.max(most, axis=1, keepdims=True)
            mean_out[l : l + 1, width:] = jnp.broadcast_to(most, (1, 128))
    for k in range(1, groups):
        send(mean_out, means.at[k - 1], mean_r.at[k.bit_length() - 1], tok=flip(tok, k, groups))
    for l in range(layers):
        with jax.named_scope("gram_%d" % l):
            product = lax.dot_general(
                left_op[l], right_op[l], (((0,), (0,)), ((), ())), preferred_element_type=F32
            )
            for t in range(groups):
                gram[t, l] = product[t * slab : (t + 1) * slab]
            for d in outward:
                pair[d, l] = send(
                    gram.at[mirror(d) * 2 + 1 - core, l], pair_in.at[d, l], pair_r.at[d, l], tok=partner
                )

    def add_pair(d, l):
        pair[d, l].wait_recv()
        mine = mirror(d) * 2 + core
        gram[mine, l] = gram[mine, l] + pair_in[d, l]

    def correct():
        overall = mean_out[:, :width]
        for k in range(1, groups):
            overall = overall + means[k - 1, :, :width]
        overall = overall / groups
        own_columns = pl.ds(pl.multiple_of(tok * slab, slab), slab)
        for l in range(layers):
            shifts = [mean_out[l : l + 1, :width] - overall[l : l + 1]]
            for k in range(1, groups):
                shifts.append(means[k - 1, l : l + 1, :width] - overall[l : l + 1])
            shifts = jnp.concatenate(shifts, axis=0)
            shifts_t[...] = shifts.T
            corr[l] = jnp.dot(
                shifts_t[own_columns] * tok_rows, shifts,
                precision=lax.Precision.HIGHEST, preferred_element_type=F32,
            )

    def await_means(bit):
        wait_bytes(means.at[2**bit - 1 : 2 ** (bit + 1) - 1], mean_r.at[bit])

    bits = range(1, groups.bit_length() - 1)
    if coded:
        def bound(l, *masks):
            total_bound = None
            for mask in masks:
                same = means[2 * mask - 1] if mask else mean_out
                both = same[l : l + 1, width:] + means[2 * mask, l : l + 1, width:]
                total_bound = both if total_bound is None else total_bound + both
            return jnp.maximum(total_bound[:, :1], 1e-30)

        def paired(d, l):
            pair[d, l].wait_recv()
            return gram[mirror(d) * 2 + core, l] + pair_in[d, l]

        def box(d, l, beyond, slot):
            return pltpu.make_async_remote_copy(
                src_ref=code_out.at[d, l], dst_ref=line_in.at[slot, l], send_sem=out_sem,
                recv_sem=gl_r.at[slot, l], device_id={"tok": mirror(beyond) * 2 + core},
                device_id_type=pl.DeviceIdType.MESH,
            )

        def post(d, l, beyond, slot, *masks, value=None):
            code_out[d, l] = encode(paired(d, l) if value is None else value, bound(l, *masks))
            box(d, l, beyond, slot).start()

        def unbox(l, slot, *masks):
            wait_bytes(line_in.at[slot, l], gl_r.at[slot, l])
            return decode(line_in[slot, l], bound(l, *masks))

        far_end = chips - 1
        with jax.named_scope("bound"):
            await_means(0)

        @pl.when(rank == 0)
        def _():
            with jax.named_scope("post"):
                for l in range(layers):
                    post(far_end, l, 1, 0, 0)
                    if l:
                        post(1, l - 1, 1, 1, 0)
                    post(2, l, 2, 3, 0)
                post(1, layers - 1, 1, 1, 0)
            await_means(1)

        @pl.when(rank == 1)
        def _():
            with jax.named_scope("post"):
                for l in range(layers):
                    post(2, l, 2, 2, 0)
                    post(0, l, 0, 1, 0)
            await_means(1)
            with jax.named_scope("relay"):
                for l in range(layers):
                    value = paired(far_end, l)
                    post(far_end, l, far_end, 2, 0, 1, value=value + unbox(l, 0, 1))

        for bit in bits[1:]:
            await_means(bit)
        with jax.named_scope("correct"):
            correct()

        def finish_sum(l):
            if l is None:
                for _ in range(3 * layers):
                    wait_bytes(code_out.at[0, 0], out_sem)
                return

            @pl.when(rank == 0)
            def _():
                value = paired(0, l) + unbox(l, 1, 1)
                gram[tok, l] = value + unbox(l, 2, 2, 3)

            @pl.when(rank == 1)
            def _():
                value = paired(1, l) + unbox(l, 3, 2)
                value = value + unbox(l, 2, 3)
                gram[tok, l] = value + unbox(l, 1, 1)

    else:
        def line_sum(d, l, primary):
            upward = low_side if primary else jnp.logical_not(low_side)
            way = jnp.where(upward, 0, 1)
            target = mirror(d)
            beyond = jnp.clip(jnp.where(upward, chip + 1, chip - 1), 0, chips - 1)
            return way, pltpu.make_async_remote_copy(
                src_ref=gram.at[target * 2 + core, l], dst_ref=line_in.at[way, target, l],
                send_sem=out_sem, recv_sem=gl_r.at[way, target, l],
                device_id={"tok": beyond * 2 + core}, device_id_type=pl.DeviceIdType.MESH,
            )

        def arrive(d, l, primary):
            way, copy = line_sum(d, l, primary)
            copy.wait_recv()
            mine = mirror(d) * 2 + core
            gram[mine, l] = gram[mine, l] + line_in[way, mirror(d), l]

        def forward(d, l, primary):
            @pl.when(d > rank if primary else d < rank)
            def _():
                if primary:
                    pl.when(rank > 0)(functools.partial(arrive, d, l, True))
                else:
                    arrive(d, l, False)
                line_sum(d, l, primary)[1].start()

        steps = []
        for d in range(chips):
            for l in range(layers):
                steps.append(((chips - 1 - d) * layers + l, True, d, l))
                if d < chips - 1:
                    steps.append((d * layers + l + layers - 0.5, False, d, l))
        seen = set()
        for _, primary, d, l in sorted(steps):
            if (d, l) not in seen:
                seen.add((d, l))
                add_pair(d, l)
            if d > 0 or not primary:
                forward(d, l, primary)
        for bit in range(groups.bit_length() - 1):
            await_means(bit)
        correct()

        def finish_sum(l):
            if l is None:
                for d in range(chips):
                    for m in range(layers):
                        for primary in (True, False):
                            @pl.when(d > rank if primary else d < rank)
                            def _():
                                line_sum(d, m, primary)[1].wait_send()
                return

            for primary in (True, False):
                @pl.when(jnp.logical_or(rank > 0, not primary))
                def _():
                    upward = low_side if primary else jnp.logical_not(low_side)
                    way = jnp.where(upward, 0, 1)
                    wait_bytes(line_in.at[way, chip, l], gl_r.at[way, chip, l])
                    gram[tok, l] = gram[tok, l] + line_in[way, chip, l]

    edge = None
    for l in range(layers):
        with jax.named_scope("own_%d" % l):
            finish_sum(l)
        result = gram[tok, l] + corr[l]
        sketch_ref[l] = result
        if l == 0:
            edge_out[...] = result.astype(BF16)
            edge = send(
                edge_out, edge_in, edge_r, section=(section + sections - 1) % sections
            )

    lane = lax.broadcasted_iota(jnp.int32, (1, 128), 1)

    def inner(first, second):
        columns = jnp.sum(first * second, axis=0, keepdims=True)
        return jnp.sum(columns, axis=1, keepdims=True)

    with jax.named_scope("prods"):
        own = [sketch_ref[l] for l in range(layers)]
        terms = [inner(own[l], own[l]) for l in range(layers)]
        terms += [inner(own[l - 1], own[l]) for l in range(1, layers)]
        row = jnp.zeros((1, 128), F32)
        for i, term in enumerate(terms):
            row = jnp.where(lane == i, term, row)
    base = 2 * layers - 1
    with jax.named_scope("edge_wait"):
        edge.wait_recv()
    beyond = edge_in[...].astype(F32)
    row = jnp.where(lane == base, inner(own[-1], beyond), row)
    prod_out[...] = jnp.where(lane == base + 1, inner(beyond, beyond), row)
    for k in range(groups):
        other = flip(tok, k, groups)
        send(prod_out, prods.at[1, k], prod_r.at[1], section=(section + 1) % sections, tok=other)
        if k:
            send(prod_out, prods.at[0, k], prod_r.at[0], tok=other)
    with jax.named_scope("prodwait"):
        wait_bytes(prods.at[0, 1:], prod_r.at[0])
        products = prod_out[...]
        for k in range(1, groups):
            products = products + prods[0, k]
        wait_bytes(prods.at[1], prod_r.at[1])
        earlier = prods[1, 0]
        for k in range(1, groups):
            earlier = earlier + prods[1, k]
    with jax.named_scope("final"):
        def item(i, values=products):
            return jnp.sum(jnp.where(lane == i, values, 0.0), axis=1, keepdims=True)

        first, last = section == 0, section == sections - 1
        before = jnp.where(first, item(0), item(layers - 1, earlier))
        before_cross = jnp.where(first, item(0), item(base, earlier))
        beyond_square = jnp.where(last, item(layers - 1), item(base + 1))
        beyond_cross = jnp.where(last, item(layers - 1), item(base))
        squares = [before] + [item(l) for l in range(layers)] + [beyond_square]
        chained = [before_cross] + [item(layers + l) for l in range(layers - 1)] + [beyond_cross]
        ratios = [chained[i] / jnp.sqrt(squares[i] * squares[i + 1]) for i in range(layers + 1)]
        column = lax.broadcasted_iota(jnp.int32, (1, 2), 1)
        for l in range(layers):
            sim_ref[l : l + 1] = jnp.where(column == 0, ratios[l], ratios[l + 1])

    with jax.named_scope("sends"):
        for copy in pending:
            copy.wait_send()
        finish_sum(None)
        for source in [chip] + [t // 2 for t in order[2::2]]:
            for c in list(chunks) + ([extra] if extra else []):
                along(source, c, lambda copy: copy.wait_send())


def finish(sketch_in, sim_in, sketch_out, sim_out, sems):
    copies = [
        pltpu.make_async_copy(source, target, sems.at[n])
        for n, (source, target) in enumerate(((sketch_in, sketch_out), (sim_in, sim_out)))
    ]
    for copy in copies:
        copy.start()
    for copy in copies:
        copy.wait()


def local(sections, groups, activations, projection):
    layers, tok_rows, model_width = activations.shape
    depth, width = projection.shape
    rows = layers * tok_rows
    chips, slab = groups // 2, width // groups
    piece = depth // sections
    share_rows = piece * SHARE // 256 // 16 * 16 if piece % 64 == 0 else piece // 2
    start_rows = min(FIRST, share_rows)
    parts = [(start_rows, 0), (share_rows - start_rows, 0), (share_rows, 1), (piece - 2 * share_rows, None)]
    parts = [part for part in parts if part[0]]
    coded = chips == 4
    dma = pltpu.SemaphoreType.DMA
    sketch, sim = pl.pallas_call(
        functools.partial(kernel, sections, groups, layers, parts, coded),
        out_shape=(pltpu.VMEM((layers, slab, width), F32), pltpu.VMEM((layers, 2), F32)),
        in_specs=[pl.BlockSpec(memory_space=pl.ANY)] * 2,
        out_specs=(pl.BlockSpec(memory_space=pltpu.VMEM),) * 2,
        scratch_shapes=[
            pltpu.VMEM((groups, rows, depth), BF16),
            pltpu.VMEM((groups, depth, width), BF16),
            pltpu.VMEM((rows, width), F32),
            pltpu.VMEM((layers, 3 * tok_rows, width), BF16),
            pltpu.VMEM((layers, 3 * tok_rows, width), BF16),
            pltpu.VMEM((groups, layers, slab, width), F32),
            pltpu.VMEM((chips, layers, slab, width), F32),
            pltpu.VMEM((4, layers, slab, width), BF16) if coded
            else pltpu.VMEM((2, chips, layers, slab, width), F32),
            pltpu.VMEM((chips, layers, slab, width), BF16),
            pltpu.VMEM((layers, width + 128), F32),
            pltpu.VMEM((groups - 1, layers, width + 128), F32),
            pltpu.VMEM((layers, slab, width), F32),
            pltpu.VMEM((width, groups), F32),
            pltpu.VMEM((slab, width), BF16),
            pltpu.VMEM((slab, width), BF16),
            pltpu.VMEM((1, 128), F32),
            pltpu.VMEM((2, groups, 1, 128), F32),
            dma(()), dma((3,)), dma((2,)), dma(()),
            dma((chips, len(parts) + 1)), dma((chips - 1, sections // 2, 2)),
            dma((chips - 1, 2)), dma((groups.bit_length() - 1,)), dma((chips, layers)),
            dma((4, layers)) if coded else dma((2, chips, layers)), dma(()), dma((2,)),
        ],
        compiler_params=pltpu.CompilerParams(
            collective_id=0, has_side_effects=True, vmem_limit_bytes=60 * 1024 * 1024
        ),
    )(activations.reshape(rows, model_width), projection)
    sketch, similarity = pl.pallas_call(
        finish,
        out_shape=(
            jax.ShapeDtypeStruct((layers, slab, width), F32),
            jax.ShapeDtypeStruct((layers, 2), F32),
        ),
        in_specs=[pl.BlockSpec(memory_space=pltpu.VMEM)] * 2,
        out_specs=(pl.BlockSpec(memory_space=pl.ANY),) * 2,
        scratch_shapes=[pltpu.SemaphoreType.DMA((2,))],
    )(*(pltpu.with_memory_space_constraint(part, pltpu.VMEM) for part in (sketch, sim)))
    return jnp.swapaxes(sketch, 1, 2), similarity


def solution(mesh):
    return jax.shard_map(
        functools.partial(local, mesh.shape["section"], mesh.shape["tok"]),
        mesh=mesh,
        in_specs=(P("section", "tok", None), P("tok", None)),
        out_specs=(P("section", None, "tok"), P("section", None)),
        check_vma=False,
    )
```

```python
import functools
import math

import jax
import jax.numpy as jnp
from jax import lax
from jax.experimental import pallas as pl
from jax.experimental.pallas import tpu as pltpu
from jax.sharding import PartitionSpec as P

F32, BF16 = jnp.float32, jnp.bfloat16
SHARE = 64
FIRST = 32
TOP = 1400.0


def flip(index, mask, size):
    result, bit = 0, 1
    while bit < size:
        digit = (index // bit) % 2
        result = result + bit * ((1 - digit) if mask & bit else digit)
        bit *= 2
    return result


def nearest(chip, n, chips):
    short = jnp.minimum(chip, chips - 1 - chip)
    low_side = chip < chips // 2
    paired = n <= 2 * short
    distance = jnp.where(paired, (n + 1) // 2, n - short)
    lower = jnp.where(paired, jnp.logical_xor(low_side, n % 2 == 0), jnp.logical_not(low_side))
    return jnp.where(lower, chip - distance, chip + distance)


def snake(place, sections):
    half = sections // 2
    return jnp.where(place < half, place, 3 * half - 1 - place)


def encode(value, bound):
    scaled = value * (TOP / bound)
    square = scaled * scaled
    fourth = square * square
    power = fourth * fourth * fourth
    return jnp.where(scaled < 0, -power, power).astype(BF16)


def decode(code, bound):
    power = code.astype(F32)
    size = jnp.abs(power)
    root = jnp.exp(jnp.log(size) * (1 / 12)) * (bound / TOP)
    root = jnp.where(size > 0, root, 0.0)
    return jnp.where(power < 0, -root, root)


def gather_plan(half_ring, others, relayed, extra):
    def near(k):
        return [("near", k, j, g) for g in range(2 if extra else 1) for j in range(1, half_ring)]

    def relay(k):
        return [("relay", k)] if half_ring > 1 else []

    before = range(1, others)
    order = [("inner_first",)] if others > 1 else []
    order += [event for k in before if k > 1 for event in near(k)]
    order += [event for k in before if k > 1 for event in relay(k)]
    order += [("own", k) for k in before]
    for k in before:
        order += [("partner", k)] + ([("inner_extra", 2)] if k == 1 else [])
    order += [("inner_extra", k) for k in range(3, others + 1)]
    last_near = near(others)
    order += last_near[: half_ring - 1] + relay(others)
    order += [("outer_extra", 1)] + last_near[half_ring - 1 :]
    order += [("far", k) for k in before] + [("outer_extra", 2), ("own", others)]
    order += [("own_far", k) for k in before] + [("partner", others), ("far", others)]
    order += [("outer_extra", k) for k in range(3, others + 1)]
    order += [("partner_far", k) for k in before]
    return [event for event in order if extra or "extra" not in event[0]]


def kernel(
    sections, groups, layers, parts, coded, acts_hbm, proj_hbm, sketch_ref, sim_ref,
    acts, proj, total, left_op, right_op, gram, pair_in, line_in, code_out, mean_out, means, corr,
    shifts_t, edge_out, edge_in, prod_out, prods,
    out_sem, acts_sem, own_sem, slab_r, line_r, ring_r, d2d_r, mean_r, pair_r, gl_r, edge_r, prod_r,
):
    section = lax.axis_index("section")
    tok = lax.axis_index("tok")
    chips = groups // 2
    chip, core = tok // 2, tok % 2
    partner = chip * 2 + 1 - core
    rows = acts.shape[1]
    tok_rows = rows // layers
    depth = proj.shape[1]
    width = proj.shape[2]
    slab = width // groups
    half_ring = sections // 2
    piece = depth // sections
    sizes = [size for size, _ in parts]
    chunks = range(len(parts))
    relayed = [c for c in chunks if parts[c][1] is not None]
    extra = len(parts) if len(relayed) < len(parts) else None
    align = math.gcd(piece, *sizes)
    place = snake(section, sections)
    to_right = snake((place + 1) % sections, sections)
    to_left = snake((place + sections - 1) % sections, sections)

    def rows_of(at, c):
        start = at % sections * piece + sum(sizes[:c])
        return pl.ds(pl.multiple_of(start, align), sizes[c])

    for n in range(sections):
        part = pl.ds(pl.multiple_of((place + n) % sections * piece, piece), piece)
        pltpu.make_async_copy(proj_hbm.at[part], proj.at[tok, part], own_sem.at[min(n, 1)]).start()

    def wait_bytes(ref, sem):
        pltpu.make_async_copy(ref, ref, sem).wait()

    with jax.named_scope("barrier"):
        barrier = pltpu.get_barrier_semaphore()
        beside = [{"tok": partner}, {"section": to_right}]
        if sections > 2:
            beside.append({"section": to_left})
        for where in beside:
            pl.semaphore_signal(
                barrier, inc=1, device_id=where, device_id_type=pl.DeviceIdType.MESH
            )
        inner_chip = jnp.logical_and(chip > 0, chip < chips - 1)
        for step in (-1, 1):
            @pl.when(jnp.logical_and(chip + step >= 0, chip + step <= chips - 1))
            def _():
                pl.semaphore_signal(
                    barrier, inc=1, device_id={"tok": tok + 2 * step},
                    device_id_type=pl.DeviceIdType.MESH,
                )
        pl.semaphore_wait(barrier, len(beside) + 1 + inner_chip.astype(jnp.int32))

    pending = []

    def remote(src, dst, recv_sem, **where):
        pending.append(
            pltpu.make_async_remote_copy(
                src_ref=src, dst_ref=dst, send_sem=out_sem, recv_sem=recv_sem,
                device_id=where, device_id_type=pl.DeviceIdType.MESH,
            )
        )
        return pending[-1]

    def send(*args, **where):
        copy = remote(*args, **where)
        copy.start()
        return copy

    def line_ref(t, c):
        return proj.at[t, rows_of(place + half_ring, c - 1) if c == extra else rows_of(place, c)]

    def line_copy(source, c, step):
        ref = line_ref(source * 2 + core, c)
        return pltpu.make_async_remote_copy(
            src_ref=ref, dst_ref=ref,
            send_sem=out_sem, recv_sem=line_r.at[source, c],
            device_id={"tok": (chip + step + chips) % chips * 2 + core},
            device_id_type=pl.DeviceIdType.MESH,
        )

    def along(source, c, action):
        for step in (-1, 1):
            inside = chip + step <= chips - 1 if step == 1 else chip + step >= 0
            away = source <= chip if step == 1 else source >= chip

            @pl.when(jnp.logical_and(inside, away))
            def _():
                action(line_copy(source, c, step))

    with jax.named_scope("own_wait"):
        wait_bytes(proj.at[tok, pl.ds(0, piece)], own_sem.at[0])
    for c in chunks:
        along(chip, c, lambda copy: copy.start())
    wait_bytes(proj.at[tok, pl.ds(0, depth - piece)], own_sem.at[1])
    partner_slab = send(proj.at[tok], proj.at[tok], slab_r, tok=partner)
    outer_chip = jnp.minimum(chip, chips - 1 - chip) == 0
    if extra:
        @pl.when(outer_chip)
        def _():
            along(chip, extra, lambda copy: copy.start())

    order = [tok, partner]
    for k in range(1, chips):
        other = nearest(chip, k, chips)
        order += [other * 2 + core, other * 2 + 1 - core]
    for n, t in enumerate(order):
        start = pl.multiple_of(t * depth, depth)
        pltpu.make_async_copy(
            acts_hbm.at[:, pl.ds(start, depth)], acts.at[n], acts_sem.at[min(n, 2)]
        ).start()
    loaded = []

    def await_acts(n):
        if min(n, 2) not in loaded:
            loaded.append(min(n, 2))
            wait_bytes(acts.at[n] if n < 2 else acts.at[2:], acts_sem.at[min(n, 2)])

    def multiply(n, first=False):
        product = jnp.dot(acts[n], proj[order[n]], preferred_element_type=F32)
        if first:
            total[...] = product
        else:
            total[...] += product

    def multiply_piece(n, at):
        part = pl.ds(pl.multiple_of(at % sections * piece, piece), piece)
        total[...] += jnp.dot(acts[n, :, part], proj[order[n], part], preferred_element_type=F32)

    with jax.named_scope("mul0"):
        await_acts(0)
        multiply(0, True)
    with jax.named_scope("mul1"):
        partner_slab.wait_recv()
        await_acts(1)
        multiply(1)

    split = piece % 128 == 0

    def share(k, ref, opposite=False):
        return remote(ref, ref, d2d_r.at[k - 1, int(opposite)], tok=partner)

    def await_shares(k, opposite):
        n = piece if opposite else depth - piece
        wait_bytes(proj.at[order[2 * k + 1], pl.ds(0, n)], d2d_r.at[k - 1, int(opposite)])

    def pass_on(k, j, way, g, ref):
        return remote(
            ref, ref, ring_r.at[k - 1, j - 1, g], section=(to_right if way == 0 else to_left)
        )

    relayed_rows = sum(sizes[c] for c in relayed)
    spans = [(0, relayed_rows)] + ([(relayed_rows, piece - relayed_rows)] if extra else [])

    near = [place]
    for step in range(1, half_ring):
        near += [place + step, place + sections - step]

    first = {}
    for k in range(1, chips):
        for c in chunks:
            ref = line_ref(order[2 * k], c)
            ways = [way for way in range(2) if half_ring > 1 or way == parts[c][1]]
            first[k, c] = [pass_on(k, 1, way, int(c not in relayed), ref) for way in ways] + [share(k, ref)]

    def line_event(k, c):
        with jax.named_scope("ev_line_%d_%d" % (k, c)):
            source = order[2 * k] // 2
            line_copy(source, c, 1).wait_recv()
            along(source, c, lambda copy: copy.start())
            for copy in first[k, c]:
                copy.start()

    nears, relays = {}, {}
    for k in range(1, chips):
        t = order[2 * k]
        for j in range(1, half_ring):
            for g, (start, n) in enumerate(spans):
                nears[k, j, g] = []
                for way in range(2):
                    at = (place + sections - j if way == 0 else place + j) % sections * piece
                    ref = proj.at[t, pl.ds(pl.multiple_of(at + start, align), n)]
                    if j + 1 < half_ring:
                        nears[k, j, g].append(pass_on(k, j + 1, way, g, ref))
                    nears[k, j, g].append(share(k, ref))
        relays[k] = []
        for c in relayed if half_ring > 1 else []:
            way = parts[c][1]
            at = place + sections - half_ring + 1 if way == 0 else place + half_ring - 1
            relays[k].append(pass_on(k, half_ring, way, 0, proj.at[t, rows_of(at, c)]))

    def near_event(k, j, g):
        with jax.named_scope("ev_near_%d_%d_%d" % (k, j, g)):
            wait_bytes(proj.at[order[2 * k], pl.ds(0, 2 * spans[g][1])], ring_r.at[k - 1, j - 1, g])
            for copy in nears[k, j, g]:
                copy.start()

    def relay_event(k):
        for copy in relays[k]:
            copy.start()

    def first_near():
        for j in range(1, half_ring):
            for g in range(len(spans)):
                near_event(1, j, g)
        relay_event(1)

    extras = {}
    if extra:
        for k in range(1, chips):
            extras[k] = share(k, line_ref(order[2 * k], extra), True)

    def extra_event(k):
        if k in extras:
            with jax.named_scope("ev_extra_%d" % k):
                source = order[2 * k] // 2
                line_copy(source, extra, 1).wait_recv()
                along(source, extra, lambda copy: copy.start())
                extras[k].start()

    early = min(3, chips)

    @pl.when(outer_chip)
    def _():
        for k in range(1, early):
            for c in chunks:
                line_event(k, c)
        if chips > 2:
            first_near()

    @pl.when(jnp.logical_not(outer_chip))
    def _():
        for c in chunks:
            for k in reversed(range(1, early)):
                line_event(k, c)

    for k in range(early, chips):
        for c in chunks:
            line_event(k, c)
    if extra:
        @pl.when(jnp.logical_not(outer_chip))
        def _():
            along(chip, extra, lambda copy: copy.start())
            extra_event(1)

    def finish_block(k, from_partner):
        n = 2 * k + from_partner
        if from_partner:
            if not split:
                await_shares(k, False)
            await_shares(k, True)
        if split:
            multiply_piece(n, place + half_ring)
        else:
            await_acts(n)
            multiply(n)

    for event in gather_plan(half_ring, chips - 1, relayed, extra):
        kind = event[0]
        if kind == "inner_first":
            pl.when(jnp.logical_not(outer_chip))(first_near)
            continue
        k = event[1]
        t = order[2 * k] if k < chips else None
        with jax.named_scope("ev_" + "_".join(str(part) for part in event)):
            if kind == "outer_extra":
                pl.when(outer_chip)(functools.partial(extra_event, k))
            elif kind == "inner_extra":
                pl.when(jnp.logical_not(outer_chip))(functools.partial(extra_event, k))
            elif kind == "near":
                near_event(*event[1:])
            elif kind == "relay":
                relay_event(k)
            elif kind == "far":
                wait_bytes(proj.at[t, pl.ds(0, relayed_rows)], ring_r.at[k - 1, half_ring - 1, 0])
                start = (place + half_ring) % sections * piece
                share(k, proj.at[t, pl.ds(pl.multiple_of(start, piece), relayed_rows)], True).start()
            elif kind in ("own", "partner"):
                if split:
                    n = 2 * k + (kind == "partner")
                    await_acts(n)
                    if kind == "partner":
                        await_shares(k, False)
                    for at in near:
                        multiply_piece(n, at)
            else:
                finish_block(k, kind == "partner_far")

    low_side = chip < chips // 2
    rank = jnp.where(low_side, chip, chips - 1 - chip)

    def mirror(d):
        return jnp.where(low_side, d, chips - 1 - d)

    pair = {}
    outward = [chips - 1 - d for d in range(chips)]
    with jax.named_scope("own_end"):
        finish_block(chips - 1, 0)
        finish_block(chips - 1, 1)
    with jax.named_scope("center"):
        for l in range(layers):
            block = total[l * tok_rows : (l + 1) * tok_rows]
            mean = jnp.sum(block, axis=0, keepdims=True) / tok_rows
            mean_out[l : l + 1, :width] = mean
            block = block - mean
            high = block.astype(BF16)
            low = (block - high.astype(F32)).astype(BF16)
            left_op[l, :tok_rows] = high
            left_op[l, tok_rows : 2 * tok_rows] = high
            left_op[l, 2 * tok_rows :] = low
            right_op[l, :tok_rows] = high
            right_op[l, tok_rows : 2 * tok_rows] = low
            right_op[l, 2 * tok_rows :] = high
            most = jnp.sum(block * block, axis=0, keepdims=True)
            most = jnp.max(most, axis=1, keepdims=True)
            mean_out[l : l + 1, width:] = jnp.broadcast_to(most, (1, 128))
    for k in range(1, groups):
        send(mean_out, means.at[k - 1], mean_r.at[k.bit_length() - 1], tok=flip(tok, k, groups))
    for l in range(layers):
        with jax.named_scope("gram_%d" % l):
            product = lax.dot_general(
                left_op[l], right_op[l], (((0,), (0,)), ((), ())), preferred_element_type=F32
            )
            for t in range(groups):
                gram[t, l] = product[t * slab : (t + 1) * slab]
            for d in outward:
                pair[d, l] = send(
                    gram.at[mirror(d) * 2 + 1 - core, l], pair_in.at[d, l], pair_r.at[d, l], tok=partner
                )

    def add_pair(d, l):
        pair[d, l].wait_recv()
        mine = mirror(d) * 2 + core
        gram[mine, l] = gram[mine, l] + pair_in[d, l]

    def correct():
        overall = mean_out[:, :width]
        for k in range(1, groups):
            overall = overall + means[k - 1, :, :width]
        overall = overall / groups
        own_columns = pl.ds(pl.multiple_of(tok * slab, slab), slab)
        for l in range(layers):
            shifts = [mean_out[l : l + 1, :width] - overall[l : l + 1]]
            for k in range(1, groups):
                shifts.append(means[k - 1, l : l + 1, :width] - overall[l : l + 1])
            shifts = jnp.concatenate(shifts, axis=0)
            shifts_t[...] = shifts.T
            corr[l] = jnp.dot(
                shifts_t[own_columns] * tok_rows, shifts,
                precision=lax.Precision.HIGHEST, preferred_element_type=F32,
            )

    def await_means(bit):
        wait_bytes(means.at[2**bit - 1 : 2 ** (bit + 1) - 1], mean_r.at[bit])

    bits = range(1, groups.bit_length() - 1)
    if coded:
        def bound(l, *masks):
            total_bound = None
            for mask in masks:
                same = means[2 * mask - 1] if mask else mean_out
                both = same[l : l + 1, width:] + means[2 * mask, l : l + 1, width:]
                total_bound = both if total_bound is None else total_bound + both
            return jnp.maximum(total_bound[:, :1], 1e-30)

        def paired(d, l):
            pair[d, l].wait_recv()
            return gram[mirror(d) * 2 + core, l] + pair_in[d, l]

        def box(d, l, beyond, slot):
            return pltpu.make_async_remote_copy(
                src_ref=code_out.at[d, l], dst_ref=line_in.at[slot, l], send_sem=out_sem,
                recv_sem=gl_r.at[slot, l], device_id={"tok": mirror(beyond) * 2 + core},
                device_id_type=pl.DeviceIdType.MESH,
            )

        def post(d, l, beyond, slot, *masks, value=None):
            code_out[d, l] = encode(paired(d, l) if value is None else value, bound(l, *masks))
            box(d, l, beyond, slot).start()

        def unbox(l, slot, *masks):
            wait_bytes(line_in.at[slot, l], gl_r.at[slot, l])
            return decode(line_in[slot, l], bound(l, *masks))

        far_end = chips - 1
        with jax.named_scope("bound"):
            await_means(0)

        @pl.when(rank == 0)
        def _():
            with jax.named_scope("post"):
                post(far_end, 0, far_end, 3, 0)
                for l in range(1, layers):
                    post(far_end, l, 1, 0, 0)
                for l in range(layers):
                    post(2, l, 2, 3, 0)
                    post(1, l, 1, 1, 0)
            await_means(1)

        @pl.when(rank == 1)
        def _():
            with jax.named_scope("post"):
                post(far_end, 0, far_end, 2, 0)
                post(2, 0, 2, 2, 0)
                for l in range(layers):
                    post(0, l, 0, 1, 0)
            await_means(1)
            with jax.named_scope("relay"):
                for l in range(1, layers):
                    value = paired(far_end, l)
                    post(far_end, l, far_end, 2, 0, 1, value=value + unbox(l, 0, 1))
                for l in range(1, layers):
                    post(2, l, 2, 2, 0)

        for bit in bits[1:]:
            await_means(bit)
        with jax.named_scope("correct"):
            correct()

        def finish_sum(l):
            if l is None:
                for _ in range(3 * layers):
                    wait_bytes(code_out.at[0, 0], out_sem)
                return

            @pl.when(rank == 0)
            def _():
                value = paired(0, l) + unbox(l, 1, 1)
                if l:
                    gram[tok, l] = value + unbox(l, 2, 2, 3)
                else:
                    gram[tok, l] = value + unbox(l, 3, 3) + unbox(l, 2, 2)

            @pl.when(rank == 1)
            def _():
                value = paired(1, l) + unbox(l, 3, 2)
                value = value + unbox(l, 2, 3)
                gram[tok, l] = value + unbox(l, 1, 1)

    else:
        def line_sum(d, l, primary):
            upward = low_side if primary else jnp.logical_not(low_side)
            way = jnp.where(upward, 0, 1)
            target = mirror(d)
            beyond = jnp.clip(jnp.where(upward, chip + 1, chip - 1), 0, chips - 1)
            return way, pltpu.make_async_remote_copy(
                src_ref=gram.at[target * 2 + core, l], dst_ref=line_in.at[way, target, l],
                send_sem=out_sem, recv_sem=gl_r.at[way, target, l],
                device_id={"tok": beyond * 2 + core}, device_id_type=pl.DeviceIdType.MESH,
            )

        def arrive(d, l, primary):
            way, copy = line_sum(d, l, primary)
            copy.wait_recv()
            mine = mirror(d) * 2 + core
            gram[mine, l] = gram[mine, l] + line_in[way, mirror(d), l]

        def forward(d, l, primary):
            @pl.when(d > rank if primary else d < rank)
            def _():
                if primary:
                    pl.when(rank > 0)(functools.partial(arrive, d, l, True))
                else:
                    arrive(d, l, False)
                line_sum(d, l, primary)[1].start()

        steps = []
        for d in range(chips):
            for l in range(layers):
                steps.append(((chips - 1 - d) * layers + l, True, d, l))
                if d < chips - 1:
                    steps.append((d * layers + l + layers - 0.5, False, d, l))
        seen = set()
        for _, primary, d, l in sorted(steps):
            if (d, l) not in seen:
                seen.add((d, l))
                add_pair(d, l)
            if d > 0 or not primary:
                forward(d, l, primary)
        for bit in range(groups.bit_length() - 1):
            await_means(bit)
        correct()

        def finish_sum(l):
            if l is None:
                for d in range(chips):
                    for m in range(layers):
                        for primary in (True, False):
                            @pl.when(d > rank if primary else d < rank)
                            def _():
                                line_sum(d, m, primary)[1].wait_send()
                return

            for primary in (True, False):
                @pl.when(jnp.logical_or(rank > 0, not primary))
                def _():
                    upward = low_side if primary else jnp.logical_not(low_side)
                    way = jnp.where(upward, 0, 1)
                    wait_bytes(line_in.at[way, chip, l], gl_r.at[way, chip, l])
                    gram[tok, l] = gram[tok, l] + line_in[way, chip, l]

    edge = None
    for l in range(layers):
        with jax.named_scope("own_%d" % l):
            finish_sum(l)
        result = gram[tok, l] + corr[l]
        sketch_ref[l] = result
        if l == 0:
            edge_out[...] = result.astype(BF16)
            edge = pltpu.make_async_remote_copy(
                src_ref=edge_out, dst_ref=edge_in, send_sem=out_sem, recv_sem=edge_r,
                device_id={"section": (section + sections - 1) % sections},
                device_id_type=pl.DeviceIdType.MESH,
            )
            pl.when(section > 0)(edge.start)

    lane = lax.broadcasted_iota(jnp.int32, (1, 128), 1)

    def inner(first, second):
        columns = jnp.sum(first * second, axis=0, keepdims=True)
        return jnp.sum(columns, axis=1, keepdims=True)

    with jax.named_scope("prods"):
        own = [sketch_ref[l] for l in range(layers)]
        terms = [inner(own[l], own[l]) for l in range(layers)]
        terms += [inner(own[l - 1], own[l]) for l in range(1, layers)]
        row = jnp.zeros((1, 128), F32)
        for i, term in enumerate(terms):
            row = jnp.where(lane == i, term, row)
    base = 2 * layers - 1
    prod_out[...] = row

    @pl.when(section < sections - 1)
    def _():
        with jax.named_scope("edge_wait"):
            edge.wait_recv()
        beyond = edge_in[...].astype(F32)
        crossed = jnp.where(lane == base, inner(own[-1], beyond), row)
        prod_out[...] = jnp.where(lane == base + 1, inner(beyond, beyond), crossed)

    onward = [
        pltpu.make_async_remote_copy(
            src_ref=prod_out, dst_ref=prods.at[1, k], send_sem=out_sem, recv_sem=prod_r.at[1],
            device_id={"section": (section + 1) % sections, "tok": flip(tok, k, groups)},
            device_id_type=pl.DeviceIdType.MESH,
        )
        for k in range(groups)
    ]
    across = [
        remote(prod_out, prods.at[0, k], prod_r.at[0], tok=flip(tok, k, groups))
        for k in range(1, groups)
    ]

    @pl.when(section < sections - 1)
    def _():
        for copy in reversed(onward):
            copy.start()

    for copy in reversed(across):
        copy.start()
    with jax.named_scope("prodwait"):
        wait_bytes(prods.at[0, 1:], prod_r.at[0])
        products = prod_out[...]
        for k in range(1, groups):
            products = products + prods[0, k]

        @pl.when(section == 0)
        def _():
            prods[1] = jnp.zeros_like(prods[1])

        @pl.when(section > 0)
        def _():
            wait_bytes(prods.at[1], prod_r.at[1])

        earlier = prods[1, 0]
        for k in range(1, groups):
            earlier = earlier + prods[1, k]
    with jax.named_scope("final"):
        def item(i, values=products):
            return jnp.sum(jnp.where(lane == i, values, 0.0), axis=1, keepdims=True)

        first, last = section == 0, section == sections - 1
        before = jnp.where(first, item(0), item(layers - 1, earlier))
        before_cross = jnp.where(first, item(0), item(base, earlier))
        beyond_square = jnp.where(last, item(layers - 1), item(base + 1))
        beyond_cross = jnp.where(last, item(layers - 1), item(base))
        squares = [before] + [item(l) for l in range(layers)] + [beyond_square]
        chained = [before_cross] + [item(layers + l) for l in range(layers - 1)] + [beyond_cross]
        ratios = [chained[i] / jnp.sqrt(squares[i] * squares[i + 1]) for i in range(layers + 1)]
        column = lax.broadcasted_iota(jnp.int32, (1, 2), 1)
        for l in range(layers):
            sim_ref[l : l + 1] = jnp.where(column == 0, ratios[l], ratios[l + 1])

    with jax.named_scope("sends"):
        for copy in pending:
            copy.wait_send()
        finish_sum(None)
        pl.when(section > 0)(edge.wait_send)

        @pl.when(section < sections - 1)
        def _():
            for copy in onward:
                copy.wait_send()

        for source in [chip] + [t // 2 for t in order[2::2]]:
            for c in list(chunks) + ([extra] if extra else []):
                along(source, c, lambda copy: copy.wait_send())


def finish(sketch_in, sim_in, sketch_out, sim_out, sems):
    copies = [
        pltpu.make_async_copy(source, target, sems.at[n])
        for n, (source, target) in enumerate(((sketch_in, sketch_out), (sim_in, sim_out)))
    ]
    for copy in copies:
        copy.start()
    for copy in copies:
        copy.wait()


def local(sections, groups, activations, projection):
    layers, tok_rows, model_width = activations.shape
    depth, width = projection.shape
    rows = layers * tok_rows
    chips, slab = groups // 2, width // groups
    piece = depth // sections
    share_rows = piece * SHARE // 256 // 16 * 16 if piece % 64 == 0 else piece // 2
    start_rows = min(FIRST, share_rows)
    parts = [(start_rows, 0), (share_rows - start_rows, 0), (share_rows, 1), (piece - 2 * share_rows, None)]
    parts = [part for part in parts if part[0]]
    coded = chips == 4
    dma = pltpu.SemaphoreType.DMA
    sketch, sim = pl.pallas_call(
        functools.partial(kernel, sections, groups, layers, parts, coded),
        out_shape=(pltpu.VMEM((layers, slab, width), F32), pltpu.VMEM((layers, 2), F32)),
        in_specs=[pl.BlockSpec(memory_space=pl.ANY)] * 2,
        out_specs=(pl.BlockSpec(memory_space=pltpu.VMEM),) * 2,
        scratch_shapes=[
            pltpu.VMEM((groups, rows, depth), BF16),
            pltpu.VMEM((groups, depth, width), BF16),
            pltpu.VMEM((rows, width), F32),
            pltpu.VMEM((layers, 3 * tok_rows, width), BF16),
            pltpu.VMEM((layers, 3 * tok_rows, width), BF16),
            pltpu.VMEM((groups, layers, slab, width), F32),
            pltpu.VMEM((chips, layers, slab, width), F32),
            pltpu.VMEM((4, layers, slab, width), BF16) if coded
            else pltpu.VMEM((2, chips, layers, slab, width), F32),
            pltpu.VMEM((chips, layers, slab, width), BF16),
            pltpu.VMEM((layers, width + 128), F32),
            pltpu.VMEM((groups - 1, layers, width + 128), F32),
            pltpu.VMEM((layers, slab, width), F32),
            pltpu.VMEM((width, groups), F32),
            pltpu.VMEM((slab, width), BF16),
            pltpu.VMEM((slab, width), BF16),
            pltpu.VMEM((1, 128), F32),
            pltpu.VMEM((2, groups, 1, 128), F32),
            dma(()), dma((3,)), dma((2,)), dma(()),
            dma((chips, len(parts) + 1)), dma((chips - 1, sections // 2, 2)),
            dma((chips - 1, 2)), dma((groups.bit_length() - 1,)), dma((chips, layers)),
            dma((4, layers)) if coded else dma((2, chips, layers)), dma(()), dma((2,)),
        ],
        compiler_params=pltpu.CompilerParams(
            collective_id=0, has_side_effects=True, vmem_limit_bytes=60 * 1024 * 1024
        ),
    )(activations.reshape(rows, model_width), projection)
    sketch, similarity = pl.pallas_call(
        finish,
        out_shape=(
            jax.ShapeDtypeStruct((layers, slab, width), F32),
            jax.ShapeDtypeStruct((layers, 2), F32),
        ),
        in_specs=[pl.BlockSpec(memory_space=pltpu.VMEM)] * 2,
        out_specs=(pl.BlockSpec(memory_space=pl.ANY),) * 2,
        scratch_shapes=[pltpu.SemaphoreType.DMA((2,))],
    )(*(pltpu.with_memory_space_constraint(part, pltpu.VMEM) for part in (sketch, sim)))
    return jnp.swapaxes(sketch, 1, 2), similarity


def solution(mesh):
    return jax.shard_map(
        functools.partial(local, mesh.shape["section"], mesh.shape["tok"]),
        mesh=mesh,
        in_specs=(P("section", "tok", None), P("tok", None)),
        out_specs=(P("section", None, "tok"), P("section", None)),
        check_vma=False,
    )
```

```python
import functools
import math

import jax
import jax.numpy as jnp
from jax import lax
from jax.experimental import pallas as pl
from jax.experimental.pallas import tpu as pltpu
from jax.sharding import PartitionSpec as P

F32, BF16 = jnp.float32, jnp.bfloat16
SHARE = 64
FIRST = 64
TOP = 1400.0


def flip(index, mask, size):
    result, bit = 0, 1
    while bit < size:
        digit = (index // bit) % 2
        result = result + bit * ((1 - digit) if mask & bit else digit)
        bit *= 2
    return result


def nearest(chip, n, chips):
    short = jnp.minimum(chip, chips - 1 - chip)
    low_side = chip < chips // 2
    paired = n <= 2 * short
    distance = jnp.where(paired, (n + 1) // 2, n - short)
    lower = jnp.where(paired, jnp.logical_xor(low_side, n % 2 == 0), jnp.logical_not(low_side))
    return jnp.where(lower, chip - distance, chip + distance)


def snake(place, sections):
    half = sections // 2
    return jnp.where(place < half, place, 3 * half - 1 - place)


def encode(value, bound):
    scaled = value * (TOP / bound)
    square = scaled * scaled
    fourth = square * square
    power = fourth * fourth * fourth
    return jnp.where(scaled < 0, -power, power).astype(BF16)


def decode(code, bound):
    power = code.astype(F32)
    size = jnp.abs(power)
    root = jnp.exp(jnp.log(size) * (1 / 12)) * (bound / TOP)
    root = jnp.where(size > 0, root, 0.0)
    return jnp.where(power < 0, -root, root)


def gather_plan(half_ring, others, relayed, extra):
    def near(k):
        return [("near", k, j, g) for g in range(2 if extra else 1) for j in range(1, half_ring)]

    def relay(k):
        return [("relay", k)] if half_ring > 1 else []

    before = range(1, others)
    order = [("inner_first",)] if others > 1 else []
    order += [event for k in before if k > 1 for event in near(k)]
    order += [event for k in before if k > 1 for event in relay(k)]
    order += [("own", k) for k in before]
    for k in before:
        order += [("partner", k)] + ([("inner_extra", 2)] if k == 1 else [])
    order += [("inner_extra", k) for k in range(3, others + 1)]
    last_near = near(others)
    order += last_near[: half_ring - 1] + relay(others)
    order += [("outer_extra", 1)] + last_near[half_ring - 1 :]
    order += [("far", k) for k in before] + [("outer_extra", 2), ("own", others)]
    order += [("own_far", k) for k in before] + [("partner", others), ("far", others)]
    order += [("outer_extra", k) for k in range(3, others + 1)]
    order += [("partner_far", k) for k in before]
    return [event for event in order if extra or "extra" not in event[0]]


def kernel(
    sections, groups, layers, parts, coded, acts_hbm, proj_hbm, sketch_ref, sim_ref,
    acts, proj, total, high_op, low_op, gram, pair_in, line_in, code_out, mean_out, means, corr,
    shifts_t, edge_out, edge_in, prod_out, prods,
    out_sem, acts_sem, own_sem, slab_r, line_r, ring_r, d2d_r, mean_r, pair_r, gl_r, edge_r, prod_r,
):
    section = lax.axis_index("section")
    tok = lax.axis_index("tok")
    chips = groups // 2
    chip, core = tok // 2, tok % 2
    partner = chip * 2 + 1 - core
    rows = acts.shape[1]
    tok_rows = rows // layers
    depth = proj.shape[1]
    width = proj.shape[2]
    slab = width // groups
    half_ring = sections // 2
    piece = depth // sections
    sizes = [size for size, _ in parts]
    chunks = range(len(parts))
    relayed = [c for c in chunks if parts[c][1] is not None]
    extra = len(parts) if len(relayed) < len(parts) else None
    align = math.gcd(piece, *sizes)
    place = snake(section, sections)
    to_right = snake((place + 1) % sections, sections)
    to_left = snake((place + sections - 1) % sections, sections)

    def rows_of(at, c):
        start = at % sections * piece + sum(sizes[:c])
        return pl.ds(pl.multiple_of(start, align), sizes[c])

    for n in range(sections):
        part = pl.ds(pl.multiple_of((place + n) % sections * piece, piece), piece)
        pltpu.make_async_copy(proj_hbm.at[part], proj.at[tok, part], own_sem.at[min(n, 1)]).start()

    def wait_bytes(ref, sem):
        pltpu.make_async_copy(ref, ref, sem).wait()

    with jax.named_scope("barrier"):
        barrier = pltpu.get_barrier_semaphore()
        beside = [{"tok": partner}, {"section": to_right}]
        if sections > 2:
            beside.append({"section": to_left})
        for where in beside:
            pl.semaphore_signal(
                barrier, inc=1, device_id=where, device_id_type=pl.DeviceIdType.MESH
            )
        inner_chip = jnp.logical_and(chip > 0, chip < chips - 1)
        for step in (-1, 1):
            @pl.when(jnp.logical_and(chip + step >= 0, chip + step <= chips - 1))
            def _():
                pl.semaphore_signal(
                    barrier, inc=1, device_id={"tok": tok + 2 * step},
                    device_id_type=pl.DeviceIdType.MESH,
                )
        pl.semaphore_wait(barrier, len(beside) + 1 + inner_chip.astype(jnp.int32))

    pending = []

    def remote(src, dst, recv_sem, **where):
        pending.append(
            pltpu.make_async_remote_copy(
                src_ref=src, dst_ref=dst, send_sem=out_sem, recv_sem=recv_sem,
                device_id=where, device_id_type=pl.DeviceIdType.MESH,
            )
        )
        return pending[-1]

    def send(*args, **where):
        copy = remote(*args, **where)
        copy.start()
        return copy

    def line_ref(t, c):
        return proj.at[t, rows_of(place + half_ring, c - 1) if c == extra else rows_of(place, c)]

    def line_copy(source, c, step):
        ref = line_ref(source * 2 + core, c)
        return pltpu.make_async_remote_copy(
            src_ref=ref, dst_ref=ref,
            send_sem=out_sem, recv_sem=line_r.at[source, c],
            device_id={"tok": (chip + step + chips) % chips * 2 + core},
            device_id_type=pl.DeviceIdType.MESH,
        )

    def along(source, c, action):
        for step in (-1, 1):
            inside = chip + step <= chips - 1 if step == 1 else chip + step >= 0
            away = source <= chip if step == 1 else source >= chip

            @pl.when(jnp.logical_and(inside, away))
            def _():
                action(line_copy(source, c, step))

    with jax.named_scope("own_wait"):
        wait_bytes(proj.at[tok, pl.ds(0, piece)], own_sem.at[0])
    for c in chunks:
        along(chip, c, lambda copy: copy.start())
    wait_bytes(proj.at[tok, pl.ds(0, depth - piece)], own_sem.at[1])
    partner_slab = send(proj.at[tok], proj.at[tok], slab_r, tok=partner)
    outer_chip = jnp.minimum(chip, chips - 1 - chip) == 0
    if extra:
        @pl.when(outer_chip)
        def _():
            along(chip, extra, lambda copy: copy.start())

    order = [tok, partner]
    for k in range(1, chips):
        other = nearest(chip, k, chips)
        order += [other * 2 + core, other * 2 + 1 - core]
    for n, t in enumerate(order):
        start = pl.multiple_of(t * depth, depth)
        pltpu.make_async_copy(
            acts_hbm.at[:, pl.ds(start, depth)], acts.at[n], acts_sem.at[min(n, 2)]
        ).start()
    loaded = []

    def await_acts(n):
        if min(n, 2) not in loaded:
            loaded.append(min(n, 2))
            wait_bytes(acts.at[n] if n < 2 else acts.at[2:], acts_sem.at[min(n, 2)])

    def multiply(n, first=False):
        product = jnp.dot(acts[n], proj[order[n]], preferred_element_type=F32)
        if first:
            total[...] = product
        else:
            total[...] += product

    def multiply_piece(n, at):
        part = pl.ds(pl.multiple_of(at % sections * piece, piece), piece)
        total[...] += jnp.dot(acts[n, :, part], proj[order[n], part], preferred_element_type=F32)

    with jax.named_scope("mul0"):
        await_acts(0)
        multiply(0, True)
    with jax.named_scope("mul1"):
        partner_slab.wait_recv()
        await_acts(1)
        multiply(1)

    split = piece % 128 == 0

    def share(k, ref, opposite=False):
        return remote(ref, ref, d2d_r.at[k - 1, int(opposite)], tok=partner)

    def await_shares(k, opposite):
        n = piece if opposite else depth - piece
        wait_bytes(proj.at[order[2 * k + 1], pl.ds(0, n)], d2d_r.at[k - 1, int(opposite)])

    def pass_on(k, j, way, g, ref):
        return remote(
            ref, ref, ring_r.at[k - 1, j - 1, g], section=(to_right if way == 0 else to_left)
        )

    relayed_rows = sum(sizes[c] for c in relayed)
    spans = [(0, relayed_rows)] + ([(relayed_rows, piece - relayed_rows)] if extra else [])

    near = [place]
    for step in range(1, half_ring):
        near += [place + step, place + sections - step]

    first = {}
    for k in range(1, chips):
        for c in chunks:
            ref = line_ref(order[2 * k], c)
            ways = [way for way in range(2) if half_ring > 1 or way == parts[c][1]]
            first[k, c] = [pass_on(k, 1, way, int(c not in relayed), ref) for way in ways] + [share(k, ref)]

    def line_event(k, c):
        with jax.named_scope("ev_line_%d_%d" % (k, c)):
            source = order[2 * k] // 2
            line_copy(source, c, 1).wait_recv()
            along(source, c, lambda copy: copy.start())
            for copy in first[k, c]:
                copy.start()

    nears, relays = {}, {}
    for k in range(1, chips):
        t = order[2 * k]
        for j in range(1, half_ring):
            for g, (start, n) in enumerate(spans):
                nears[k, j, g] = []
                for way in range(2):
                    at = (place + sections - j if way == 0 else place + j) % sections * piece
                    ref = proj.at[t, pl.ds(pl.multiple_of(at + start, align), n)]
                    if j + 1 < half_ring:
                        nears[k, j, g].append(pass_on(k, j + 1, way, g, ref))
                    nears[k, j, g].append(share(k, ref))
        relays[k] = []
        for c in relayed if half_ring > 1 else []:
            way = parts[c][1]
            at = place + sections - half_ring + 1 if way == 0 else place + half_ring - 1
            relays[k].append(pass_on(k, half_ring, way, 0, proj.at[t, rows_of(at, c)]))

    def near_event(k, j, g):
        with jax.named_scope("ev_near_%d_%d_%d" % (k, j, g)):
            wait_bytes(proj.at[order[2 * k], pl.ds(0, 2 * spans[g][1])], ring_r.at[k - 1, j - 1, g])
            for copy in nears[k, j, g]:
                copy.start()

    def relay_event(k):
        for copy in relays[k]:
            copy.start()

    def first_near():
        for j in range(1, half_ring):
            for g in range(len(spans)):
                near_event(1, j, g)
        relay_event(1)

    extras = {}
    if extra:
        for k in range(1, chips):
            extras[k] = share(k, line_ref(order[2 * k], extra), True)

    def extra_event(k):
        if k in extras:
            with jax.named_scope("ev_extra_%d" % k):
                source = order[2 * k] // 2
                line_copy(source, extra, 1).wait_recv()
                along(source, extra, lambda copy: copy.start())
                extras[k].start()

    early = min(3, chips)

    @pl.when(outer_chip)
    def _():
        for k in range(1, early):
            for c in chunks:
                line_event(k, c)
        if chips > 2:
            first_near()

    @pl.when(jnp.logical_not(outer_chip))
    def _():
        for c in chunks:
            for k in reversed(range(1, early)):
                line_event(k, c)

    for k in range(early, chips):
        for c in chunks:
            line_event(k, c)
    if extra:
        @pl.when(jnp.logical_not(outer_chip))
        def _():
            along(chip, extra, lambda copy: copy.start())
            extra_event(1)

    def finish_block(k, from_partner):
        n = 2 * k + from_partner
        if from_partner:
            if not split:
                await_shares(k, False)
            await_shares(k, True)
        if split:
            multiply_piece(n, place + half_ring)
        else:
            await_acts(n)
            multiply(n)

    for event in gather_plan(half_ring, chips - 1, relayed, extra):
        kind = event[0]
        if kind == "inner_first":
            pl.when(jnp.logical_not(outer_chip))(first_near)
            continue
        k = event[1]
        t = order[2 * k] if k < chips else None
        with jax.named_scope("ev_" + "_".join(str(part) for part in event)):
            if kind == "outer_extra":
                pl.when(outer_chip)(functools.partial(extra_event, k))
            elif kind == "inner_extra":
                pl.when(jnp.logical_not(outer_chip))(functools.partial(extra_event, k))
            elif kind == "near":
                near_event(*event[1:])
            elif kind == "relay":
                relay_event(k)
            elif kind == "far":
                wait_bytes(proj.at[t, pl.ds(0, relayed_rows)], ring_r.at[k - 1, half_ring - 1, 0])
                start = (place + half_ring) % sections * piece
                share(k, proj.at[t, pl.ds(pl.multiple_of(start, piece), relayed_rows)], True).start()
            elif kind in ("own", "partner"):
                if split:
                    n = 2 * k + (kind == "partner")
                    await_acts(n)
                    if kind == "partner":
                        await_shares(k, False)
                    for at in near:
                        multiply_piece(n, at)
            else:
                finish_block(k, kind == "partner_far")

    low_side = chip < chips // 2
    rank = jnp.where(low_side, chip, chips - 1 - chip)

    def mirror(d):
        return jnp.where(low_side, d, chips - 1 - d)

    pair = {}
    outward = [chips - 1 - d for d in range(chips)]
    with jax.named_scope("own_end"):
        finish_block(chips - 1, 0)
        finish_block(chips - 1, 1)
    with jax.named_scope("center"):
        for l in range(layers):
            block = total[l * tok_rows : (l + 1) * tok_rows]
            mean = jnp.sum(block, axis=0, keepdims=True) / tok_rows
            mean_out[l : l + 1, :width] = mean
            block = block - mean
            high = block.astype(BF16)
            high_op[l] = high
            low_op[l] = (block - high.astype(F32)).astype(BF16)
            most = jnp.sum(block * block, axis=0, keepdims=True)
            most = jnp.max(most, axis=1, keepdims=True)
            mean_out[l : l + 1, width:] = jnp.broadcast_to(most, (1, 128))
    for k in range(1, groups):
        send(mean_out, means.at[k - 1], mean_r.at[k.bit_length() - 1], tok=flip(tok, k, groups))
    for l in range(layers):
        with jax.named_scope("gram_%d" % l):
            columns = (((0,), (0,)), ((), ()))
            cross = lax.dot_general(high_op[l], low_op[l], columns, preferred_element_type=F32)
            square = lax.dot_general(high_op[l], high_op[l], columns, preferred_element_type=F32)
            product = square + (cross + cross.T)
            for t in range(groups):
                gram[t, l] = product[t * slab : (t + 1) * slab]
            for d in outward:
                pair[d, l] = send(
                    gram.at[mirror(d) * 2 + 1 - core, l], pair_in.at[d, l], pair_r.at[d, l], tok=partner
                )

    def add_pair(d, l):
        pair[d, l].wait_recv()
        mine = mirror(d) * 2 + core
        gram[mine, l] = gram[mine, l] + pair_in[d, l]

    def correct():
        overall = mean_out[:, :width]
        for k in range(1, groups):
            overall = overall + means[k - 1, :, :width]
        overall = overall / groups
        own_columns = pl.ds(pl.multiple_of(tok * slab, slab), slab)
        for l in range(layers):
            shifts = [mean_out[l : l + 1, :width] - overall[l : l + 1]]
            for k in range(1, groups):
                shifts.append(means[k - 1, l : l + 1, :width] - overall[l : l + 1])
            shifts = jnp.concatenate(shifts, axis=0)
            shifts_t[...] = shifts.T
            corr[l] = jnp.dot(
                shifts_t[own_columns] * tok_rows, shifts,
                precision=lax.Precision.HIGHEST, preferred_element_type=F32,
            )

    def await_means(bit):
        wait_bytes(means.at[2**bit - 1 : 2 ** (bit + 1) - 1], mean_r.at[bit])

    bits = range(1, groups.bit_length() - 1)
    if coded:
        def bound(l, *masks):
            total_bound = None
            for mask in masks:
                same = means[2 * mask - 1] if mask else mean_out
                both = same[l : l + 1, width:] + means[2 * mask, l : l + 1, width:]
                total_bound = both if total_bound is None else total_bound + both
            return jnp.maximum(total_bound[:, :1], 1e-34)

        def paired(d, l):
            pair[d, l].wait_recv()
            return gram[mirror(d) * 2 + core, l] + pair_in[d, l]

        def box(d, l, beyond, slot):
            return pltpu.make_async_remote_copy(
                src_ref=code_out.at[d, l], dst_ref=line_in.at[slot, l], send_sem=out_sem,
                recv_sem=gl_r.at[slot, l], device_id={"tok": mirror(beyond) * 2 + core},
                device_id_type=pl.DeviceIdType.MESH,
            )

        def post(d, l, beyond, slot, *masks, value=None):
            code_out[d, l] = encode(paired(d, l) if value is None else value, bound(l, *masks))
            box(d, l, beyond, slot).start()

        def unbox(l, slot, *masks):
            wait_bytes(line_in.at[slot, l], gl_r.at[slot, l])
            return decode(line_in[slot, l], bound(l, *masks))

        far_end = chips - 1
        with jax.named_scope("bound"):
            await_means(0)

        @pl.when(rank == 0)
        def _():
            with jax.named_scope("post"):
                post(far_end, 0, far_end, 3, 0)
                for l in range(1, layers):
                    post(far_end, l, 1, 0, 0)
                for l in range(layers):
                    post(2, l, 2, 3, 0)
                    post(1, l, 1, 1, 0)
            await_means(1)

        @pl.when(rank == 1)
        def _():
            with jax.named_scope("post"):
                post(far_end, 0, far_end, 2, 0)
                post(2, 0, 2, 2, 0)
                for l in range(layers):
                    post(0, l, 0, 1, 0)
            await_means(1)
            with jax.named_scope("relay"):
                for l in range(1, layers):
                    value = paired(far_end, l)
                    post(far_end, l, far_end, 2, 0, 1, value=value + unbox(l, 0, 1))
                for l in range(1, layers):
                    post(2, l, 2, 2, 0)

        for bit in bits[1:]:
            await_means(bit)
        with jax.named_scope("correct"):
            correct()

        def finish_sum(l):
            if l is None:
                for _ in range(3 * layers):
                    wait_bytes(code_out.at[0, 0], out_sem)
                return

            @pl.when(rank == 0)
            def _():
                value = paired(0, l) + unbox(l, 1, 1)
                if l:
                    gram[tok, l] = value + unbox(l, 2, 2, 3)
                else:
                    gram[tok, l] = value + unbox(l, 3, 3) + unbox(l, 2, 2)

            @pl.when(rank == 1)
            def _():
                value = paired(1, l) + unbox(l, 3, 2)
                value = value + unbox(l, 2, 3)
                gram[tok, l] = value + unbox(l, 1, 1)

    else:
        def line_sum(d, l, primary):
            upward = low_side if primary else jnp.logical_not(low_side)
            way = jnp.where(upward, 0, 1)
            target = mirror(d)
            beyond = jnp.clip(jnp.where(upward, chip + 1, chip - 1), 0, chips - 1)
            return way, pltpu.make_async_remote_copy(
                src_ref=gram.at[target * 2 + core, l], dst_ref=line_in.at[way, target, l],
                send_sem=out_sem, recv_sem=gl_r.at[way, target, l],
                device_id={"tok": beyond * 2 + core}, device_id_type=pl.DeviceIdType.MESH,
            )

        def arrive(d, l, primary):
            way, copy = line_sum(d, l, primary)
            copy.wait_recv()
            mine = mirror(d) * 2 + core
            gram[mine, l] = gram[mine, l] + line_in[way, mirror(d), l]

        def forward(d, l, primary):
            @pl.when(d > rank if primary else d < rank)
            def _():
                if primary:
                    pl.when(rank > 0)(functools.partial(arrive, d, l, True))
                else:
                    arrive(d, l, False)
                line_sum(d, l, primary)[1].start()

        steps = []
        for d in range(chips):
            for l in range(layers):
                steps.append(((chips - 1 - d) * layers + l, True, d, l))
                if d < chips - 1:
                    steps.append((d * layers + l + layers - 0.5, False, d, l))
        seen = set()
        for _, primary, d, l in sorted(steps):
            if (d, l) not in seen:
                seen.add((d, l))
                add_pair(d, l)
            if d > 0 or not primary:
                forward(d, l, primary)
        for bit in range(groups.bit_length() - 1):
            await_means(bit)
        correct()

        def finish_sum(l):
            if l is None:
                for d in range(chips):
                    for m in range(layers):
                        for primary in (True, False):
                            @pl.when(d > rank if primary else d < rank)
                            def _():
                                line_sum(d, m, primary)[1].wait_send()
                return

            for primary in (True, False):
                @pl.when(jnp.logical_or(rank > 0, not primary))
                def _():
                    upward = low_side if primary else jnp.logical_not(low_side)
                    way = jnp.where(upward, 0, 1)
                    wait_bytes(line_in.at[way, chip, l], gl_r.at[way, chip, l])
                    gram[tok, l] = gram[tok, l] + line_in[way, chip, l]

    edge = None
    for l in range(layers):
        with jax.named_scope("own_%d" % l):
            finish_sum(l)
        result = gram[tok, l] + corr[l]
        sketch_ref[l] = result
        if l == 0:
            edge_out[...] = result.astype(BF16)
            edge = pltpu.make_async_remote_copy(
                src_ref=edge_out, dst_ref=edge_in, send_sem=out_sem, recv_sem=edge_r,
                device_id={"section": (section + sections - 1) % sections},
                device_id_type=pl.DeviceIdType.MESH,
            )
            pl.when(section > 0)(edge.start)

    lane = lax.broadcasted_iota(jnp.int32, (1, 128), 1)

    def inner(first, second):
        columns = jnp.sum(first * second, axis=0, keepdims=True)
        return jnp.sum(columns, axis=1, keepdims=True)

    with jax.named_scope("prods"):
        own = [sketch_ref[l] for l in range(layers)]
        terms = [inner(own[l], own[l]) for l in range(layers)]
        terms += [inner(own[l - 1], own[l]) for l in range(1, layers)]
        row = jnp.zeros((1, 128), F32)
        for i, term in enumerate(terms):
            row = jnp.where(lane == i, term, row)
    base = 2 * layers - 1
    prod_out[...] = row

    @pl.when(section < sections - 1)
    def _():
        with jax.named_scope("edge_wait"):
            edge.wait_recv()
        beyond = edge_in[...].astype(F32)
        crossed = jnp.where(lane == base, inner(own[-1], beyond), row)
        prod_out[...] = jnp.where(lane == base + 1, inner(beyond, beyond), crossed)

    onward = [
        pltpu.make_async_remote_copy(
            src_ref=prod_out, dst_ref=prods.at[1, k], send_sem=out_sem, recv_sem=prod_r.at[1],
            device_id={"section": (section + 1) % sections, "tok": flip(tok, k, groups)},
            device_id_type=pl.DeviceIdType.MESH,
        )
        for k in range(groups)
    ]
    across = [
        remote(prod_out, prods.at[0, k], prod_r.at[0], tok=flip(tok, k, groups))
        for k in range(1, groups)
    ]

    for copy in reversed(across):
        copy.start()

    @pl.when(section < sections - 1)
    def _():
        for copy in reversed(onward):
            copy.start()
    with jax.named_scope("prodwait"):
        wait_bytes(prods.at[0, 1:], prod_r.at[0])
        products = prod_out[...]
        for k in range(1, groups):
            products = products + prods[0, k]

        @pl.when(section == 0)
        def _():
            prods[1] = jnp.zeros_like(prods[1])

        @pl.when(section > 0)
        def _():
            wait_bytes(prods.at[1], prod_r.at[1])

        earlier = prods[1, 0]
        for k in range(1, groups):
            earlier = earlier + prods[1, k]
    with jax.named_scope("final"):
        def item(i, values=products):
            return jnp.sum(jnp.where(lane == i, values, 0.0), axis=1, keepdims=True)

        first, last = section == 0, section == sections - 1
        before = jnp.where(first, item(0), item(layers - 1, earlier))
        before_cross = jnp.where(first, item(0), item(base, earlier))
        beyond_square = jnp.where(last, item(layers - 1), item(base + 1))
        beyond_cross = jnp.where(last, item(layers - 1), item(base))
        squares = [before] + [item(l) for l in range(layers)] + [beyond_square]
        chained = [before_cross] + [item(layers + l) for l in range(layers - 1)] + [beyond_cross]
        ratios = [chained[i] / jnp.sqrt(squares[i] * squares[i + 1]) for i in range(layers + 1)]
        column = lax.broadcasted_iota(jnp.int32, (1, 2), 1)
        for l in range(layers):
            sim_ref[l : l + 1] = jnp.where(column == 0, ratios[l], ratios[l + 1])

    with jax.named_scope("sends"):
        for copy in pending:
            copy.wait_send()
        finish_sum(None)
        pl.when(section > 0)(edge.wait_send)

        @pl.when(section < sections - 1)
        def _():
            for copy in onward:
                copy.wait_send()

        for source in [chip] + [t // 2 for t in order[2::2]]:
            for c in list(chunks) + ([extra] if extra else []):
                along(source, c, lambda copy: copy.wait_send())


def finish(sketch_in, sim_in, sketch_out, sim_out, sems):
    copies = [
        pltpu.make_async_copy(source, target, sems.at[n])
        for n, (source, target) in enumerate(((sketch_in, sketch_out), (sim_in, sim_out)))
    ]
    for copy in copies:
        copy.start()
    for copy in copies:
        copy.wait()


def local(sections, groups, activations, projection):
    layers, tok_rows, model_width = activations.shape
    depth, width = projection.shape
    rows = layers * tok_rows
    chips, slab = groups // 2, width // groups
    piece = depth // sections
    share_rows = piece * SHARE // 256 // 16 * 16 if piece % 64 == 0 else piece // 2
    start_rows = min(FIRST, share_rows)
    parts = [(start_rows, 0), (share_rows - start_rows, 0), (share_rows, 1), (piece - 2 * share_rows, None)]
    parts = [part for part in parts if part[0]]
    coded = chips == 4
    dma = pltpu.SemaphoreType.DMA
    sketch, sim = pl.pallas_call(
        functools.partial(kernel, sections, groups, layers, parts, coded),
        out_shape=(pltpu.VMEM((layers, slab, width), F32), pltpu.VMEM((layers, 2), F32)),
        in_specs=[pl.BlockSpec(memory_space=pl.ANY)] * 2,
        out_specs=(pl.BlockSpec(memory_space=pltpu.VMEM),) * 2,
        scratch_shapes=[
            pltpu.VMEM((groups, rows, depth), BF16),
            pltpu.VMEM((groups, depth, width), BF16),
            pltpu.VMEM((rows, width), F32),
            pltpu.VMEM((layers, tok_rows, width), BF16),
            pltpu.VMEM((layers, tok_rows, width), BF16),
            pltpu.VMEM((groups, layers, slab, width), F32),
            pltpu.VMEM((chips, layers, slab, width), F32),
            pltpu.VMEM((4, layers, slab, width), BF16) if coded
            else pltpu.VMEM((2, chips, layers, slab, width), F32),
            pltpu.VMEM((chips, layers, slab, width), BF16),
            pltpu.VMEM((layers, width + 128), F32),
            pltpu.VMEM((groups - 1, layers, width + 128), F32),
            pltpu.VMEM((layers, slab, width), F32),
            pltpu.VMEM((width, groups), F32),
            pltpu.VMEM((slab, width), BF16),
            pltpu.VMEM((slab, width), BF16),
            pltpu.VMEM((1, 128), F32),
            pltpu.VMEM((2, groups, 1, 128), F32),
            dma(()), dma((3,)), dma((2,)), dma(()),
            dma((chips, len(parts) + 1)), dma((chips - 1, sections // 2, 2)),
            dma((chips - 1, 2)), dma((groups.bit_length() - 1,)), dma((chips, layers)),
            dma((4, layers)) if coded else dma((2, chips, layers)), dma(()), dma((2,)),
        ],
        compiler_params=pltpu.CompilerParams(
            collective_id=0, has_side_effects=True, vmem_limit_bytes=60 * 1024 * 1024
        ),
    )(activations.reshape(rows, model_width), projection)
    sketch, similarity = pl.pallas_call(
        finish,
        out_shape=(
            jax.ShapeDtypeStruct((layers, slab, width), F32),
            jax.ShapeDtypeStruct((layers, 2), F32),
        ),
        in_specs=[pl.BlockSpec(memory_space=pltpu.VMEM)] * 2,
        out_specs=(pl.BlockSpec(memory_space=pl.ANY),) * 2,
        scratch_shapes=[pltpu.SemaphoreType.DMA((2,))],
    )(*(pltpu.with_memory_space_constraint(part, pltpu.VMEM) for part in (sketch, sim)))
    return jnp.swapaxes(sketch, 1, 2), similarity


def solution(mesh):
    return jax.shard_map(
        functools.partial(local, mesh.shape["section"], mesh.shape["tok"]),
        mesh=mesh,
        in_specs=(P("section", "tok", None), P("tok", None)),
        out_specs=(P("section", None, "tok"), P("section", None)),
        check_vma=False,
    )
```

```python
import functools
import math

import jax
import jax.numpy as jnp
from jax import lax
from jax.experimental import pallas as pl
from jax.experimental.pallas import tpu as pltpu
from jax.sharding import PartitionSpec as P

F32, BF16 = jnp.float32, jnp.bfloat16
SHARE = 64
FIRST = 64
TOP = 1400.0


def flip(index, mask, size):
    result, bit = 0, 1
    while bit < size:
        digit = (index // bit) % 2
        result = result + bit * ((1 - digit) if mask & bit else digit)
        bit *= 2
    return result


def nearest(chip, n, chips):
    short = jnp.minimum(chip, chips - 1 - chip)
    low_side = chip < chips // 2
    paired = n <= 2 * short
    distance = jnp.where(paired, (n + 1) // 2, n - short)
    lower = jnp.where(paired, jnp.logical_xor(low_side, n % 2 == 0), jnp.logical_not(low_side))
    return jnp.where(lower, chip - distance, chip + distance)


def snake(place, sections):
    half = sections // 2
    return jnp.where(place < half, place, 3 * half - 1 - place)


def encode(value, bound):
    scaled = value * (TOP / bound)
    square = scaled * scaled
    fourth = square * square
    power = fourth * fourth * fourth
    return jnp.where(scaled < 0, -power, power).astype(BF16)


def decode(code, bound):
    power = code.astype(F32)
    size = jnp.abs(power)
    root = jnp.exp(jnp.log(size) * (1 / 12)) * (bound / TOP)
    root = jnp.where(size > 0, root, 0.0)
    return jnp.where(power < 0, -root, root)


def gather_plan(half_ring, others, relayed, extra):
    def near(k):
        return [("near", k, j, g) for g in range(2 if extra else 1) for j in range(1, half_ring)]

    def relay(k):
        return [("relay", k)] if half_ring > 1 else []

    before = range(1, others)
    order = [("inner_first",)] if others > 1 else []
    order += [event for k in before if k > 1 for event in near(k)]
    order += [event for k in before if k > 1 for event in relay(k)]
    order += [("own", k) for k in before]
    for k in before:
        order += [("partner", k)] + ([("inner_extra", 2)] if k == 1 else [])
    order += [("inner_extra", k) for k in range(3, others + 1)]
    last_near = near(others)
    order += last_near[: half_ring - 1] + relay(others)
    order += [("outer_extra", 1)] + last_near[half_ring - 1 :]
    order += [("far", k) for k in before] + [("outer_extra", 2), ("own", others)]
    order += [("own_far", k) for k in before] + [("far", others)]
    order += [("outer_extra", k) for k in range(3, others + 1)]
    order += [("partner", others)]
    order += [("partner_far", k) for k in before]
    return [event for event in order if extra or "extra" not in event[0]]


def kernel(
    sections, groups, layers, parts, coded, acts_hbm, proj_hbm, sketch_ref, sim_ref,
    acts, proj, total, high_op, low_op, gram, pair_in, line_in, code_out, mean_out, means, corr,
    shifts_t, edge_out, edge_in, prod_out, prods,
    out_sem, acts_sem, own_sem, slab_r, line_r, ring_r, d2d_r, mean_r, pair_r, gl_r, edge_r, prod_r,
):
    section = lax.axis_index("section")
    tok = lax.axis_index("tok")
    chips = groups // 2
    chip, core = tok // 2, tok % 2
    partner = chip * 2 + 1 - core
    rows = acts.shape[1]
    tok_rows = rows // layers
    depth = proj.shape[1]
    width = proj.shape[2]
    slab = width // groups
    half_ring = sections // 2
    piece = depth // sections
    sizes = [size for size, _ in parts]
    chunks = range(len(parts))
    relayed = [c for c in chunks if parts[c][1] is not None]
    extra = len(parts) if len(relayed) < len(parts) else None
    align = math.gcd(piece, *sizes)
    place = snake(section, sections)
    to_right = snake((place + 1) % sections, sections)
    to_left = snake((place + sections - 1) % sections, sections)

    def rows_of(at, c):
        start = at % sections * piece + sum(sizes[:c])
        return pl.ds(pl.multiple_of(start, align), sizes[c])

    for n in range(sections):
        part = pl.ds(pl.multiple_of((place + n) % sections * piece, piece), piece)
        pltpu.make_async_copy(proj_hbm.at[part], proj.at[tok, part], own_sem.at[min(n, 1)]).start()

    def wait_bytes(ref, sem):
        pltpu.make_async_copy(ref, ref, sem).wait()

    with jax.named_scope("barrier"):
        barrier = pltpu.get_barrier_semaphore()
        beside = [{"tok": partner}, {"section": to_right}]
        if sections > 2:
            beside.append({"section": to_left})
        for where in beside:
            pl.semaphore_signal(
                barrier, inc=1, device_id=where, device_id_type=pl.DeviceIdType.MESH
            )
        inner_chip = jnp.logical_and(chip > 0, chip < chips - 1)
        for step in (-1, 1):
            @pl.when(jnp.logical_and(chip + step >= 0, chip + step <= chips - 1))
            def _():
                pl.semaphore_signal(
                    barrier, inc=1, device_id={"tok": tok + 2 * step},
                    device_id_type=pl.DeviceIdType.MESH,
                )
        pl.semaphore_wait(barrier, len(beside) + 1 + inner_chip.astype(jnp.int32))

    pending = []

    def remote(src, dst, recv_sem, **where):
        pending.append(
            pltpu.make_async_remote_copy(
                src_ref=src, dst_ref=dst, send_sem=out_sem, recv_sem=recv_sem,
                device_id=where, device_id_type=pl.DeviceIdType.MESH,
            )
        )
        return pending[-1]

    def send(*args, **where):
        copy = remote(*args, **where)
        copy.start()
        return copy

    def line_ref(t, c):
        return proj.at[t, rows_of(place + half_ring, c - 1) if c == extra else rows_of(place, c)]

    def line_copy(source, c, step):
        ref = line_ref(source * 2 + core, c)
        return pltpu.make_async_remote_copy(
            src_ref=ref, dst_ref=ref,
            send_sem=out_sem, recv_sem=line_r.at[source, c],
            device_id={"tok": (chip + step + chips) % chips * 2 + core},
            device_id_type=pl.DeviceIdType.MESH,
        )

    def along(source, c, action):
        for step in (-1, 1):
            inside = chip + step <= chips - 1 if step == 1 else chip + step >= 0
            away = source <= chip if step == 1 else source >= chip

            @pl.when(jnp.logical_and(inside, away))
            def _():
                action(line_copy(source, c, step))

    with jax.named_scope("own_wait"):
        wait_bytes(proj.at[tok, pl.ds(0, piece)], own_sem.at[0])
    for c in chunks:
        along(chip, c, lambda copy: copy.start())
    wait_bytes(proj.at[tok, pl.ds(0, depth - piece)], own_sem.at[1])
    partner_slab = send(proj.at[tok], proj.at[tok], slab_r, tok=partner)
    outer_chip = jnp.minimum(chip, chips - 1 - chip) == 0
    if extra:
        @pl.when(outer_chip)
        def _():
            along(chip, extra, lambda copy: copy.start())

    order = [tok, partner]
    for k in range(1, chips):
        other = nearest(chip, k, chips)
        order += [other * 2 + core, other * 2 + 1 - core]
    for n, t in enumerate(order):
        start = pl.multiple_of(t * depth, depth)
        pltpu.make_async_copy(
            acts_hbm.at[:, pl.ds(start, depth)], acts.at[n], acts_sem.at[min(n, 2)]
        ).start()
    loaded = []

    def await_acts(n):
        if min(n, 2) not in loaded:
            loaded.append(min(n, 2))
            wait_bytes(acts.at[n] if n < 2 else acts.at[2:], acts_sem.at[min(n, 2)])

    def multiply(n, first=False):
        product = jnp.dot(acts[n], proj[order[n]], preferred_element_type=F32)
        if first:
            total[...] = product
        else:
            total[...] += product

    def multiply_piece(n, at):
        part = pl.ds(pl.multiple_of(at % sections * piece, piece), piece)
        total[...] += jnp.dot(acts[n, :, part], proj[order[n], part], preferred_element_type=F32)

    with jax.named_scope("mul0"):
        await_acts(0)
        multiply(0, True)
    with jax.named_scope("mul1"):
        partner_slab.wait_recv()
        await_acts(1)
        multiply(1)

    split = piece % 128 == 0

    def share(k, ref, opposite=False):
        return remote(ref, ref, d2d_r.at[k - 1, int(opposite)], tok=partner)

    def await_shares(k, opposite):
        n = piece if opposite else depth - piece
        wait_bytes(proj.at[order[2 * k + 1], pl.ds(0, n)], d2d_r.at[k - 1, int(opposite)])

    def pass_on(k, j, way, g, ref):
        return remote(
            ref, ref, ring_r.at[k - 1, j - 1, g], section=(to_right if way == 0 else to_left)
        )

    relayed_rows = sum(sizes[c] for c in relayed)
    spans = [(0, relayed_rows)] + ([(relayed_rows, piece - relayed_rows)] if extra else [])

    near = [place]
    for step in range(1, half_ring):
        near += [place + step, place + sections - step]

    first = {}
    for k in range(1, chips):
        for c in chunks:
            ref = line_ref(order[2 * k], c)
            ways = [way for way in range(2) if half_ring > 1 or way == parts[c][1]]
            first[k, c] = [pass_on(k, 1, way, int(c not in relayed), ref) for way in ways] + [share(k, ref)]

    def line_event(k, c):
        with jax.named_scope("ev_line_%d_%d" % (k, c)):
            source = order[2 * k] // 2
            line_copy(source, c, 1).wait_recv()
            along(source, c, lambda copy: copy.start())
            for copy in first[k, c]:
                copy.start()

    nears, relays = {}, {}
    for k in range(1, chips):
        t = order[2 * k]
        for j in range(1, half_ring):
            for g, (start, n) in enumerate(spans):
                nears[k, j, g] = []
                for way in range(2):
                    at = (place + sections - j if way == 0 else place + j) % sections * piece
                    ref = proj.at[t, pl.ds(pl.multiple_of(at + start, align), n)]
                    if j + 1 < half_ring:
                        nears[k, j, g].append(pass_on(k, j + 1, way, g, ref))
                    nears[k, j, g].append(share(k, ref))
        relays[k] = []
        for c in relayed if half_ring > 1 else []:
            way = parts[c][1]
            at = place + sections - half_ring + 1 if way == 0 else place + half_ring - 1
            relays[k].append(pass_on(k, half_ring, way, 0, proj.at[t, rows_of(at, c)]))

    def near_event(k, j, g):
        with jax.named_scope("ev_near_%d_%d_%d" % (k, j, g)):
            wait_bytes(proj.at[order[2 * k], pl.ds(0, 2 * spans[g][1])], ring_r.at[k - 1, j - 1, g])
            for copy in nears[k, j, g]:
                copy.start()

    def relay_event(k):
        for copy in relays[k]:
            copy.start()

    def first_near():
        for j in range(1, half_ring):
            for g in range(len(spans)):
                near_event(1, j, g)
        relay_event(1)

    extras = {}
    if extra:
        for k in range(1, chips):
            extras[k] = share(k, line_ref(order[2 * k], extra), True)

    def extra_event(k):
        if k in extras:
            with jax.named_scope("ev_extra_%d" % k):
                source = order[2 * k] // 2
                line_copy(source, extra, 1).wait_recv()
                along(source, extra, lambda copy: copy.start())
                extras[k].start()

    early = min(3, chips)

    @pl.when(outer_chip)
    def _():
        for k in range(1, early):
            for c in chunks:
                line_event(k, c)
        if chips > 2:
            first_near()

    @pl.when(jnp.logical_not(outer_chip))
    def _():
        for c in chunks:
            for k in reversed(range(1, early)):
                line_event(k, c)

    for k in range(early, chips):
        for c in chunks:
            line_event(k, c)
    if extra:
        @pl.when(jnp.logical_not(outer_chip))
        def _():
            along(chip, extra, lambda copy: copy.start())
            extra_event(1)

    def finish_block(k, from_partner):
        n = 2 * k + from_partner
        if from_partner:
            if not split:
                await_shares(k, False)
            await_shares(k, True)
        if split:
            multiply_piece(n, place + half_ring)
        else:
            await_acts(n)
            multiply(n)

    for event in gather_plan(half_ring, chips - 1, relayed, extra):
        kind = event[0]
        if kind == "inner_first":
            pl.when(jnp.logical_not(outer_chip))(first_near)
            continue
        k = event[1]
        t = order[2 * k] if k < chips else None
        with jax.named_scope("ev_" + "_".join(str(part) for part in event)):
            if kind == "outer_extra":
                pl.when(outer_chip)(functools.partial(extra_event, k))
            elif kind == "inner_extra":
                pl.when(jnp.logical_not(outer_chip))(functools.partial(extra_event, k))
            elif kind == "near":
                near_event(*event[1:])
            elif kind == "relay":
                relay_event(k)
            elif kind == "far":
                wait_bytes(proj.at[t, pl.ds(0, relayed_rows)], ring_r.at[k - 1, half_ring - 1, 0])
                start = (place + half_ring) % sections * piece
                share(k, proj.at[t, pl.ds(pl.multiple_of(start, piece), relayed_rows)], True).start()
            elif kind in ("own", "partner"):
                if split:
                    n = 2 * k + (kind == "partner")
                    await_acts(n)
                    if kind == "partner":
                        await_shares(k, False)
                    for at in near:
                        multiply_piece(n, at)
            else:
                finish_block(k, kind == "partner_far")

    low_side = chip < chips // 2
    rank = jnp.where(low_side, chip, chips - 1 - chip)

    def mirror(d):
        return jnp.where(low_side, d, chips - 1 - d)

    pair = {}
    outward = [chips - 1 - d for d in range(chips)]
    with jax.named_scope("own_end"):
        finish_block(chips - 1, 0)
        finish_block(chips - 1, 1)
    with jax.named_scope("center"):
        for l in range(layers):
            block = total[l * tok_rows : (l + 1) * tok_rows]
            mean = jnp.sum(block, axis=0, keepdims=True) / tok_rows
            mean_out[l : l + 1, :width] = mean
            block = block - mean
            high = block.astype(BF16)
            high_op[l] = high
            low_op[l] = (block - high.astype(F32)).astype(BF16)
            most = jnp.sum(block * block, axis=0, keepdims=True)
            most = jnp.max(most, axis=1, keepdims=True)
            mean_out[l : l + 1, width:] = jnp.broadcast_to(most, (1, 128))
    for k in range(1, groups):
        send(mean_out, means.at[k - 1], mean_r.at[k.bit_length() - 1], tok=flip(tok, k, groups))
    for l in range(layers):
        with jax.named_scope("gram_%d" % l):
            columns = (((0,), (0,)), ((), ()))
            cross = lax.dot_general(high_op[l], low_op[l], columns, preferred_element_type=F32)
            square = lax.dot_general(high_op[l], high_op[l], columns, preferred_element_type=F32)
            product = square + (cross + cross.T)
            for t in range(groups):
                gram[t, l] = product[t * slab : (t + 1) * slab]
            for d in outward:
                pair[d, l] = send(
                    gram.at[mirror(d) * 2 + 1 - core, l], pair_in.at[d, l], pair_r.at[d, l], tok=partner
                )

    def add_pair(d, l):
        pair[d, l].wait_recv()
        mine = mirror(d) * 2 + core
        gram[mine, l] = gram[mine, l] + pair_in[d, l]

    def correct():
        overall = mean_out[:, :width]
        for k in range(1, groups):
            overall = overall + means[k - 1, :, :width]
        overall = overall / groups
        own_columns = pl.ds(pl.multiple_of(tok * slab, slab), slab)
        for l in range(layers):
            shifts = [mean_out[l : l + 1, :width] - overall[l : l + 1]]
            for k in range(1, groups):
                shifts.append(means[k - 1, l : l + 1, :width] - overall[l : l + 1])
            shifts = jnp.concatenate(shifts, axis=0)
            shifts_t[...] = shifts.T
            corr[l] = jnp.dot(
                shifts_t[own_columns] * tok_rows, shifts,
                precision=lax.Precision.HIGHEST, preferred_element_type=F32,
            )

    def await_means(bit):
        wait_bytes(means.at[2**bit - 1 : 2 ** (bit + 1) - 1], mean_r.at[bit])

    bits = range(1, groups.bit_length() - 1)
    if coded:
        def bound(l, *masks):
            total_bound = None
            for mask in masks:
                same = means[2 * mask - 1] if mask else mean_out
                both = same[l : l + 1, width:] + means[2 * mask, l : l + 1, width:]
                total_bound = both if total_bound is None else total_bound + both
            return jnp.maximum(total_bound[:, :1], 1e-34)

        def paired(d, l):
            pair[d, l].wait_recv()
            return gram[mirror(d) * 2 + core, l] + pair_in[d, l]

        def box(d, l, beyond, slot):
            return pltpu.make_async_remote_copy(
                src_ref=code_out.at[d, l], dst_ref=line_in.at[slot, l], send_sem=out_sem,
                recv_sem=gl_r.at[slot, l], device_id={"tok": mirror(beyond) * 2 + core},
                device_id_type=pl.DeviceIdType.MESH,
            )

        def post(d, l, beyond, slot, *masks, value=None):
            code_out[d, l] = encode(paired(d, l) if value is None else value, bound(l, *masks))
            box(d, l, beyond, slot).start()

        def unbox(l, slot, *masks):
            wait_bytes(line_in.at[slot, l], gl_r.at[slot, l])
            return decode(line_in[slot, l], bound(l, *masks))

        far_end = chips - 1
        with jax.named_scope("bound"):
            await_means(0)

        @pl.when(rank == 0)
        def _():
            with jax.named_scope("post"):
                post(far_end, 0, far_end, 3, 0)
                for l in range(1, layers):
                    post(far_end, l, 1, 0, 0)
                for l in range(layers):
                    post(2, l, 2, 3, 0)
                    post(1, l, 1, 1, 0)
            await_means(1)

        @pl.when(rank == 1)
        def _():
            with jax.named_scope("post"):
                post(far_end, 0, far_end, 2, 0)
                post(2, 0, 2, 2, 0)
                for l in range(layers):
                    post(0, l, 0, 1, 0)
            await_means(1)
            with jax.named_scope("relay"):
                for l in range(1, layers):
                    value = paired(far_end, l)
                    post(far_end, l, far_end, 2, 0, 1, value=value + unbox(l, 0, 1))
                for l in range(1, layers):
                    post(2, l, 2, 2, 0)

        for bit in bits[1:]:
            await_means(bit)
        with jax.named_scope("correct"):
            correct()

        def finish_sum(l):
            if l is None:
                for _ in range(3 * layers):
                    wait_bytes(code_out.at[0, 0], out_sem)
                return

            @pl.when(rank == 0)
            def _():
                value = paired(0, l) + unbox(l, 1, 1)
                if l:
                    gram[tok, l] = value + unbox(l, 2, 2, 3)
                else:
                    gram[tok, l] = value + unbox(l, 3, 3) + unbox(l, 2, 2)

            @pl.when(rank == 1)
            def _():
                value = paired(1, l) + unbox(l, 3, 2)
                value = value + unbox(l, 2, 3)
                gram[tok, l] = value + unbox(l, 1, 1)

    else:
        def line_sum(d, l, primary):
            upward = low_side if primary else jnp.logical_not(low_side)
            way = jnp.where(upward, 0, 1)
            target = mirror(d)
            beyond = jnp.clip(jnp.where(upward, chip + 1, chip - 1), 0, chips - 1)
            return way, pltpu.make_async_remote_copy(
                src_ref=gram.at[target * 2 + core, l], dst_ref=line_in.at[way, target, l],
                send_sem=out_sem, recv_sem=gl_r.at[way, target, l],
                device_id={"tok": beyond * 2 + core}, device_id_type=pl.DeviceIdType.MESH,
            )

        def arrive(d, l, primary):
            way, copy = line_sum(d, l, primary)
            copy.wait_recv()
            mine = mirror(d) * 2 + core
            gram[mine, l] = gram[mine, l] + line_in[way, mirror(d), l]

        def forward(d, l, primary):
            @pl.when(d > rank if primary else d < rank)
            def _():
                if primary:
                    pl.when(rank > 0)(functools.partial(arrive, d, l, True))
                else:
                    arrive(d, l, False)
                line_sum(d, l, primary)[1].start()

        steps = []
        for d in range(chips):
            for l in range(layers):
                steps.append(((chips - 1 - d) * layers + l, True, d, l))
                if d < chips - 1:
                    steps.append((d * layers + l + layers - 0.5, False, d, l))
        seen = set()
        for _, primary, d, l in sorted(steps):
            if (d, l) not in seen:
                seen.add((d, l))
                add_pair(d, l)
            if d > 0 or not primary:
                forward(d, l, primary)
        for bit in range(groups.bit_length() - 1):
            await_means(bit)
        correct()

        def finish_sum(l):
            if l is None:
                for d in range(chips):
                    for m in range(layers):
                        for primary in (True, False):
                            @pl.when(d > rank if primary else d < rank)
                            def _():
                                line_sum(d, m, primary)[1].wait_send()
                return

            for primary in (True, False):
                @pl.when(jnp.logical_or(rank > 0, not primary))
                def _():
                    upward = low_side if primary else jnp.logical_not(low_side)
                    way = jnp.where(upward, 0, 1)
                    wait_bytes(line_in.at[way, chip, l], gl_r.at[way, chip, l])
                    gram[tok, l] = gram[tok, l] + line_in[way, chip, l]

    edge = None
    for l in range(layers):
        with jax.named_scope("own_%d" % l):
            finish_sum(l)
        result = gram[tok, l] + corr[l]
        sketch_ref[l] = result
        if l == 0:
            edge_out[...] = result.astype(BF16)
            edge = pltpu.make_async_remote_copy(
                src_ref=edge_out, dst_ref=edge_in, send_sem=out_sem, recv_sem=edge_r,
                device_id={"section": (section + sections - 1) % sections},
                device_id_type=pl.DeviceIdType.MESH,
            )
            pl.when(section > 0)(edge.start)

    lane = lax.broadcasted_iota(jnp.int32, (1, 128), 1)

    def inner(first, second):
        columns = jnp.sum(first * second, axis=0, keepdims=True)
        return jnp.sum(columns, axis=1, keepdims=True)

    with jax.named_scope("prods"):
        own = [sketch_ref[l] for l in range(layers)]
        terms = [inner(own[l], own[l]) for l in range(layers)]
        terms += [inner(own[l - 1], own[l]) for l in range(1, layers)]
        row = jnp.zeros((1, 128), F32)
        for i, term in enumerate(terms):
            row = jnp.where(lane == i, term, row)
    base = 2 * layers - 1
    prod_out[...] = row

    @pl.when(section < sections - 1)
    def _():
        with jax.named_scope("edge_wait"):
            edge.wait_recv()
        beyond = edge_in[...].astype(F32)
        crossed = jnp.where(lane == base, inner(own[-1], beyond), row)
        prod_out[...] = jnp.where(lane == base + 1, inner(beyond, beyond), crossed)

    onward = [
        pltpu.make_async_remote_copy(
            src_ref=prod_out, dst_ref=prods.at[1, k], send_sem=out_sem, recv_sem=prod_r.at[1],
            device_id={"section": (section + 1) % sections, "tok": flip(tok, k, groups)},
            device_id_type=pl.DeviceIdType.MESH,
        )
        for k in range(groups)
    ]
    across = [
        remote(prod_out, prods.at[0, k], prod_r.at[0], tok=flip(tok, k, groups))
        for k in range(1, groups)
    ]

    for copy in reversed(across):
        copy.start()

    @pl.when(section < sections - 1)
    def _():
        for copy in reversed(onward):
            copy.start()
    with jax.named_scope("prodwait"):
        wait_bytes(prods.at[0, 1:], prod_r.at[0])
        products = prod_out[...]
        for k in range(1, groups):
            products = products + prods[0, k]

        @pl.when(section == 0)
        def _():
            prods[1] = jnp.zeros_like(prods[1])

        @pl.when(section > 0)
        def _():
            wait_bytes(prods.at[1], prod_r.at[1])

        earlier = prods[1, 0]
        for k in range(1, groups):
            earlier = earlier + prods[1, k]
    with jax.named_scope("final"):
        def item(i, values=products):
            return jnp.sum(jnp.where(lane == i, values, 0.0), axis=1, keepdims=True)

        first, last = section == 0, section == sections - 1
        before = jnp.where(first, item(0), item(layers - 1, earlier))
        before_cross = jnp.where(first, item(0), item(base, earlier))
        beyond_square = jnp.where(last, item(layers - 1), item(base + 1))
        beyond_cross = jnp.where(last, item(layers - 1), item(base))
        squares = [before] + [item(l) for l in range(layers)] + [beyond_square]
        chained = [before_cross] + [item(layers + l) for l in range(layers - 1)] + [beyond_cross]
        ratios = [chained[i] / jnp.sqrt(squares[i] * squares[i + 1]) for i in range(layers + 1)]
        column = lax.broadcasted_iota(jnp.int32, (1, 2), 1)
        for l in range(layers):
            sim_ref[l : l + 1] = jnp.where(column == 0, ratios[l], ratios[l + 1])

    with jax.named_scope("sends"):
        for copy in pending:
            copy.wait_send()
        finish_sum(None)
        pl.when(section > 0)(edge.wait_send)

        @pl.when(section < sections - 1)
        def _():
            for copy in onward:
                copy.wait_send()

        for source in [chip] + [t // 2 for t in order[2::2]]:
            for c in list(chunks) + ([extra] if extra else []):
                along(source, c, lambda copy: copy.wait_send())


def finish(sketch_in, sim_in, sketch_out, sim_out, sems):
    copies = [
        pltpu.make_async_copy(source, target, sems.at[n])
        for n, (source, target) in enumerate(((sketch_in, sketch_out), (sim_in, sim_out)))
    ]
    for copy in copies:
        copy.start()
    for copy in copies:
        copy.wait()


def local(sections, groups, activations, projection):
    layers, tok_rows, model_width = activations.shape
    depth, width = projection.shape
    rows = layers * tok_rows
    chips, slab = groups // 2, width // groups
    piece = depth // sections
    share_rows = piece * SHARE // 256 // 16 * 16 if piece % 64 == 0 else piece // 2
    start_rows = min(FIRST, share_rows)
    parts = [(start_rows, 0), (share_rows - start_rows, 0), (share_rows, 1), (piece - 2 * share_rows, None)]
    parts = [part for part in parts if part[0]]
    coded = chips == 4
    dma = pltpu.SemaphoreType.DMA
    sketch, sim = pl.pallas_call(
        functools.partial(kernel, sections, groups, layers, parts, coded),
        out_shape=(pltpu.VMEM((layers, slab, width), F32), pltpu.VMEM((layers, 2), F32)),
        in_specs=[pl.BlockSpec(memory_space=pl.ANY)] * 2,
        out_specs=(pl.BlockSpec(memory_space=pltpu.VMEM),) * 2,
        scratch_shapes=[
            pltpu.VMEM((groups, rows, depth), BF16),
            pltpu.VMEM((groups, depth, width), BF16),
            pltpu.VMEM((rows, width), F32),
            pltpu.VMEM((layers, tok_rows, width), BF16),
            pltpu.VMEM((layers, tok_rows, width), BF16),
            pltpu.VMEM((groups, layers, slab, width), F32),
            pltpu.VMEM((chips, layers, slab, width), F32),
            pltpu.VMEM((4, layers, slab, width), BF16) if coded
            else pltpu.VMEM((2, chips, layers, slab, width), F32),
            pltpu.VMEM((chips, layers, slab, width), BF16),
            pltpu.VMEM((layers, width + 128), F32),
            pltpu.VMEM((groups - 1, layers, width + 128), F32),
            pltpu.VMEM((layers, slab, width), F32),
            pltpu.VMEM((width, groups), F32),
            pltpu.VMEM((slab, width), BF16),
            pltpu.VMEM((slab, width), BF16),
            pltpu.VMEM((1, 128), F32),
            pltpu.VMEM((2, groups, 1, 128), F32),
            dma(()), dma((3,)), dma((2,)), dma(()),
            dma((chips, len(parts) + 1)), dma((chips - 1, sections // 2, 2)),
            dma((chips - 1, 2)), dma((groups.bit_length() - 1,)), dma((chips, layers)),
            dma((4, layers)) if coded else dma((2, chips, layers)), dma(()), dma((2,)),
        ],
        compiler_params=pltpu.CompilerParams(
            collective_id=0, has_side_effects=True, vmem_limit_bytes=60 * 1024 * 1024
        ),
    )(activations.reshape(rows, model_width), projection)
    sketch, similarity = pl.pallas_call(
        finish,
        out_shape=(
            jax.ShapeDtypeStruct((layers, slab, width), F32),
            jax.ShapeDtypeStruct((layers, 2), F32),
        ),
        in_specs=[pl.BlockSpec(memory_space=pltpu.VMEM)] * 2,
        out_specs=(pl.BlockSpec(memory_space=pl.ANY),) * 2,
        scratch_shapes=[pltpu.SemaphoreType.DMA((2,))],
    )(*(pltpu.with_memory_space_constraint(part, pltpu.VMEM) for part in (sketch, sim)))
    return jnp.swapaxes(sketch, 1, 2), similarity


def solution(mesh):
    return jax.shard_map(
        functools.partial(local, mesh.shape["section"], mesh.shape["tok"]),
        mesh=mesh,
        in_specs=(P("section", "tok", None), P("tok", None)),
        out_specs=(P("section", None, "tok"), P("section", None)),
        check_vma=False,
    )
```

```python
import functools
import math

import jax
import jax.numpy as jnp
from jax import lax
from jax.experimental import pallas as pl
from jax.experimental.pallas import tpu as pltpu
from jax.sharding import PartitionSpec as P

F32, BF16 = jnp.float32, jnp.bfloat16
SHARE = 64
FIRST = 64
TOP = 1400.0


def flip(index, mask, size):
    result, bit = 0, 1
    while bit < size:
        digit = (index // bit) % 2
        result = result + bit * ((1 - digit) if mask & bit else digit)
        bit *= 2
    return result


def nearest(chip, n, chips):
    short = jnp.minimum(chip, chips - 1 - chip)
    low_side = chip < chips // 2
    paired = n <= 2 * short
    distance = jnp.where(paired, (n + 1) // 2, n - short)
    lower = jnp.where(paired, jnp.logical_xor(low_side, n % 2 == 0), jnp.logical_not(low_side))
    return jnp.where(lower, chip - distance, chip + distance)


def snake(place, sections):
    half = sections // 2
    return jnp.where(place < half, place, 3 * half - 1 - place)


def encode(value, bound):
    scaled = value * (TOP / bound)
    square = scaled * scaled
    fourth = square * square
    power = fourth * fourth * fourth
    return jnp.where(scaled < 0, -power, power).astype(BF16)


def decode(code, bound):
    power = code.astype(F32)
    size = jnp.abs(power)
    root = jnp.exp(jnp.log(size) * (1 / 12)) * (bound / TOP)
    root = jnp.where(size > 0, root, 0.0)
    return jnp.where(power < 0, -root, root)


def gather_plan(half_ring, others, relayed, extra):
    def near(k):
        return [("near", k, j, g) for g in range(2 if extra else 1) for j in range(1, half_ring)]

    def relay(k):
        return [("relay", k)] if half_ring > 1 else []

    before = range(1, others)
    order = [("inner_first",)] if others > 1 else []
    order += [event for k in before if k > 1 for event in near(k)]
    order += [event for k in before if k > 1 for event in relay(k)]
    order += [("own", k) for k in before]
    for k in before:
        order += [("partner", k)] + ([("inner_extra", 2)] if k == 1 else [])
    order += [("inner_extra", k) for k in range(3, others + 1)]
    last_near = near(others)
    order += last_near[: half_ring - 1] + relay(others)
    order += [("outer_extra", 1)] + last_near[half_ring - 1 :]
    order += [("far", k) for k in before] + [("outer_extra", 2), ("own", others)]
    order += [("far", others)]
    order += [("outer_extra", k) for k in range(3, others + 1)]
    order += [("own_far", k) for k in before] + [("partner", others)]
    order += [("partner_far", k) for k in before]
    return [event for event in order if extra or "extra" not in event[0]]


def kernel(
    sections, groups, layers, parts, coded, acts_hbm, proj_hbm, sketch_ref, sim_ref,
    acts, proj, total, high_op, low_op, gram, pair_in, line_in, code_out, mean_out, means, corr,
    shifts_t, edge_out, edge_in, prod_out, prods,
    out_sem, acts_sem, own_sem, slab_r, line_r, ring_r, d2d_r, mean_r, pair_r, gl_r, edge_r, prod_r,
):
    section = lax.axis_index("section")
    tok = lax.axis_index("tok")
    chips = groups // 2
    chip, core = tok // 2, tok % 2
    partner = chip * 2 + 1 - core
    rows = acts.shape[1]
    tok_rows = rows // layers
    depth = proj.shape[1]
    width = proj.shape[2]
    slab = width // groups
    half_ring = sections // 2
    piece = depth // sections
    sizes = [size for size, _ in parts]
    chunks = range(len(parts))
    relayed = [c for c in chunks if parts[c][1] is not None]
    extra = len(parts) if len(relayed) < len(parts) else None
    align = math.gcd(piece, *sizes)
    place = snake(section, sections)
    to_right = snake((place + 1) % sections, sections)
    to_left = snake((place + sections - 1) % sections, sections)

    def rows_of(at, c):
        start = at % sections * piece + sum(sizes[:c])
        return pl.ds(pl.multiple_of(start, align), sizes[c])

    for n in range(sections):
        part = pl.ds(pl.multiple_of((place + n) % sections * piece, piece), piece)
        pltpu.make_async_copy(proj_hbm.at[part], proj.at[tok, part], own_sem.at[min(n, 1)]).start()

    def wait_bytes(ref, sem):
        pltpu.make_async_copy(ref, ref, sem).wait()

    with jax.named_scope("barrier"):
        barrier = pltpu.get_barrier_semaphore()
        beside = [{"tok": partner}, {"section": to_right}]
        if sections > 2:
            beside.append({"section": to_left})
        for where in beside:
            pl.semaphore_signal(
                barrier, inc=1, device_id=where, device_id_type=pl.DeviceIdType.MESH
            )
        inner_chip = jnp.logical_and(chip > 0, chip < chips - 1)
        for step in (-1, 1):
            @pl.when(jnp.logical_and(chip + step >= 0, chip + step <= chips - 1))
            def _():
                pl.semaphore_signal(
                    barrier, inc=1, device_id={"tok": tok + 2 * step},
                    device_id_type=pl.DeviceIdType.MESH,
                )
        pl.semaphore_wait(barrier, len(beside) + 1 + inner_chip.astype(jnp.int32))

    pending = []

    def remote(src, dst, recv_sem, **where):
        pending.append(
            pltpu.make_async_remote_copy(
                src_ref=src, dst_ref=dst, send_sem=out_sem, recv_sem=recv_sem,
                device_id=where, device_id_type=pl.DeviceIdType.MESH,
            )
        )
        return pending[-1]

    def send(*args, **where):
        copy = remote(*args, **where)
        copy.start()
        return copy

    def line_ref(t, c):
        return proj.at[t, rows_of(place + half_ring, c - 1) if c == extra else rows_of(place, c)]

    def line_copy(source, c, step):
        ref = line_ref(source * 2 + core, c)
        return pltpu.make_async_remote_copy(
            src_ref=ref, dst_ref=ref,
            send_sem=out_sem, recv_sem=line_r.at[source, c],
            device_id={"tok": (chip + step + chips) % chips * 2 + core},
            device_id_type=pl.DeviceIdType.MESH,
        )

    def along(source, c, action):
        for step in (-1, 1):
            inside = chip + step <= chips - 1 if step == 1 else chip + step >= 0
            away = source <= chip if step == 1 else source >= chip

            @pl.when(jnp.logical_and(inside, away))
            def _():
                action(line_copy(source, c, step))

    with jax.named_scope("own_wait"):
        wait_bytes(proj.at[tok, pl.ds(0, piece)], own_sem.at[0])
    for c in chunks:
        along(chip, c, lambda copy: copy.start())
    wait_bytes(proj.at[tok, pl.ds(0, depth - piece)], own_sem.at[1])
    partner_slab = send(proj.at[tok], proj.at[tok], slab_r, tok=partner)
    outer_chip = jnp.minimum(chip, chips - 1 - chip) == 0
    if extra:
        @pl.when(outer_chip)
        def _():
            along(chip, extra, lambda copy: copy.start())

    order = [tok, partner]
    for k in range(1, chips):
        other = nearest(chip, k, chips)
        order += [other * 2 + core, other * 2 + 1 - core]
    for n, t in enumerate(order):
        start = pl.multiple_of(t * depth, depth)
        pltpu.make_async_copy(
            acts_hbm.at[:, pl.ds(start, depth)], acts.at[n], acts_sem.at[min(n, 2)]
        ).start()
    loaded = []

    def await_acts(n):
        if min(n, 2) not in loaded:
            loaded.append(min(n, 2))
            wait_bytes(acts.at[n] if n < 2 else acts.at[2:], acts_sem.at[min(n, 2)])

    def multiply(n, first=False):
        product = jnp.dot(acts[n], proj[order[n]], preferred_element_type=F32)
        if first:
            total[...] = product
        else:
            total[...] += product

    def multiply_piece(n, at):
        part = pl.ds(pl.multiple_of(at % sections * piece, piece), piece)
        total[...] += jnp.dot(acts[n, :, part], proj[order[n], part], preferred_element_type=F32)

    with jax.named_scope("mul0"):
        await_acts(0)
        multiply(0, True)
    with jax.named_scope("mul1"):
        partner_slab.wait_recv()
        await_acts(1)
        multiply(1)

    split = piece % 128 == 0

    def share(k, ref, opposite=False):
        return remote(ref, ref, d2d_r.at[k - 1, int(opposite)], tok=partner)

    def await_shares(k, opposite):
        n = piece if opposite else depth - piece
        wait_bytes(proj.at[order[2 * k + 1], pl.ds(0, n)], d2d_r.at[k - 1, int(opposite)])

    def pass_on(k, j, way, g, ref):
        return remote(
            ref, ref, ring_r.at[k - 1, j - 1, g], section=(to_right if way == 0 else to_left)
        )

    relayed_rows = sum(sizes[c] for c in relayed)
    spans = [(0, relayed_rows)] + ([(relayed_rows, piece - relayed_rows)] if extra else [])

    near = [place]
    for step in range(1, half_ring):
        near += [place + step, place + sections - step]

    first = {}
    for k in range(1, chips):
        for c in chunks:
            ref = line_ref(order[2 * k], c)
            ways = [way for way in range(2) if half_ring > 1 or way == parts[c][1]]
            first[k, c] = [pass_on(k, 1, way, int(c not in relayed), ref) for way in ways] + [share(k, ref)]

    def line_event(k, c):
        with jax.named_scope("ev_line_%d_%d" % (k, c)):
            source = order[2 * k] // 2
            line_copy(source, c, 1).wait_recv()
            along(source, c, lambda copy: copy.start())
            for copy in first[k, c]:
                copy.start()

    nears, relays = {}, {}
    for k in range(1, chips):
        t = order[2 * k]
        for j in range(1, half_ring):
            for g, (start, n) in enumerate(spans):
                nears[k, j, g] = []
                for way in range(2):
                    at = (place + sections - j if way == 0 else place + j) % sections * piece
                    ref = proj.at[t, pl.ds(pl.multiple_of(at + start, align), n)]
                    if j + 1 < half_ring:
                        nears[k, j, g].append(pass_on(k, j + 1, way, g, ref))
                    nears[k, j, g].append(share(k, ref))
        relays[k] = []
        for c in relayed if half_ring > 1 else []:
            way = parts[c][1]
            at = place + sections - half_ring + 1 if way == 0 else place + half_ring - 1
            relays[k].append(pass_on(k, half_ring, way, 0, proj.at[t, rows_of(at, c)]))

    def near_event(k, j, g):
        with jax.named_scope("ev_near_%d_%d_%d" % (k, j, g)):
            wait_bytes(proj.at[order[2 * k], pl.ds(0, 2 * spans[g][1])], ring_r.at[k - 1, j - 1, g])
            for copy in nears[k, j, g]:
                copy.start()

    def relay_event(k):
        for copy in relays[k]:
            copy.start()

    def first_near():
        for j in range(1, half_ring):
            for g in range(len(spans)):
                near_event(1, j, g)
        relay_event(1)

    extras = {}
    if extra:
        for k in range(1, chips):
            extras[k] = share(k, line_ref(order[2 * k], extra), True)

    def extra_event(k):
        if k in extras:
            with jax.named_scope("ev_extra_%d" % k):
                source = order[2 * k] // 2
                line_copy(source, extra, 1).wait_recv()
                along(source, extra, lambda copy: copy.start())
                extras[k].start()

    early = min(3, chips)

    @pl.when(outer_chip)
    def _():
        for k in range(1, early):
            for c in chunks:
                line_event(k, c)
        if chips > 2:
            first_near()

    @pl.when(jnp.logical_not(outer_chip))
    def _():
        for c in chunks:
            for k in reversed(range(1, early)):
                line_event(k, c)

    for k in range(early, chips):
        for c in chunks:
            line_event(k, c)
    if extra:
        @pl.when(jnp.logical_not(outer_chip))
        def _():
            along(chip, extra, lambda copy: copy.start())
            extra_event(1)

    def finish_block(k, from_partner):
        n = 2 * k + from_partner
        if from_partner:
            if not split:
                await_shares(k, False)
            await_shares(k, True)
        if split:
            multiply_piece(n, place + half_ring)
        else:
            await_acts(n)
            multiply(n)

    for event in gather_plan(half_ring, chips - 1, relayed, extra):
        kind = event[0]
        if kind == "inner_first":
            pl.when(jnp.logical_not(outer_chip))(first_near)
            continue
        k = event[1]
        t = order[2 * k] if k < chips else None
        with jax.named_scope("ev_" + "_".join(str(part) for part in event)):
            if kind == "outer_extra":
                pl.when(outer_chip)(functools.partial(extra_event, k))
            elif kind == "inner_extra":
                pl.when(jnp.logical_not(outer_chip))(functools.partial(extra_event, k))
            elif kind == "near":
                near_event(*event[1:])
            elif kind == "relay":
                relay_event(k)
            elif kind == "far":
                wait_bytes(proj.at[t, pl.ds(0, relayed_rows)], ring_r.at[k - 1, half_ring - 1, 0])
                start = (place + half_ring) % sections * piece
                share(k, proj.at[t, pl.ds(pl.multiple_of(start, piece), relayed_rows)], True).start()
            elif kind in ("own", "partner"):
                if split:
                    n = 2 * k + (kind == "partner")
                    await_acts(n)
                    if kind == "partner":
                        await_shares(k, False)
                    for at in near:
                        multiply_piece(n, at)
            else:
                finish_block(k, kind == "partner_far")

    low_side = chip < chips // 2
    rank = jnp.where(low_side, chip, chips - 1 - chip)

    def mirror(d):
        return jnp.where(low_side, d, chips - 1 - d)

    pair = {}
    outward = [chips - 1 - d for d in range(chips)]
    with jax.named_scope("own_end"):
        finish_block(chips - 1, 0)
        finish_block(chips - 1, 1)
    with jax.named_scope("center"):
        for l in range(layers):
            block = total[l * tok_rows : (l + 1) * tok_rows]
            mean = jnp.sum(block, axis=0, keepdims=True) / tok_rows
            mean_out[l : l + 1, :width] = mean
            block = block - mean
            high = block.astype(BF16)
            high_op[l] = high
            low_op[l] = (block - high.astype(F32)).astype(BF16)
            most = jnp.sum(block * block, axis=0, keepdims=True)
            most = jnp.max(most, axis=1, keepdims=True)
            mean_out[l : l + 1, width:] = jnp.broadcast_to(most, (1, 128))
    for k in range(1, groups):
        send(mean_out, means.at[k - 1], mean_r.at[k.bit_length() - 1], tok=flip(tok, k, groups))
    for l in range(layers):
        with jax.named_scope("gram_%d" % l):
            columns = (((0,), (0,)), ((), ()))
            cross = lax.dot_general(high_op[l], low_op[l], columns, preferred_element_type=F32)
            square = lax.dot_general(high_op[l], high_op[l], columns, preferred_element_type=F32)
            product = square + (cross + cross.T)
            for t in range(groups):
                gram[t, l] = product[t * slab : (t + 1) * slab]
            for d in outward:
                pair[d, l] = send(
                    gram.at[mirror(d) * 2 + 1 - core, l], pair_in.at[d, l], pair_r.at[d, l], tok=partner
                )

    def add_pair(d, l):
        pair[d, l].wait_recv()
        mine = mirror(d) * 2 + core
        gram[mine, l] = gram[mine, l] + pair_in[d, l]

    def correct():
        overall = mean_out[:, :width]
        for k in range(1, groups):
            overall = overall + means[k - 1, :, :width]
        overall = overall / groups
        own_columns = pl.ds(pl.multiple_of(tok * slab, slab), slab)
        for l in range(layers):
            shifts = [mean_out[l : l + 1, :width] - overall[l : l + 1]]
            for k in range(1, groups):
                shifts.append(means[k - 1, l : l + 1, :width] - overall[l : l + 1])
            shifts = jnp.concatenate(shifts, axis=0)
            shifts_t[...] = shifts.T
            corr[l] = jnp.dot(
                shifts_t[own_columns] * tok_rows, shifts,
                precision=lax.Precision.HIGHEST, preferred_element_type=F32,
            )

    def await_means(bit):
        wait_bytes(means.at[2**bit - 1 : 2 ** (bit + 1) - 1], mean_r.at[bit])

    bits = range(1, groups.bit_length() - 1)
    if coded:
        def bound(l, *masks):
            total_bound = None
            for mask in masks:
                same = means[2 * mask - 1] if mask else mean_out
                both = same[l : l + 1, width:] + means[2 * mask, l : l + 1, width:]
                total_bound = both if total_bound is None else total_bound + both
            return jnp.maximum(total_bound[:, :1], 1e-34)

        def paired(d, l):
            pair[d, l].wait_recv()
            return gram[mirror(d) * 2 + core, l] + pair_in[d, l]

        def box(d, l, beyond, slot):
            return pltpu.make_async_remote_copy(
                src_ref=code_out.at[d, l], dst_ref=line_in.at[slot, l], send_sem=out_sem,
                recv_sem=gl_r.at[slot, l], device_id={"tok": mirror(beyond) * 2 + core},
                device_id_type=pl.DeviceIdType.MESH,
            )

        def post(d, l, beyond, slot, *masks, value=None):
            code_out[d, l] = encode(paired(d, l) if value is None else value, bound(l, *masks))
            box(d, l, beyond, slot).start()

        def unbox(l, slot, *masks):
            wait_bytes(line_in.at[slot, l], gl_r.at[slot, l])
            return decode(line_in[slot, l], bound(l, *masks))

        far_end = chips - 1
        with jax.named_scope("bound"):
            await_means(0)

        @pl.when(rank == 0)
        def _():
            with jax.named_scope("post"):
                post(far_end, 0, far_end, 3, 0)
                for l in range(1, layers):
                    post(far_end, l, 1, 0, 0)
                for l in range(layers):
                    post(2, l, 2, 3, 0)
                    post(1, l, 1, 1, 0)
            await_means(1)

        @pl.when(rank == 1)
        def _():
            with jax.named_scope("post"):
                post(far_end, 0, far_end, 2, 0)
                post(2, 0, 2, 2, 0)
                for l in range(layers):
                    post(0, l, 0, 1, 0)
            await_means(1)
            with jax.named_scope("relay"):
                for l in range(1, layers):
                    value = paired(far_end, l)
                    post(far_end, l, far_end, 2, 0, 1, value=value + unbox(l, 0, 1))
                for l in range(1, layers):
                    post(2, l, 2, 2, 0)

        for bit in bits[1:]:
            await_means(bit)
        with jax.named_scope("correct"):
            correct()

        def finish_sum(l):
            if l is None:
                for _ in range(3 * layers):
                    wait_bytes(code_out.at[0, 0], out_sem)
                return

            @pl.when(rank == 0)
            def _():
                value = paired(0, l) + unbox(l, 1, 1)
                if l:
                    gram[tok, l] = value + unbox(l, 2, 2, 3)
                else:
                    gram[tok, l] = value + unbox(l, 3, 3) + unbox(l, 2, 2)

            @pl.when(rank == 1)
            def _():
                value = paired(1, l) + unbox(l, 3, 2)
                value = value + unbox(l, 2, 3)
                gram[tok, l] = value + unbox(l, 1, 1)

    else:
        def line_sum(d, l, primary):
            upward = low_side if primary else jnp.logical_not(low_side)
            way = jnp.where(upward, 0, 1)
            target = mirror(d)
            beyond = jnp.clip(jnp.where(upward, chip + 1, chip - 1), 0, chips - 1)
            return way, pltpu.make_async_remote_copy(
                src_ref=gram.at[target * 2 + core, l], dst_ref=line_in.at[way, target, l],
                send_sem=out_sem, recv_sem=gl_r.at[way, target, l],
                device_id={"tok": beyond * 2 + core}, device_id_type=pl.DeviceIdType.MESH,
            )

        def arrive(d, l, primary):
            way, copy = line_sum(d, l, primary)
            copy.wait_recv()
            mine = mirror(d) * 2 + core
            gram[mine, l] = gram[mine, l] + line_in[way, mirror(d), l]

        def forward(d, l, primary):
            @pl.when(d > rank if primary else d < rank)
            def _():
                if primary:
                    pl.when(rank > 0)(functools.partial(arrive, d, l, True))
                else:
                    arrive(d, l, False)
                line_sum(d, l, primary)[1].start()

        steps = []
        for d in range(chips):
            for l in range(layers):
                steps.append(((chips - 1 - d) * layers + l, True, d, l))
                if d < chips - 1:
                    steps.append((d * layers + l + layers - 0.5, False, d, l))
        seen = set()
        for _, primary, d, l in sorted(steps):
            if (d, l) not in seen:
                seen.add((d, l))
                add_pair(d, l)
            if d > 0 or not primary:
                forward(d, l, primary)
        for bit in range(groups.bit_length() - 1):
            await_means(bit)
        correct()

        def finish_sum(l):
            if l is None:
                for d in range(chips):
                    for m in range(layers):
                        for primary in (True, False):
                            @pl.when(d > rank if primary else d < rank)
                            def _():
                                line_sum(d, m, primary)[1].wait_send()
                return

            for primary in (True, False):
                @pl.when(jnp.logical_or(rank > 0, not primary))
                def _():
                    upward = low_side if primary else jnp.logical_not(low_side)
                    way = jnp.where(upward, 0, 1)
                    wait_bytes(line_in.at[way, chip, l], gl_r.at[way, chip, l])
                    gram[tok, l] = gram[tok, l] + line_in[way, chip, l]

    edge = None
    for l in range(layers):
        with jax.named_scope("own_%d" % l):
            finish_sum(l)
        result = gram[tok, l] + corr[l]
        sketch_ref[l] = result
        if l == 0:
            edge_out[...] = result.astype(BF16)
            edge = pltpu.make_async_remote_copy(
                src_ref=edge_out, dst_ref=edge_in, send_sem=out_sem, recv_sem=edge_r,
                device_id={"section": (section + sections - 1) % sections},
                device_id_type=pl.DeviceIdType.MESH,
            )
            pl.when(section > 0)(edge.start)

    lane = lax.broadcasted_iota(jnp.int32, (1, 128), 1)

    def inner(first, second):
        columns = jnp.sum(first * second, axis=0, keepdims=True)
        return jnp.sum(columns, axis=1, keepdims=True)

    with jax.named_scope("prods"):
        own = [sketch_ref[l] for l in range(layers)]
        terms = [inner(own[l], own[l]) for l in range(layers)]
        terms += [inner(own[l - 1], own[l]) for l in range(1, layers)]
        row = jnp.zeros((1, 128), F32)
        for i, term in enumerate(terms):
            row = jnp.where(lane == i, term, row)
    base = 2 * layers - 1
    prod_out[...] = row

    @pl.when(section < sections - 1)
    def _():
        with jax.named_scope("edge_wait"):
            edge.wait_recv()
        beyond = edge_in[...].astype(F32)
        crossed = jnp.where(lane == base, inner(own[-1], beyond), row)
        prod_out[...] = jnp.where(lane == base + 1, inner(beyond, beyond), crossed)

    onward = [
        pltpu.make_async_remote_copy(
            src_ref=prod_out, dst_ref=prods.at[1, k], send_sem=out_sem, recv_sem=prod_r.at[1],
            device_id={"section": (section + 1) % sections, "tok": flip(tok, k, groups)},
            device_id_type=pl.DeviceIdType.MESH,
        )
        for k in range(groups)
    ]
    across = [
        remote(prod_out, prods.at[0, k], prod_r.at[0], tok=flip(tok, k, groups))
        for k in range(1, groups)
    ]

    for copy in reversed(across):
        copy.start()

    @pl.when(section < sections - 1)
    def _():
        for copy in reversed(onward):
            copy.start()
    with jax.named_scope("prodwait"):
        wait_bytes(prods.at[0, 1:], prod_r.at[0])
        products = prod_out[...]
        for k in range(1, groups):
            products = products + prods[0, k]

        @pl.when(section == 0)
        def _():
            prods[1] = jnp.zeros_like(prods[1])

        @pl.when(section > 0)
        def _():
            wait_bytes(prods.at[1], prod_r.at[1])

        earlier = prods[1, 0]
        for k in range(1, groups):
            earlier = earlier + prods[1, k]
    with jax.named_scope("final"):
        def item(i, values=products):
            return jnp.sum(jnp.where(lane == i, values, 0.0), axis=1, keepdims=True)

        first, last = section == 0, section == sections - 1
        before = jnp.where(first, item(0), item(layers - 1, earlier))
        before_cross = jnp.where(first, item(0), item(base, earlier))
        beyond_square = jnp.where(last, item(layers - 1), item(base + 1))
        beyond_cross = jnp.where(last, item(layers - 1), item(base))
        squares = [before] + [item(l) for l in range(layers)] + [beyond_square]
        chained = [before_cross] + [item(layers + l) for l in range(layers - 1)] + [beyond_cross]
        ratios = [chained[i] / jnp.sqrt(squares[i] * squares[i + 1]) for i in range(layers + 1)]
        column = lax.broadcasted_iota(jnp.int32, (1, 2), 1)
        for l in range(layers):
            sim_ref[l : l + 1] = jnp.where(column == 0, ratios[l], ratios[l + 1])

    with jax.named_scope("sends"):
        for copy in pending:
            copy.wait_send()
        finish_sum(None)
        pl.when(section > 0)(edge.wait_send)

        @pl.when(section < sections - 1)
        def _():
            for copy in onward:
                copy.wait_send()

        for source in [chip] + [t // 2 for t in order[2::2]]:
            for c in list(chunks) + ([extra] if extra else []):
                along(source, c, lambda copy: copy.wait_send())


def finish(sketch_in, sim_in, sketch_out, sim_out, sems):
    copies = [
        pltpu.make_async_copy(source, target, sems.at[n])
        for n, (source, target) in enumerate(((sketch_in, sketch_out), (sim_in, sim_out)))
    ]
    for copy in copies:
        copy.start()
    for copy in copies:
        copy.wait()


def local(sections, groups, activations, projection):
    layers, tok_rows, model_width = activations.shape
    depth, width = projection.shape
    rows = layers * tok_rows
    chips, slab = groups // 2, width // groups
    piece = depth // sections
    share_rows = piece * SHARE // 256 // 16 * 16 if piece % 64 == 0 else piece // 2
    start_rows = min(FIRST, share_rows)
    parts = [(start_rows, 0), (share_rows - start_rows, 0), (share_rows, 1), (piece - 2 * share_rows, None)]
    parts = [part for part in parts if part[0]]
    coded = chips == 4
    dma = pltpu.SemaphoreType.DMA
    sketch, sim = pl.pallas_call(
        functools.partial(kernel, sections, groups, layers, parts, coded),
        out_shape=(pltpu.VMEM((layers, slab, width), F32), pltpu.VMEM((layers, 2), F32)),
        in_specs=[pl.BlockSpec(memory_space=pl.ANY)] * 2,
        out_specs=(pl.BlockSpec(memory_space=pltpu.VMEM),) * 2,
        scratch_shapes=[
            pltpu.VMEM((groups, rows, depth), BF16),
            pltpu.VMEM((groups, depth, width), BF16),
            pltpu.VMEM((rows, width), F32),
            pltpu.VMEM((layers, tok_rows, width), BF16),
            pltpu.VMEM((layers, tok_rows, width), BF16),
            pltpu.VMEM((groups, layers, slab, width), F32),
            pltpu.VMEM((chips, layers, slab, width), F32),
            pltpu.VMEM((4, layers, slab, width), BF16) if coded
            else pltpu.VMEM((2, chips, layers, slab, width), F32),
            pltpu.VMEM((chips, layers, slab, width), BF16),
            pltpu.VMEM((layers, width + 128), F32),
            pltpu.VMEM((groups - 1, layers, width + 128), F32),
            pltpu.VMEM((layers, slab, width), F32),
            pltpu.VMEM((width, groups), F32),
            pltpu.VMEM((slab, width), BF16),
            pltpu.VMEM((slab, width), BF16),
            pltpu.VMEM((1, 128), F32),
            pltpu.VMEM((2, groups, 1, 128), F32),
            dma(()), dma((3,)), dma((2,)), dma(()),
            dma((chips, len(parts) + 1)), dma((chips - 1, sections // 2, 2)),
            dma((chips - 1, 2)), dma((groups.bit_length() - 1,)), dma((chips, layers)),
            dma((4, layers)) if coded else dma((2, chips, layers)), dma(()), dma((2,)),
        ],
        compiler_params=pltpu.CompilerParams(
            collective_id=0, has_side_effects=True, vmem_limit_bytes=60 * 1024 * 1024
        ),
    )(activations.reshape(rows, model_width), projection)
    sketch, similarity = pl.pallas_call(
        finish,
        out_shape=(
            jax.ShapeDtypeStruct((layers, slab, width), F32),
            jax.ShapeDtypeStruct((layers, 2), F32),
        ),
        in_specs=[pl.BlockSpec(memory_space=pltpu.VMEM)] * 2,
        out_specs=(pl.BlockSpec(memory_space=pl.ANY),) * 2,
        scratch_shapes=[pltpu.SemaphoreType.DMA((2,))],
    )(*(pltpu.with_memory_space_constraint(part, pltpu.VMEM) for part in (sketch, sim)))
    return jnp.swapaxes(sketch, 1, 2), similarity


def solution(mesh):
    return jax.shard_map(
        functools.partial(local, mesh.shape["section"], mesh.shape["tok"]),
        mesh=mesh,
        in_specs=(P("section", "tok", None), P("tok", None)),
        out_specs=(P("section", None, "tok"), P("section", None)),
        check_vma=False,
    )
```
